32 devices in a mesh: dp: 8 (over y, x, core), tensor: 4 (over z).
Axes of the slice: x: 2, y: 2, z: 4, core: 2. Of those that a mesh axis runs over, the one named last changes fastest.
Arguments:
- hidden: bfloat16 [1024, 8192], P('dp')
- q_weight: float32 [8192, 4096], P(('dp', 'tensor')), may hold values from -0.0625 to 0.0625
- k_weight: float32 [8192, 1024], P(('dp', 'tensor')), may hold values from -0.0625 to 0.0625
- v_weight: float32 [8192, 1024], P(('dp', 'tensor')), may hold values from -0.0625 to 0.0625
- o_weight: float32 [8192, 4096], P(('dp', 'tensor')), may hold values from -0.09375 to 0.09375
- input_gain: float32 [8192], replicated, may hold values from 0.25 to 1.75
- post_gain: float32 [8192], replicated, may hold values from 0.25 to 1.75
- key_cache: bfloat16 [1024, 64, 8, 128], P('dp', None, 'tensor'), may hold values from -1000 to 1000
- value_cache: bfloat16 [1024, 64, 8, 128], P('dp', None, 'tensor'), may hold values from -6 to 6
- lengths: int32 [1024], P('dp'), may hold values from 1 to 64
Outputs:
- new_hidden: bfloat16 [1024, 8192], P('dp')
- normed: bfloat16 [1024, 8192], P('dp')
- fresh_token_keys: bfloat16 [1024, 8, 128], P('dp', 'tensor')
- new_values: bfloat16 [1024, 8, 128], P('dp', 'tensor')
The draws below stay inside these ranges and needn't reach their ends.
All inputs are finite; a program needn't handle non-finite values.
Results may differ from the reference program's by a relative error of at most 0.012.
The reference program's roundings to bfloat16 on the way count: a program that leaves them out, or rounds other values in their place, can miss the bound.
Values may be sent and summed in bfloat16 or wider, within the bound.
A program may use at most 128 MiB of HBM per device.

```python
import math
import jax
import jax.numpy as jnp
from jax import lax

D = 8192
HEADS = 32
KV_HEADS = 8
HEAD_DIM = 128
CACHE = 64
QD = 4096
KD = 1024
GROUP = 4
BATCH = 1024


def draw_hidden(key, part):
    key_base, key_rows, key_column_slice = jax.random.split(key, 3)
    base = jax.random.normal(key_base, (BATCH, D), jnp.float32)
    row_scale = jnp.exp(jax.random.uniform(key_rows, (BATCH, 1), jnp.float32) * math.log(10.0))
    rising = jnp.exp(jnp.arange(D, dtype=jnp.float32)[None, :] / D * math.log(3.0))
    column_scale = jnp.exp(jax.random.uniform(key_column_slice, (1, D), jnp.float32) * math.log(10.0)) * rising
    return (0.03 * base * row_scale * column_scale).astype(jnp.bfloat16)


def draw_key_cache(key, part):
    key_base = jax.random.fold_in(key, 0)
    shape_full = (BATCH, CACHE, KV_HEADS, HEAD_DIM)
    base = jax.random.normal(key_base, shape_full, jnp.float32)
    return base.astype(jnp.bfloat16)


def touch_ends(entries, rng, low, top_value):
    longest = entries.shape.index(max(entries.shape))
    spots = []
    for shift in (0, 1):
        where = [jax.random.randint(jax.random.fold_in(rng, axis), (), 0, length) for axis, length in enumerate(entries.shape)]
        where[longest] = (where[longest] + shift) % entries.shape[longest]
        spots.append(tuple(where))
    return entries.at[spots[0]].set(low).at[spots[1]].set(top_value)


def block_scale(stream_key, shape, shards, least, top_value):
    loudness = 1.0
    for dim, shards_of in shards:
        heights = jax.random.uniform(jax.random.fold_in(jax.random.fold_in(stream_key, 6), dim), (shards_of,), jnp.float32, least / len(shards), top_value / len(shards))
        loudness = loudness * jnp.repeat(jnp.exp(heights), shape[dim] // shards_of).reshape((-1,) + (1,) * (len(shape) - 1 - dim))
    return loudness


def scatter_about(rng, dims, scale, reach, cuts=(), kind=jnp.bfloat16):
    values = jax.random.normal(rng, dims, jnp.float32) * scale
    if len(cuts) > 0:
        values = block_scale(rng, dims, cuts, -0.22, 0.18) * values
    return jnp.clip(values, min=-reach, max=reach).astype(kind)


def setup_inputs(seed: int = 0) -> dict:
    arg_keys = jax.random.split(jax.random.key(seed), 11)
    return {
        "hidden": draw_hidden(jax.random.fold_in(arg_keys[10], 71), 0),
        "q_weight": scatter_about(arg_keys[1], (D, QD), D ** -0.5, 0.0625, ((0, 32),), jnp.float32),
        "k_weight": scatter_about(arg_keys[2], (D, KD), D ** -0.5, 0.0625, ((0, 32),), jnp.float32),
        "v_weight": scatter_about(arg_keys[3], (D, KD), D ** -0.5, 0.0625, ((0, 32),), jnp.float32),
        "o_weight": scatter_about(arg_keys[4], (D, QD), QD ** -0.5, 0.09375, ((0, 32),), jnp.float32),
        "input_gain": jnp.clip(1.0 + 0.15 * jax.random.normal(arg_keys[5], (D,), jnp.float32), 0.25, 1.75),
        "post_gain": jnp.clip(1.0 + 0.15 * jax.random.normal(arg_keys[6], (D,), jnp.float32), 0.25, 1.75),
        "key_cache": draw_key_cache(jax.random.fold_in(arg_keys[10], 71), 0),
        "value_cache": scatter_about(arg_keys[8], (BATCH, CACHE, KV_HEADS, HEAD_DIM), 1.0, 6.0, ((0, 8), (2, 4))),
        "lengths": touch_ends(jax.random.randint(arg_keys[9], (BATCH,), 1, CACHE + 1), jax.random.fold_in(arg_keys[9], 1), 1, CACHE).astype(jnp.int32),
    }


epsilon = 1e-05
rope_base = 500000.0

def rms_gain(values, gain_vector):
    mean_square = lax.optimization_barrier(jnp.mean(values * values, axis=-1, keepdims=True))
    return values * lax.rsqrt(mean_square + epsilon) * gain_vector

def rotate(values, positions):
    half_dim = values.shape[-1] // 2
    index_row = jnp.arange(half_dim, dtype=jnp.float32)
    frequency = jnp.exp(-math.log(rope_base) * index_row / half_dim)
    angle = positions.astype(jnp.float32)[:, None, None] * frequency[None, None, :]
    first_half = values[..., :half_dim]
    second_half = values[..., half_dim:]
    return jnp.concatenate([first_half * jnp.cos(angle) - second_half * jnp.sin(angle), second_half * jnp.cos(angle) + first_half * jnp.sin(angle)], axis=-1)

def reference(hidden, q_weight, k_weight, v_weight, o_weight, input_gain, post_gain, key_cache, value_cache, lengths):
    w_query = q_weight.astype(jnp.bfloat16)
    w_key = k_weight.astype(jnp.bfloat16)
    value_matrix = v_weight.astype(jnp.bfloat16)
    w_out = o_weight.astype(jnp.bfloat16)
    row_count = hidden.shape[0]
    normal_in = rms_gain(hidden.astype(jnp.float32), input_gain).astype(jnp.bfloat16)
    query = jnp.dot(normal_in, w_query, preferred_element_type=jnp.float32)
    key_part = jnp.dot(normal_in, w_key, preferred_element_type=jnp.float32)
    value_part = jnp.dot(normal_in, value_matrix, preferred_element_type=jnp.float32)
    query_b = rotate(query.reshape(row_count, HEADS, HEAD_DIM), lengths).astype(jnp.bfloat16)
    fresh_token_keys = rotate(key_part.reshape(row_count, KV_HEADS, HEAD_DIM), lengths).astype(jnp.bfloat16)
    new_values = value_part.reshape(row_count, KV_HEADS, HEAD_DIM).astype(jnp.bfloat16)
    grouped_heads = query_b.astype(jnp.float32).reshape(row_count, KV_HEADS, GROUP, HEAD_DIM)
    reciprocal_root = 1.0 / math.sqrt(HEAD_DIM)
    scores = jnp.einsum('bkgd,blkd->bkgl', grouped_heads, key_cache.astype(jnp.float32)) * reciprocal_root
    self_token_score = jnp.einsum('lfxa,lfa->lfx', grouped_heads, fresh_token_keys.astype(jnp.float32)) * reciprocal_root
    visible = jnp.arange(CACHE, dtype=jnp.int32)[None, :] < lengths.astype(jnp.int32)[:, None]
    scores = jnp.where(visible[:, None, None, :], scores, -jnp.inf)
    largest = jnp.maximum(lax.optimization_barrier(jnp.max(scores, axis=-1)), self_token_score)
    kept_exp = jnp.exp(scores - largest[..., None])
    own_exp = jnp.exp(self_token_score - largest)
    softmax_divisor = lax.optimization_barrier(jnp.sum(kept_exp, axis=-1)) + own_exp
    weights_kept = (kept_exp / softmax_divisor[..., None]).astype(jnp.bfloat16)
    own_weight = (own_exp / softmax_divisor).astype(jnp.bfloat16)
    attended = jnp.einsum('bkgl,blkd->bkgd', weights_kept.astype(jnp.float32), value_cache.astype(jnp.float32))
    attended = attended + own_weight.astype(jnp.float32)[..., None] * new_values.astype(jnp.float32)[:, :, None, :]
    attended = attended.reshape(row_count, HEADS * HEAD_DIM).astype(jnp.bfloat16)
    mixed = jnp.dot(attended, w_out.T, preferred_element_type=jnp.float32)
    residual = hidden.astype(jnp.float32) + mixed
    new_hidden = residual.astype(jnp.bfloat16)
    normed = rms_gain(residual, post_gain).astype(jnp.bfloat16)
    return (new_hidden, normed, fresh_token_keys, new_values)
```

```python
import functools
import math

import jax
import jax.numpy as jnp
from jax import lax
from jax.experimental import pallas as pl
from jax.experimental.pallas import tpu as pltpu
from jax.sharding import PartitionSpec as P

HEADS = 32
KV_HEADS = 8
HEAD_DIM = 128

CHUNKS = 1

BF = jnp.bfloat16
F32 = jnp.float32

epsilon = 1e-05
rope_base = 500000.0


def rms_gain(values, gain_vector):
    mean_square = jnp.mean(values * values, axis=-1, keepdims=True)
    return values * lax.rsqrt(mean_square + epsilon) * gain_vector


def rotate(values, positions):
    half_dim = values.shape[-1] // 2
    index_row = jnp.arange(half_dim, dtype=jnp.float32)
    frequency = jnp.exp(-math.log(rope_base) * index_row / half_dim)
    angle = positions.astype(jnp.float32)[:, None, None] * frequency[None, None, :]
    first_half = values[..., :half_dim]
    second_half = values[..., half_dim:]
    return jnp.concatenate(
        [
            first_half * jnp.cos(angle) - second_half * jnp.sin(angle),
            second_half * jnp.cos(angle) + first_half * jnp.sin(angle),
        ],
        axis=-1,
    )


def attend(query_b, fresh_token_keys, new_values, key_cache, value_cache, lengths):
    row_count, kv_count = (fresh_token_keys.shape[0], fresh_token_keys.shape[1])
    grouped_heads = query_b.reshape(row_count, kv_count, -1, HEAD_DIM)
    reciprocal_root = 1.0 / math.sqrt(HEAD_DIM)
    scores = (
        jnp.einsum("bkgd,blkd->bkgl", grouped_heads, key_cache, preferred_element_type=jnp.float32)
        * reciprocal_root
    )
    self_token_score = (
        jnp.einsum(
            "lfxa,lfa->lfx", grouped_heads, fresh_token_keys, preferred_element_type=jnp.float32
        )
        * reciprocal_root
    )
    visible = jnp.arange(key_cache.shape[1], dtype=jnp.int32)[None, :] < lengths[:, None]
    scores = jnp.where(visible[:, None, None, :], scores, -jnp.inf)
    largest = jnp.maximum(jnp.max(scores, axis=-1), self_token_score)
    kept_exp = jnp.exp(scores - largest[..., None])
    own_exp = jnp.exp(self_token_score - largest)
    softmax_divisor = jnp.sum(kept_exp, axis=-1) + own_exp
    weights_kept = (kept_exp / softmax_divisor[..., None]).astype(jnp.bfloat16)
    own_weight = (own_exp / softmax_divisor).astype(jnp.bfloat16)
    attended = jnp.einsum(
        "bkgl,blkd->bkgd", weights_kept, value_cache, preferred_element_type=jnp.float32
    )
    attended = (
        attended
        + own_weight.astype(jnp.float32)[..., None] * new_values.astype(jnp.float32)[:, :, None, :]
    )
    return attended.reshape(row_count, -1).astype(jnp.bfloat16)


def swap(x, axis, mask, size):
    return lax.ppermute(x, axis, [(i, i ^ mask) for i in range(size)])


def add(a, b):
    return (a.astype(F32) + b.astype(F32)).astype(BF)


def bits_of(size):
    return [1 << k for k in range(size.bit_length() - 1)]


def scatter_sum(parts, bits, axis, size):
    for b in bits:
        up = sorted(m for m in parts if m & b)
        got = swap(jnp.stack([parts[m] for m in up]), axis, b, size)
        parts = {m: add(parts[m], got[up.index(m | b)]) for m in parts if not m & b}
    return parts[0]


def gather_all(x, bits, axis, size):
    held = {0: x}
    for b in bits:
        keys = sorted(held)
        got = swap(jnp.stack([held[m] for m in keys]), axis, b, size)
        held.update({m | b: got[k] for k, m in enumerate(keys)})
    return held


def norm_pieces_kernel(nd, nt, feat, hidden_ref, gain_ref, *outs):
    me, ten = lax.axis_index("dp"), lax.axis_index("tensor")
    h = hidden_ref[...].astype(F32)
    scale = lax.rsqrt(jnp.mean(h * h, axis=-1, keepdims=True) + epsilon)
    for m in range(nd):
        at = pl.ds(pl.multiple_of(((me ^ m) * nt + ten) * feat, feat), feat)
        outs[m][...] = (hidden_ref[:, at].astype(F32) * scale * gain_ref[:, at]).astype(BF)


def norm_pieces(hidden, gain, nd, nt, feat):
    rows, width = hidden.shape
    if feat % 128:
        me, ten = lax.axis_index("dp"), lax.axis_index("tensor")
        normal_in = rms_gain(hidden.astype(F32), gain).astype(BF)
        return [
            lax.dynamic_slice_in_dim(normal_in, ((me ^ m) * nt + ten) * feat, feat, 1)
            for m in range(nd)
        ]
    tile = min(32, rows)
    return pl.pallas_call(
        functools.partial(norm_pieces_kernel, nd, nt, feat),
        grid=(rows // tile,),
        in_specs=[
            pl.BlockSpec((tile, width), lambda i: (i, 0)),
            pl.BlockSpec((1, width), lambda i: (0, 0)),
        ],
        out_specs=[pl.BlockSpec((tile, feat), lambda i: (i, 0))] * nd,
        out_shape=[jax.ShapeDtypeStruct((rows, feat), BF)] * nd,
        cost_estimate=pl.CostEstimate(flops=rows * width * 20, bytes_accessed=4 * rows * width, transcendentals=0),
    )(hidden, gain.reshape(1, width))


def finish_kernel(nd, nt, feat, masks, hidden_ref, gain_ref, *refs):
    blocks, (new_ref, normed_ref), (res, squares) = refs[: len(masks)], refs[-4:-2], refs[-2:]
    me, ten = lax.axis_index("dp"), lax.axis_index("tensor")
    squares[...] = jnp.zeros_like(squares)
    for ref, group in zip(blocks, masks):
        for k, s in enumerate(group):
            for m in range(nd):
                col = ((me ^ m) * nt + (ten ^ s)) * feat
                at = pl.ds(pl.multiple_of(col, feat), feat)
                r = hidden_ref[:, at].astype(F32) + ref[k, m].astype(F32)
                new_ref[:, at] = r.astype(BF)
                res[:, at] = r
                squares[...] += r * r
    mean = jnp.sum(squares[...], axis=-1, keepdims=True) / res.shape[1]
    normed_ref[...] = (res[...] * lax.rsqrt(mean + epsilon) * gain_ref[...]).astype(BF)


def finish(hidden, gain, first, count, stages, nd, nt, feat, before):
    rows, width = hidden.shape
    tile = min(32, count)
    base = first // tile
    masks = [g for g, _ in stages]
    row = pl.BlockSpec((tile, width), lambda i: (i + base, 0))
    specs = [row, pl.BlockSpec((1, width), lambda i: (0, 0))]
    for g, _ in stages:
        specs.append(pl.BlockSpec((len(g), nd, tile, feat), lambda i: (0, 0, i, 0)))
    args = [hidden, gain.reshape(1, width)] + [x for _, x in stages]
    alias = {}
    if before is not None:
        alias = {len(args): 0, len(args) + 1: 1}
        specs += [pl.BlockSpec(memory_space=pl.ANY)] * 2
        args += list(before)
    return pl.pallas_call(
        functools.partial(finish_kernel, nd, nt, feat, masks),
        grid=(count // tile,),
        in_specs=specs,
        out_specs=[row, row],
        out_shape=[jax.ShapeDtypeStruct((rows, width), BF)] * 2,
        scratch_shapes=[pltpu.VMEM((tile, width), F32), pltpu.VMEM((tile, feat), F32)],
        input_output_aliases=alias,
        cost_estimate=pl.CostEstimate(flops=count * width * 20, bytes_accessed=8 * count * width, transcendentals=0),
    )(*args)


def flip(i, mask):
    for b in (1, 2, 4, 8, 16, 32, 64):
        if mask & b:
            i = i + b - 2 * b * ((i // b) % 2)
    return i


def project_kernel(nd, nt, own_ref, *refs):
    w_refs, (fin, att, prod, zs, zr, ds, dr, ps, pr, fs, fr) = refs[:nt], refs[nt:]
    me, ten = lax.axis_index("dp"), lax.axis_index("tensor")
    rows = own_ref.shape[0]
    half = rows // 2
    evens = list(range(0, nd, 2))
    high, zbits = bits_of(nd)[1:], bits_of(nt)[::-1]
    levels = [[m for m in evens if bin(m).count("1") == k] for k in range(len(high) + 1)]
    pairs = [[n for m in level for n in (m, m + 1)] for level in levels]
    slot = {m: k for k, m in enumerate(m for group in pairs for m in group)}
    orders = (high + [1], high[::-1] + [1])
    started = []

    def send(src, dst, ssem, rsem, where):
        copy = pltpu.make_async_remote_copy(
            src_ref=src, dst_ref=dst, send_sem=ssem, recv_sem=rsem,
            device_id=where, device_id_type=pl.DeviceIdType.MESH,
        )
        copy.start()
        started.append(copy)

    def await_into(dst, sem):
        pltpu.make_async_remote_copy(
            src_ref=dst, dst_ref=dst, send_sem=sem, recv_sem=sem,
            device_id={"dp": me}, device_id_type=pl.DeviceIdType.MESH,
        ).wait_recv()

    barrier = pltpu.get_barrier_semaphore()
    for m in range(1, nd):
        pl.semaphore_signal(
            barrier, inc=1, device_id={"dp": flip(me, m)}, device_id_type=pl.DeviceIdType.MESH
        )
    for b in zbits:
        pl.semaphore_signal(
            barrier, inc=1, device_id={"tensor": flip(ten, b)}, device_id_type=pl.DeviceIdType.MESH
        )
    pl.semaphore_wait(barrier, nd - 1 + len(zbits))

    def block(m, s):
        return own_ref if m == 0 and s == 0 else att.at[s, slot[m]]

    def z_sends(s):
        for b in zbits:
            if b < (s & -s) or s == 0:
                send(block(0, s), att.at[s | b, 0], zs.at[s | b], zr.at[s | b], {"tensor": flip(ten, b)})

    def dp_sends(m, s, h):
        order = orders[h]
        used = [order.index(b) for b in order if m & b]
        for b in order[max(used) + 1 if used else 0 :]:
            part = pl.ds(h * half, half)
            send(
                block(m, s).at[part], att.at[s, slot[m | b], part],
                ds.at[s, m | b, h], dr.at[s, m | b, h], {"dp": flip(me, b)},
            )

    def arrive(m, s, h):
        await_into(att.at[s, slot[m], pl.ds(h * half, half)], dr.at[s, m, h])

    def relay(level, s):
        for h in (0, 1):
            for m in levels[level]:
                arrive(m, s, h)
                dp_sends(m, s, h)

    def multiply(level):
        ms = pairs[level]
        for s in range(nt):
            for m in ms[1::2]:
                for h in (0, 1):
                    arrive(m, s, h)
        first, group, out = slot[ms[0]], len(ms), None
        for s in range(nt):
            lhs = att[s, first : first + group].reshape(group * rows, -1)
            term = jnp.dot(lhs, w_refs[s][...], preferred_element_type=F32)
            out = term if out is None else out + term
        prod[pl.ds(first, group)] = out.astype(BF).reshape(group, rows, -1)
        for m in ms:
            if m:
                send(prod.at[slot[m]], fin.at[0, m], ps.at[m], pr.at[m], {"dp": flip(me, m)})

    def spread(m, s):
        for b in zbits:
            if b < (s & -s) or s == 0:
                send(fin.at[s, m], fin.at[s | b, m], fs.at[s | b, m], fr.at[s | b, m], {"tensor": flip(ten, b)})

    def own_results(ms):
        for m in ms:
            if m:
                await_into(fin.at[0, m], pr.at[m])
                spread(m, 0)

    passing = [s for s in range(1, nt) if (s & -s) > 1][::-1]
    passing.sort(key=lambda s: (bin(s).count("1"), -s))
    ending = [s for s in range(1, nt) if s & 1]

    def pass_on(ms):
        for s in passing:
            for m in ms:
                await_into(fin.at[s, m], fr.at[s, m])
                spread(m, s)

    z_sends(0)
    for h in (0, 1):
        dp_sends(0, 0, h)
    att[0, 0] = own_ref[...]
    walk = [0] + passing + ending
    for k, s in enumerate(walk):
        if s:
            await_into(att.at[s, 0], zr.at[s])
            z_sends(s)
            for h in (0, 1):
                dp_sends(0, s, h)
            if k > 1:
                relay(1, walk[k - 2])

    multiply(0)
    fin[0, 0] = prod[0]
    spread(0, 0)
    own_results(pairs[0])
    for level in range(1, len(levels)):
        for s in walk[max(len(walk) - 2, 0) if level == 1 else 0 : -1]:
            relay(level, s)
        pass_on(pairs[level - 1])
        relay(level, walk[-1])
        multiply(level)
        own_results(pairs[level])
    pass_on(pairs[-1])
    for group in pairs:
        for m in group:
            for s in ending:
                await_into(fin.at[s, m], fr.at[s, m])
    for copy in started:
        copy.wait_send()


def project(attended, w_out, nd, nt, feat):
    rows, qc = attended.shape
    dma = pltpu.SemaphoreType.DMA
    return pl.pallas_call(
        functools.partial(project_kernel, nd, nt),
        in_specs=[pl.BlockSpec(memory_space=pltpu.VMEM)] * (1 + nt),
        out_specs=pl.BlockSpec(memory_space=pltpu.VMEM),
        out_shape=jax.ShapeDtypeStruct((nt, nd, rows, feat), BF),
        scratch_shapes=[
            pltpu.VMEM((nt, nd, rows, qc), BF),
            pltpu.VMEM((nd, rows, feat), BF),
            dma((nt,)), dma((nt,)),
            dma((nt, nd, 2)), dma((nt, nd, 2)),
            dma((nd,)), dma((nd,)),
            dma((nt, nd)), dma((nt, nd)),
        ],
        compiler_params=pltpu.CompilerParams(
            collective_id=1, has_side_effects=True, vmem_limit_bytes=48 * 1024 * 1024
        ),
    )(attended, *w_out)


def shards(
    hidden,
    q_weight,
    k_weight,
    v_weight,
    o_weight,
    input_gain,
    post_gain,
    key_cache,
    value_cache,
    lengths,
):
    nt = lax.axis_size("tensor")
    nd = lax.axis_size("dp")
    me, ten = lax.axis_index("dp"), lax.axis_index("tensor")
    rows, width = hidden.shape
    heads_here, kv_here = HEADS // nt, KV_HEADS // nt
    qc, kc = heads_here * HEAD_DIM, kv_here * HEAD_DIM
    feat = q_weight.shape[0]
    low, high = [1], bits_of(nd)[1:]
    orders = (low + high, low + high[::-1])
    odd = [m for m in range(nd) if m & 1]
    even = [m for m in range(nd) if not m & 1]
    count = rows // CHUNKS

    def columns(w, s, n):
        return lax.dynamic_slice_in_dim(w, (ten ^ s) * n, n, 1).astype(BF)

    pieces = norm_pieces(hidden, input_gain, nd, nt, feat)
    pieces = [swap(p, "dp", m, nd) if m else p for m, p in enumerate(pieces)]
    w_in = [
        jnp.concatenate(
            [columns(q_weight, s, qc), columns(k_weight, s, kc), columns(v_weight, s, kc)], axis=1
        )
        for s in range(nt)
    ]
    w_out = [columns(o_weight, s, qc) for s in range(nt)]
    if feat % 128 == 0:
        w_out = [w.T for w in w_out]

    fresh, values, outs = [], [], None
    for c in range(CHUNKS):
        r0 = c * count
        cut = [p[r0 : r0 + count] for p in pieces]
        lhs_odd = jnp.concatenate([cut[m] for m in odd])
        lhs_even = jnp.concatenate([cut[m] for m in even])
        total, behind = None, []
        for k, s in enumerate(reversed(range(nt))):
            if k and k % 2 == 0:
                held = lax.optimization_barrier((lhs_odd, lhs_even, *behind))
                lhs_odd, lhs_even, behind = held[0], held[1], []
            away = jnp.dot(lhs_odd, w_in[s], preferred_element_type=F32).astype(BF)
            got = swap(away, "dp", 1, nd)
            behind.append(got)
            acc = jnp.dot(lhs_even, w_in[s], preferred_element_type=F32) + got.astype(F32)
            acc = acc.astype(BF).reshape(len(even), count, -1)
            parts = {m: acc[j] for j, m in enumerate(even)}
            part = scatter_sum(parts, orders[k % 2][1:], "dp", nd)
            part = (swap(part, "tensor", s, nt) if s else part).astype(F32)
            total = part if total is None else total + part
        query, key_part, value_part = total[:, :qc], total[:, qc : qc + kc], total[:, qc + kc :]

        here = slice(r0, r0 + count)
        query_b = rotate(query.reshape(count, heads_here, HEAD_DIM), lengths[here]).astype(BF)
        keys = rotate(key_part.reshape(count, kv_here, HEAD_DIM), lengths[here]).astype(BF)
        news = value_part.reshape(count, kv_here, HEAD_DIM).astype(BF)
        fresh.append(keys)
        values.append(news)
        attended = attend(
            query_b, keys, news, key_cache[here], value_cache[here], lengths[here]
        )

        if feat % 128 == 0:
            mine = project(attended, w_out, nd, nt, feat)
            outs = finish(
                hidden, post_gain, r0, count, [(tuple(range(nt)), mine)], nd, nt, feat, outs
            )
            continue
        by_tensor = gather_all(attended, bits_of(nt)[::-1], "tensor", nt)
        product = None
        for k, s in enumerate(sorted(by_tensor, key=lambda s: (s & 1, s))):
            blocks = gather_all(by_tensor[s], orders[k % 2][1:] + low, "dp", nd)
            lhs = jnp.concatenate([blocks[m] for m in range(nd)])
            term = lax.dot_general(
                lhs, w_out[s], (((1,), (1,)), ((), ())), preferred_element_type=F32
            )
            product = term if product is None else product + term
        product = product.astype(BF).reshape(nd, count, feat)
        mine = jnp.stack([swap(product[m], "dp", m, nd) if m else product[0] for m in range(nd)])
        for b in bits_of(nd):
            v = mine.reshape(nd // (2 * b), 2, b, count, feat)
            mine = jnp.where((me & b) != 0, v[:, ::-1], v).reshape(nd, count, feat)
        mine = mine[None]
        for b in bits_of(nt)[::-1]:
            got = swap(mine, "tensor", b, nt)
            first = jnp.where((ten & b) != 0, got, mine)
            second = jnp.where((ten & b) != 0, mine, got)
            mine = jnp.stack([first, second], axis=1).reshape((-1,) + mine.shape[1:])
        mixed = mine.transpose(2, 1, 0, 3).reshape(count, width).astype(F32)
        residual = hidden[here].astype(F32) + mixed
        pair = (residual.astype(BF), rms_gain(residual, post_gain).astype(BF))
        outs = pair if outs is None else tuple(jnp.concatenate(z) for z in zip(outs, pair))
    return (outs[0], outs[1], jnp.concatenate(fresh), jnp.concatenate(values))


def solution(mesh):
    in_specs = (
        P("dp", None),
        P(("dp", "tensor"), None),
        P(("dp", "tensor"), None),
        P(("dp", "tensor"), None),
        P(("dp", "tensor"), None),
        P(),
        P(),
        P("dp", None, "tensor", None),
        P("dp", None, "tensor", None),
        P("dp"),
    )
    out_specs = (P("dp", None), P("dp", None), P("dp", "tensor", None), P("dp", "tensor", None))
    return jax.shard_map(shards, mesh=mesh, in_specs=in_specs, out_specs=out_specs, check_vma=False)
```

```python
import functools
import math

import jax
import jax.numpy as jnp
from jax import lax
from jax.experimental import pallas as pl
from jax.experimental.pallas import tpu as pltpu
from jax.sharding import PartitionSpec as P

HEADS = 32
KV_HEADS = 8
HEAD_DIM = 128

CHUNKS = 1

BF = jnp.bfloat16
F32 = jnp.float32

epsilon = 1e-05
rope_base = 500000.0


def rms_gain(values, gain_vector):
    mean_square = jnp.mean(values * values, axis=-1, keepdims=True)
    return values * lax.rsqrt(mean_square + epsilon) * gain_vector


def rotate(values, positions):
    half_dim = values.shape[-1] // 2
    index_row = jnp.arange(half_dim, dtype=jnp.float32)
    frequency = jnp.exp(-math.log(rope_base) * index_row / half_dim)
    angle = positions.astype(jnp.float32)[:, None, None] * frequency[None, None, :]
    first_half = values[..., :half_dim]
    second_half = values[..., half_dim:]
    return jnp.concatenate(
        [
            first_half * jnp.cos(angle) - second_half * jnp.sin(angle),
            second_half * jnp.cos(angle) + first_half * jnp.sin(angle),
        ],
        axis=-1,
    )


def attend(query_b, fresh_token_keys, new_values, key_cache, value_cache, lengths):
    row_count, kv_count = (fresh_token_keys.shape[0], fresh_token_keys.shape[1])
    grouped_heads = query_b.reshape(row_count, kv_count, -1, HEAD_DIM)
    reciprocal_root = 1.0 / math.sqrt(HEAD_DIM)
    scores = (
        jnp.einsum("bkgd,blkd->bkgl", grouped_heads, key_cache, preferred_element_type=jnp.float32)
        * reciprocal_root
    )
    self_token_score = (
        jnp.einsum(
            "lfxa,lfa->lfx", grouped_heads, fresh_token_keys, preferred_element_type=jnp.float32
        )
        * reciprocal_root
    )
    visible = jnp.arange(key_cache.shape[1], dtype=jnp.int32)[None, :] < lengths[:, None]
    scores = jnp.where(visible[:, None, None, :], scores, -jnp.inf)
    largest = jnp.maximum(jnp.max(scores, axis=-1), self_token_score)
    kept_exp = jnp.exp(scores - largest[..., None])
    own_exp = jnp.exp(self_token_score - largest)
    softmax_divisor = jnp.sum(kept_exp, axis=-1) + own_exp
    weights_kept = (kept_exp / softmax_divisor[..., None]).astype(jnp.bfloat16)
    own_weight = (own_exp / softmax_divisor).astype(jnp.bfloat16)
    attended = jnp.einsum(
        "bkgl,blkd->bkgd", weights_kept, value_cache, preferred_element_type=jnp.float32
    )
    attended = (
        attended
        + own_weight.astype(jnp.float32)[..., None] * new_values.astype(jnp.float32)[:, :, None, :]
    )
    return attended.reshape(row_count, -1).astype(jnp.bfloat16)


def swap(x, axis, mask, size):
    return lax.ppermute(x, axis, [(i, i ^ mask) for i in range(size)])


def add(a, b):
    return (a.astype(F32) + b.astype(F32)).astype(BF)


def bits_of(size):
    return [1 << k for k in range(size.bit_length() - 1)]


def scatter_sum(parts, bits, axis, size):
    for b in bits:
        up = sorted(m for m in parts if m & b)
        got = swap(jnp.stack([parts[m] for m in up]), axis, b, size)
        parts = {m: add(parts[m], got[up.index(m | b)]) for m in parts if not m & b}
    return parts[0]


def gather_all(x, bits, axis, size):
    held = {0: x}
    for b in bits:
        keys = sorted(held)
        got = swap(jnp.stack([held[m] for m in keys]), axis, b, size)
        held.update({m | b: got[k] for k, m in enumerate(keys)})
    return held


def norm_pieces_kernel(nd, nt, feat, hidden_ref, gain_ref, *outs):
    me, ten = lax.axis_index("dp"), lax.axis_index("tensor")
    h = hidden_ref[...].astype(F32)
    scale = lax.rsqrt(jnp.mean(h * h, axis=-1, keepdims=True) + epsilon)
    for m in range(nd):
        at = pl.ds(pl.multiple_of(((me ^ m) * nt + ten) * feat, feat), feat)
        outs[m][...] = (hidden_ref[:, at].astype(F32) * scale * gain_ref[:, at]).astype(BF)


def norm_pieces(hidden, gain, nd, nt, feat):
    rows, width = hidden.shape
    if feat % 128:
        me, ten = lax.axis_index("dp"), lax.axis_index("tensor")
        normal_in = rms_gain(hidden.astype(F32), gain).astype(BF)
        return [
            lax.dynamic_slice_in_dim(normal_in, ((me ^ m) * nt + ten) * feat, feat, 1)
            for m in range(nd)
        ]
    tile = min(32, rows)
    return pl.pallas_call(
        functools.partial(norm_pieces_kernel, nd, nt, feat),
        grid=(rows // tile,),
        in_specs=[
            pl.BlockSpec((tile, width), lambda i: (i, 0)),
            pl.BlockSpec((1, width), lambda i: (0, 0)),
        ],
        out_specs=[pl.BlockSpec((tile, feat), lambda i: (i, 0))] * nd,
        out_shape=[jax.ShapeDtypeStruct((rows, feat), BF)] * nd,
        cost_estimate=pl.CostEstimate(flops=rows * width * 20, bytes_accessed=4 * rows * width, transcendentals=0),
    )(hidden, gain.reshape(1, width))


def finish_kernel(nd, nt, feat, masks, hidden_ref, gain_ref, *refs):
    blocks, (new_ref, normed_ref), (res, squares) = refs[: len(masks)], refs[-4:-2], refs[-2:]
    me, ten = lax.axis_index("dp"), lax.axis_index("tensor")
    squares[...] = jnp.zeros_like(squares)
    for ref, group in zip(blocks, masks):
        for k, s in enumerate(group):
            for m in range(nd):
                col = ((me ^ m) * nt + (ten ^ s)) * feat
                at = pl.ds(pl.multiple_of(col, feat), feat)
                r = hidden_ref[:, at].astype(F32) + ref[k, m].astype(F32)
                new_ref[:, at] = r.astype(BF)
                res[:, at] = r
                squares[...] += r * r
    mean = jnp.sum(squares[...], axis=-1, keepdims=True) / res.shape[1]
    normed_ref[...] = (res[...] * lax.rsqrt(mean + epsilon) * gain_ref[...]).astype(BF)


def finish(hidden, gain, first, count, stages, nd, nt, feat, before):
    rows, width = hidden.shape
    tile = min(32, count)
    base = first // tile
    masks = [g for g, _ in stages]
    row = pl.BlockSpec((tile, width), lambda i: (i + base, 0))
    specs = [row, pl.BlockSpec((1, width), lambda i: (0, 0))]
    for g, _ in stages:
        specs.append(pl.BlockSpec((len(g), nd, tile, feat), lambda i: (0, 0, i, 0)))
    args = [hidden, gain.reshape(1, width)] + [x for _, x in stages]
    alias = {}
    if before is not None:
        alias = {len(args): 0, len(args) + 1: 1}
        specs += [pl.BlockSpec(memory_space=pl.ANY)] * 2
        args += list(before)
    return pl.pallas_call(
        functools.partial(finish_kernel, nd, nt, feat, masks),
        grid=(count // tile,),
        in_specs=specs,
        out_specs=[row, row],
        out_shape=[jax.ShapeDtypeStruct((rows, width), BF)] * 2,
        scratch_shapes=[pltpu.VMEM((tile, width), F32), pltpu.VMEM((tile, feat), F32)],
        input_output_aliases=alias,
        cost_estimate=pl.CostEstimate(flops=count * width * 20, bytes_accessed=8 * count * width, transcendentals=0),
    )(*args)


def flip(i, mask):
    for b in (1, 2, 4, 8, 16, 32, 64):
        if mask & b:
            i = i + b - 2 * b * ((i // b) % 2)
    return i


def inputs_kernel(nd, nt, hidden_ref, gain_ref, q_ref, k_ref, v_ref, out_ref, *scratch):
    wf, wsend, w2, araw, an, srow, sall, even, away, gotc = scratch[:10]
    hops = bits_of(nd)[1:]
    H = len(hops)
    snd, rcv = scratch[10 : 10 + H], scratch[10 + H : 10 + 2 * H]
    zsnd, zrcv, ls, ws, wr, as_, ar, ss, sr, cs, cr, hs, hr, zs, zr = scratch[10 + 2 * H :]
    me, ten = lax.axis_index("dp"), lax.axis_index("tensor")
    rows, width = hidden_ref.shape
    feat = q_ref.shape[0]
    wide = w2.shape[-1]
    qc, kc = q_ref.shape[1] // nt, k_ref.shape[1] // nt
    keep = list(range(0, nt, 2))[::-1]
    spans = [(q_ref, qc, j) for j in range(qc // wide)]
    spans += [(w, kc, j) for w in (k_ref, v_ref) for j in range(kc // wide)]
    chunks = [(s, n) for s in keep for n in range(len(spans))]
    evens = list(range(0, nd, 2))
    orders = (hops, hops[::-1])
    started = []

    def send(src, dst, ssem, rsem, where):
        copy = pltpu.make_async_remote_copy(
            src_ref=src, dst_ref=dst, send_sem=ssem, recv_sem=rsem,
            device_id=where, device_id_type=pl.DeviceIdType.MESH,
        )
        copy.start()
        started.append(copy)

    def await_into(dst, sem):
        pltpu.make_async_remote_copy(
            src_ref=dst, dst_ref=dst, send_sem=sem, recv_sem=sem,
            device_id={"dp": me}, device_id_type=pl.DeviceIdType.MESH,
        ).wait_recv()

    def load(c, e):
        s, n = chunks[c]
        ref, size, j = spans[n]
        at = pl.ds(pl.multiple_of(flip(ten, s | e) * size + j * wide, wide), wide)
        return pltpu.make_async_copy(ref.at[:, at], wf.at[e, c], ls.at[e, c])

    for e in (1, 0):
        for c in range(len(chunks)):
            load(c, e).start()

    peers = [1] + [s for s in keep if s]
    barrier = pltpu.get_barrier_semaphore()
    for m in range(1, nd):
        pl.semaphore_signal(
            barrier, inc=1, device_id={"dp": flip(me, m)}, device_id_type=pl.DeviceIdType.MESH
        )
    for b in peers:
        pl.semaphore_signal(
            barrier, inc=1, device_id={"tensor": flip(ten, b)}, device_id_type=pl.DeviceIdType.MESH
        )
    pl.semaphore_wait(barrier, nd - 1 + len(peers))

    def features(m, e):
        return pl.ds(pl.multiple_of((flip(me, m) * nt + flip(ten, e)) * feat, feat), feat)

    far_first = sorted(range(1, nd), key=lambda m: (-bin(m >> 1).count("1"), m))
    for m in far_first:
        for e in (0, 1):
            send(
                hidden_ref.at[:, features(m, e)], araw.at[m, e],
                as_.at[m, e], ar.at[m, e], {"dp": flip(me, m)},
            )
    for c in range(len(chunks)):
        load(c, 1).wait()
        wsend[c] = wf[1, c].astype(BF)
        send(wsend.at[c], w2.at[c, 1], ws.at[c], wr.at[c], {"tensor": flip(ten, 1)})

    step = 512

    def squares(i, acc):
        h = hidden_ref[:, pl.ds(pl.multiple_of(i * step, step), step)].astype(F32)
        h = h * h
        for j in range(0, step, 128):
            acc = acc + h[:, j : j + 128]
        return acc

    acc = lax.fori_loop(0, width // step, squares, jnp.zeros((rows, 128), F32))
    scale = lax.rsqrt(jnp.sum(acc, axis=-1, keepdims=True) / width + epsilon)
    scale = jnp.broadcast_to(scale, (rows, 128))
    srow[...] = scale.T[:8]
    for m in far_first:
        send(srow, sall.at[m], ss.at[m], sr.at[m], {"dp": flip(me, m)})
    for c in range(len(chunks)):
        load(c, 0).wait()
        w2[c, 0] = wf[0, c].astype(BF)

    def normalise(raw, scale, e):
        out = []
        for j in range(0, feat, 128):
            at = pl.ds(pl.multiple_of((me * nt + flip(ten, e)) * feat + j, 128), 128)
            out.append((raw[:, j : j + 128].astype(F32) * scale * gain_ref[:, at]).astype(BF))
        return jnp.concatenate(out, axis=1)

    for e in (0, 1):
        an[e, 0, 0] = normalise(hidden_ref[:, features(0, e)], scale, e)
    for m in range(1, nd):
        await_into(sall.at[m], sr.at[m])
        other = jnp.broadcast_to(sall[m][:1], (128, rows)).T
        for e in (0, 1):
            await_into(araw.at[m, e], ar.at[m, e])
            an[e, m % 2, m // 2] = normalise(araw[m, e], other, e)

    def place(c):
        order = orders[c % 2]
        return [sum(b for i, b in enumerate(order) if p >> (H - 1 - i) & 1) for p in range(len(evens))]

    def product(c, odd):
        out = None
        for e in (0, 1):
            lhs = an[e, odd].reshape(len(evens) * rows, feat)
            term = jnp.dot(lhs, w2[c, e], preferred_element_type=F32)
            out = term if out is None else out + term
        return out.reshape(len(evens), rows, wide)

    def begin(c):
        await_into(w2.at[c, 1], wr.at[c])
        out = product(c, 1).astype(BF)
        for p, m in enumerate(place(c)):
            away[c, p] = out[m // 2]
        send(away.at[c], gotc.at[c], cs.at[c], cr.at[c], {"dp": flip(me, 1)})
        out = product(c, 0)
        for p, m in enumerate(place(c)):
            even[c, p] = out[m // 2]

    def hop(c, l):
        g = len(evens) >> l
        if l == 0:
            await_into(gotc.at[c], cr.at[c])
            got = gotc[c]
        else:
            await_into(rcv[l - 1].at[c], hr.at[c, l - 1])
            got = rcv[l - 1][c]
        if l < H:
            g //= 2
            even[c, :g] = even[c, :g] + got[:g].astype(F32)
            snd[l][c] = (even[c, g : 2 * g] + got[g:].astype(F32)).astype(BF)
            bit = orders[c % 2][l]
            send(snd[l].at[c], rcv[l].at[c], hs.at[c, l], hr.at[c, l], {"dp": flip(me, bit)})
            return
        done = even[c, 0] + got[0].astype(F32)
        s, n = chunks[c]
        if s:
            zsnd[c] = done.astype(BF)
            send(zsnd.at[c], zrcv.at[c], zs.at[c], zr.at[c], {"tensor": flip(ten, s)})
        else:
            out_ref[:, n * wide : (n + 1) * wide] = done

    lags = [1 + 2 * l for l in range(H + 1)]
    for i in range(len(chunks) + lags[-1]):
        for l in range(H, -1, -1):
            c = i - lags[l]
            if 0 <= c < len(chunks):
                hop(c, l)
        if i < len(chunks):
            begin(i)
    for c, (s, n) in enumerate(chunks):
        if s:
            await_into(zrcv.at[c], zr.at[c])
            out_ref[:, n * wide : (n + 1) * wide] += zrcv[c].astype(F32)
    for copy in started:
        copy.wait_send()


def inputs(hidden, gain, q_weight, k_weight, v_weight, nd, nt):
    rows, width = hidden.shape
    feat, wide = q_weight.shape[0], 256
    columns = (q_weight.shape[1] + 2 * k_weight.shape[1]) // nt
    C, half, H = columns // wide * (nt // 2), nd // 2, nd.bit_length() - 2
    dma, vm = pltpu.SemaphoreType.DMA, pltpu.VMEM
    hop_bufs = [vm((C, half >> (l + 1), rows, wide), BF) for l in range(H)]
    place = pl.BlockSpec(memory_space=pltpu.VMEM)
    return pl.pallas_call(
        functools.partial(inputs_kernel, nd, nt),
        in_specs=[place, place] + [pl.BlockSpec(memory_space=pl.ANY)] * 3,
        out_specs=place,
        out_shape=jax.ShapeDtypeStruct((rows, columns), F32),
        scratch_shapes=[
            vm((2, C, feat, wide), F32),
            vm((C, feat, wide), BF),
            vm((C, 2, feat, wide), BF),
            vm((nd, 2, rows, feat), BF),
            vm((2, 2, half, rows, feat), BF),
            vm((8, rows), F32),
            vm((nd, 8, rows), F32),
            vm((C, half, rows, wide), F32),
            vm((C, half, rows, wide), BF),
            vm((C, half, rows, wide), BF),
            *hop_bufs,
            *hop_bufs,
            vm((C, rows, wide), BF),
            vm((C, rows, wide), BF),
            dma((2, C)),
            dma((C,)), dma((C,)),
            dma((nd, 2)), dma((nd, 2)),
            dma((nd,)), dma((nd,)),
            dma((C,)), dma((C,)),
            dma((C, H)), dma((C, H)),
            dma((C,)), dma((C,)),
        ],
        compiler_params=pltpu.CompilerParams(
            collective_id=2, has_side_effects=True, vmem_limit_bytes=56 * 1024 * 1024
        ),
    )(hidden, gain.reshape(1, width), q_weight, k_weight, v_weight)


def project_kernel(nd, nt, own_ref, w_ref, fin, att, prod, wf, wt, acc, ls, zs, zr, ds, dr, ps, pr, fs, fr):
    me, ten = lax.axis_index("dp"), lax.axis_index("tensor")
    rows, qc = own_ref.shape
    half = rows // 2
    evens = list(range(0, nd, 2))
    high, zbits = bits_of(nd)[1:], bits_of(nt)[::-1]
    levels = [[m for m in evens if bin(m).count("1") == k] for k in range(len(high) + 1)]
    pairs = [[n for m in level for n in (m, m + 1)] for level in levels]
    slot = {m: k for k, m in enumerate(m for group in pairs for m in group)}
    orders = (high + [1], high[::-1] + [1])
    waves = [[s for s in range(nt) if bin(s).count("1") == k][::-1] for k in range(1, len(zbits) + 1)]
    walk = [0] + [s for wave in waves for s in wave]
    started = []

    def send(src, dst, ssem, rsem, where):
        copy = pltpu.make_async_remote_copy(
            src_ref=src, dst_ref=dst, send_sem=ssem, recv_sem=rsem,
            device_id=where, device_id_type=pl.DeviceIdType.MESH,
        )
        copy.start()
        started.append(copy)

    def await_into(dst, sem):
        pltpu.make_async_remote_copy(
            src_ref=dst, dst_ref=dst, send_sem=sem, recv_sem=sem,
            device_id={"dp": me}, device_id_type=pl.DeviceIdType.MESH,
        ).wait_recv()

    def load(s):
        at = pl.ds(pl.multiple_of(flip(ten, s) * qc, qc), qc)
        return pltpu.make_async_copy(w_ref.at[:, at], wf.at[s], ls.at[s])

    for s in walk:
        load(s).start()
    barrier = pltpu.get_barrier_semaphore()
    for m in range(1, nd):
        pl.semaphore_signal(
            barrier, inc=1, device_id={"dp": flip(me, m)}, device_id_type=pl.DeviceIdType.MESH
        )
    for b in zbits:
        pl.semaphore_signal(
            barrier, inc=1, device_id={"tensor": flip(ten, b)}, device_id_type=pl.DeviceIdType.MESH
        )
    pl.semaphore_wait(barrier, nd - 1 + len(zbits))

    def block(m, s):
        return own_ref if m == 0 and s == 0 else att.at[s, slot[m]]

    def z_sends(s, h):
        part = pl.ds(h * half, half)
        for b in zbits:
            if b < (s & -s) or s == 0:
                send(
                    block(0, s).at[part], att.at[s | b, 0, part],
                    zs.at[s | b, h], zr.at[s | b, h], {"tensor": flip(ten, b)},
                )

    def dp_sends(m, s, h, bits):
        order = orders[h]
        used = [order.index(b) for b in order if m & b]
        for b in order[max(used) + 1 if used else 0 :]:
            if b in bits:
                part = pl.ds(h * half, half)
                send(
                    block(m, s).at[part], att.at[s, slot[m | b], part],
                    ds.at[s, m | b, h], dr.at[s, m | b, h], {"dp": flip(me, b)},
                )

    def arrive(m, s, h):
        await_into(att.at[s, slot[m], pl.ds(h * half, half)], dr.at[s, m, h])

    def near(level, s):
        for h in (0, 1):
            for m in levels[level]:
                arrive(m, s, h)
                dp_sends(m, s, h, [1])

    def far(level, s):
        for h in (0, 1):
            for m in levels[level]:
                dp_sends(m, s, h, high)

    def relay(level, s):
        near(level, s)
        far(level, s)

    def partial(level, s):
        ms = pairs[level]
        for m in ms[1::2]:
            for h in (0, 1):
                arrive(m, s, h)
        first, group = slot[ms[0]], len(ms)
        lhs = att[s, first : first + group].reshape(group * rows, -1)
        term = jnp.dot(lhs, wt[s], preferred_element_type=F32)
        if s == 0:
            acc[: group * rows] = term
        elif s != walk[-1]:
            acc[: group * rows] += term
        else:
            out = acc[: group * rows] + term
            prod[pl.ds(first, group)] = out.astype(BF).reshape(group, rows, -1)
            for m in ms:
                if m:
                    send(prod.at[slot[m]], fin.at[0, m], ps.at[m], pr.at[m], {"dp": flip(me, m)})

    def spread(m, s):
        for b in zbits:
            if b < (s & -s) or s == 0:
                send(fin.at[s, m], fin.at[s | b, m], fs.at[s | b, m], fr.at[s | b, m], {"tensor": flip(ten, b)})

    def own_results(ms):
        for m in ms:
            if m:
                await_into(fin.at[0, m], pr.at[m])
                spread(m, 0)

    passing = [s for s in walk[1:] if not s & 1]
    ending = [s for s in range(1, nt) if s & 1]

    def pass_on(ms):
        for s in passing:
            for m in ms:
                await_into(fin.at[s, m], fr.at[s, m])
                spread(m, s)

    for h in (0, 1):
        z_sends(0, h)
    for h in (0, 1):
        dp_sends(0, 0, h, high + [1])
    att[0, 0] = own_ref[...]
    for s in walk:
        load(s).wait()
        wt[s] = wf[s].T.astype(BF)
    waiting = list(walk)
    for wave in waves:
        for h in (0, 1):
            for s in wave:
                await_into(att.at[s, 0, pl.ds(h * half, half)], zr.at[s, h])
                z_sends(s, h)
                dp_sends(0, s, h, high + [1])
            if h == 0:
                relay(1, waiting.pop(0))

    for s in walk:
        partial(0, s)
    fin[0, 0] = prod[0]
    spread(0, 0)
    own_results(pairs[0])
    for level in range(1, len(levels)):
        for s in waiting[:-1]:
            relay(level, s)
        for s in walk[:-1]:
            partial(level, s)
        pass_on(pairs[level - 1])
        near(level, walk[-1])
        partial(level, walk[-1])
        far(level, walk[-1])
        own_results(pairs[level])
        waiting = list(walk)
    pass_on(pairs[-1])
    for group in pairs:
        for m in group:
            for s in ending:
                await_into(fin.at[s, m], fr.at[s, m])
    for copy in started:
        copy.wait_send()


def project(attended, o_weight, nd, nt, feat):
    rows, qc = attended.shape
    dma = pltpu.SemaphoreType.DMA
    return pl.pallas_call(
        functools.partial(project_kernel, nd, nt),
        in_specs=[pl.BlockSpec(memory_space=pltpu.VMEM), pl.BlockSpec(memory_space=pl.ANY)],
        out_specs=pl.BlockSpec(memory_space=pltpu.VMEM),
        out_shape=jax.ShapeDtypeStruct((nt, nd, rows, feat), BF),
        scratch_shapes=[
            pltpu.VMEM((nt, nd, rows, qc), BF),
            pltpu.VMEM((nd, rows, feat), BF),
            pltpu.VMEM((nt, feat, qc), F32),
            pltpu.VMEM((nt, qc, feat), BF),
            pltpu.VMEM((nd * rows, feat), F32),
            dma((nt,)),
            dma((nt, 2)), dma((nt, 2)),
            dma((nt, nd, 2)), dma((nt, nd, 2)),
            dma((nd,)), dma((nd,)),
            dma((nt, nd)), dma((nt, nd)),
        ],
        compiler_params=pltpu.CompilerParams(
            collective_id=1, has_side_effects=True, vmem_limit_bytes=48 * 1024 * 1024
        ),
    )(attended, o_weight)


def shards(
    hidden,
    q_weight,
    k_weight,
    v_weight,
    o_weight,
    input_gain,
    post_gain,
    key_cache,
    value_cache,
    lengths,
):
    nt = lax.axis_size("tensor")
    nd = lax.axis_size("dp")
    me, ten = lax.axis_index("dp"), lax.axis_index("tensor")
    rows, width = hidden.shape
    heads_here, kv_here = HEADS // nt, KV_HEADS // nt
    qc, kc = heads_here * HEAD_DIM, kv_here * HEAD_DIM
    feat = q_weight.shape[0]
    low, high = [1], bits_of(nd)[1:]
    orders = (low + high, low + high[::-1])
    odd = [m for m in range(nd) if m & 1]
    even = [m for m in range(nd) if not m & 1]
    count = rows // CHUNKS

    def columns(w, s, n):
        return lax.dynamic_slice_in_dim(w, (ten ^ s) * n, n, 1).astype(BF)

    together = feat % 128 == 0 and kc % 256 == 0 and rows == 128 and nt > 1 and nd > 2 and CHUNKS == 1
    if not together:
        pieces = norm_pieces(hidden, input_gain, nd, nt, feat)
        pieces = [swap(p, "dp", m, nd) if m else p for m, p in enumerate(pieces)]
        w_in = [
            jnp.concatenate(
                [columns(q_weight, s, qc), columns(k_weight, s, kc), columns(v_weight, s, kc)], axis=1
            )
            for s in range(nt)
        ]
    w_out = [columns(o_weight, s, qc) for s in range(nt)]

    fresh, values, outs = [], [], None
    for c in range(CHUNKS):
        r0 = c * count
        if together:
            total = inputs(hidden, input_gain, q_weight, k_weight, v_weight, nd, nt)
        else:
            cut = [p[r0 : r0 + count] for p in pieces]
            lhs_odd = jnp.concatenate([cut[m] for m in odd])
            lhs_even = jnp.concatenate([cut[m] for m in even])
            total, behind = None, []
            for k, s in enumerate(reversed(range(nt))):
                if k and k % 2 == 0:
                    held = lax.optimization_barrier((lhs_odd, lhs_even, *behind))
                    lhs_odd, lhs_even, behind = held[0], held[1], []
                away = jnp.dot(lhs_odd, w_in[s], preferred_element_type=F32).astype(BF)
                got = swap(away, "dp", 1, nd)
                behind.append(got)
                acc = jnp.dot(lhs_even, w_in[s], preferred_element_type=F32) + got.astype(F32)
                acc = acc.astype(BF).reshape(len(even), count, -1)
                parts = {m: acc[j] for j, m in enumerate(even)}
                part = scatter_sum(parts, orders[k % 2][1:], "dp", nd)
                part = (swap(part, "tensor", s, nt) if s else part).astype(F32)
                total = part if total is None else total + part
        query, key_part, value_part = total[:, :qc], total[:, qc : qc + kc], total[:, qc + kc :]

        here = slice(r0, r0 + count)
        query_b = rotate(query.reshape(count, heads_here, HEAD_DIM), lengths[here]).astype(BF)
        keys = rotate(key_part.reshape(count, kv_here, HEAD_DIM), lengths[here]).astype(BF)
        news = value_part.reshape(count, kv_here, HEAD_DIM).astype(BF)
        fresh.append(keys)
        values.append(news)
        attended = attend(
            query_b, keys, news, key_cache[here], value_cache[here], lengths[here]
        )

        if feat % 128 == 0:
            mine = project(attended, o_weight, nd, nt, feat)
            outs = finish(
                hidden, post_gain, r0, count, [(tuple(range(nt)), mine)], nd, nt, feat, outs
            )
            continue
        by_tensor = gather_all(attended, bits_of(nt)[::-1], "tensor", nt)
        product = None
        for k, s in enumerate(sorted(by_tensor, key=lambda s: (s & 1, s))):
            blocks = gather_all(by_tensor[s], orders[k % 2][1:] + low, "dp", nd)
            lhs = jnp.concatenate([blocks[m] for m in range(nd)])
            term = lax.dot_general(
                lhs, w_out[s], (((1,), (1,)), ((), ())), preferred_element_type=F32
            )
            product = term if product is None else product + term
        product = product.astype(BF).reshape(nd, count, feat)
        mine = jnp.stack([swap(product[m], "dp", m, nd) if m else product[0] for m in range(nd)])
        for b in bits_of(nd):
            v = mine.reshape(nd // (2 * b), 2, b, count, feat)
            mine = jnp.where((me & b) != 0, v[:, ::-1], v).reshape(nd, count, feat)
        mine = mine[None]
        for b in bits_of(nt)[::-1]:
            got = swap(mine, "tensor", b, nt)
            first = jnp.where((ten & b) != 0, got, mine)
            second = jnp.where((ten & b) != 0, mine, got)
            mine = jnp.stack([first, second], axis=1).reshape((-1,) + mine.shape[1:])
        mixed = mine.transpose(2, 1, 0, 3).reshape(count, width).astype(F32)
        residual = hidden[here].astype(F32) + mixed
        pair = (residual.astype(BF), rms_gain(residual, post_gain).astype(BF))
        outs = pair if outs is None else tuple(jnp.concatenate(z) for z in zip(outs, pair))
    return (outs[0], outs[1], jnp.concatenate(fresh), jnp.concatenate(values))


def solution(mesh):
    in_specs = (
        P("dp", None),
        P(("dp", "tensor"), None),
        P(("dp", "tensor"), None),
        P(("dp", "tensor"), None),
        P(("dp", "tensor"), None),
        P(),
        P(),
        P("dp", None, "tensor", None),
        P("dp", None, "tensor", None),
        P("dp"),
    )
    out_specs = (P("dp", None), P("dp", None), P("dp", "tensor", None), P("dp", "tensor", None))
    return jax.shard_map(shards, mesh=mesh, in_specs=in_specs, out_specs=out_specs, check_vma=False)
```

```python
import functools
import math

import jax
import jax.numpy as jnp
from jax import lax
from jax.experimental import pallas as pl
from jax.experimental.pallas import tpu as pltpu
from jax.sharding import PartitionSpec as P

HEADS = 32
KV_HEADS = 8
HEAD_DIM = 128

CHUNKS = 1

BF = jnp.bfloat16
F32 = jnp.float32

epsilon = 1e-05
rope_base = 500000.0


def rms_gain(values, gain_vector):
    mean_square = jnp.mean(values * values, axis=-1, keepdims=True)
    return values * lax.rsqrt(mean_square + epsilon) * gain_vector


def rotate(values, positions):
    half_dim = values.shape[-1] // 2
    index_row = jnp.arange(half_dim, dtype=jnp.float32)
    frequency = jnp.exp(-math.log(rope_base) * index_row / half_dim)
    angle = positions.astype(jnp.float32)[:, None, None] * frequency[None, None, :]
    first_half = values[..., :half_dim]
    second_half = values[..., half_dim:]
    return jnp.concatenate(
        [
            first_half * jnp.cos(angle) - second_half * jnp.sin(angle),
            second_half * jnp.cos(angle) + first_half * jnp.sin(angle),
        ],
        axis=-1,
    )


def attend(query_b, fresh_token_keys, new_values, key_cache, value_cache, lengths):
    row_count, kv_count = (fresh_token_keys.shape[0], fresh_token_keys.shape[1])
    grouped_heads = query_b.reshape(row_count, kv_count, -1, HEAD_DIM)
    reciprocal_root = 1.0 / math.sqrt(HEAD_DIM)
    scores = (
        jnp.einsum("bkgd,blkd->bkgl", grouped_heads, key_cache, preferred_element_type=jnp.float32)
        * reciprocal_root
    )
    self_token_score = (
        jnp.einsum(
            "lfxa,lfa->lfx", grouped_heads, fresh_token_keys, preferred_element_type=jnp.float32
        )
        * reciprocal_root
    )
    visible = jnp.arange(key_cache.shape[1], dtype=jnp.int32)[None, :] < lengths[:, None]
    scores = jnp.where(visible[:, None, None, :], scores, -jnp.inf)
    largest = jnp.maximum(jnp.max(scores, axis=-1), self_token_score)
    kept_exp = jnp.exp(scores - largest[..., None])
    own_exp = jnp.exp(self_token_score - largest)
    softmax_divisor = jnp.sum(kept_exp, axis=-1) + own_exp
    weights_kept = (kept_exp / softmax_divisor[..., None]).astype(jnp.bfloat16)
    own_weight = (own_exp / softmax_divisor).astype(jnp.bfloat16)
    attended = jnp.einsum(
        "bkgl,blkd->bkgd", weights_kept, value_cache, preferred_element_type=jnp.float32
    )
    attended = (
        attended
        + own_weight.astype(jnp.float32)[..., None] * new_values.astype(jnp.float32)[:, :, None, :]
    )
    return attended.reshape(row_count, -1).astype(jnp.bfloat16)


def swap(x, axis, mask, size):
    return lax.ppermute(x, axis, [(i, i ^ mask) for i in range(size)])


def add(a, b):
    return (a.astype(F32) + b.astype(F32)).astype(BF)


def bits_of(size):
    return [1 << k for k in range(size.bit_length() - 1)]


def scatter_sum(parts, bits, axis, size):
    for b in bits:
        up = sorted(m for m in parts if m & b)
        got = swap(jnp.stack([parts[m] for m in up]), axis, b, size)
        parts = {m: add(parts[m], got[up.index(m | b)]) for m in parts if not m & b}
    return parts[0]


def gather_all(x, bits, axis, size):
    held = {0: x}
    for b in bits:
        keys = sorted(held)
        got = swap(jnp.stack([held[m] for m in keys]), axis, b, size)
        held.update({m | b: got[k] for k, m in enumerate(keys)})
    return held


def norm_pieces_kernel(nd, nt, feat, hidden_ref, gain_ref, *outs):
    me, ten = lax.axis_index("dp"), lax.axis_index("tensor")
    h = hidden_ref[...].astype(F32)
    scale = lax.rsqrt(jnp.mean(h * h, axis=-1, keepdims=True) + epsilon)
    for m in range(nd):
        at = pl.ds(pl.multiple_of(((me ^ m) * nt + ten) * feat, feat), feat)
        outs[m][...] = (hidden_ref[:, at].astype(F32) * scale * gain_ref[:, at]).astype(BF)


def norm_pieces(hidden, gain, nd, nt, feat):
    rows, width = hidden.shape
    if feat % 128:
        me, ten = lax.axis_index("dp"), lax.axis_index("tensor")
        normal_in = rms_gain(hidden.astype(F32), gain).astype(BF)
        return [
            lax.dynamic_slice_in_dim(normal_in, ((me ^ m) * nt + ten) * feat, feat, 1)
            for m in range(nd)
        ]
    tile = min(32, rows)
    return pl.pallas_call(
        functools.partial(norm_pieces_kernel, nd, nt, feat),
        grid=(rows // tile,),
        in_specs=[
            pl.BlockSpec((tile, width), lambda i: (i, 0)),
            pl.BlockSpec((1, width), lambda i: (0, 0)),
        ],
        out_specs=[pl.BlockSpec((tile, feat), lambda i: (i, 0))] * nd,
        out_shape=[jax.ShapeDtypeStruct((rows, feat), BF)] * nd,
        cost_estimate=pl.CostEstimate(flops=rows * width * 20, bytes_accessed=4 * rows * width, transcendentals=0),
    )(hidden, gain.reshape(1, width))


def finish_kernel(nd, nt, feat, masks, hidden_ref, gain_ref, *refs):
    blocks, (new_ref, normed_ref), (res, squares) = refs[: len(masks)], refs[-4:-2], refs[-2:]
    me, ten = lax.axis_index("dp"), lax.axis_index("tensor")
    squares[...] = jnp.zeros_like(squares)
    for ref, group in zip(blocks, masks):
        for k, s in enumerate(group):
            for m in range(nd):
                col = ((me ^ m) * nt + (ten ^ s)) * feat
                at = pl.ds(pl.multiple_of(col, feat), feat)
                r = hidden_ref[:, at].astype(F32) + ref[k, m].astype(F32)
                new_ref[:, at] = r.astype(BF)
                res[:, at] = r
                squares[...] += r * r
    mean = jnp.sum(squares[...], axis=-1, keepdims=True) / res.shape[1]
    normed_ref[...] = (res[...] * lax.rsqrt(mean + epsilon) * gain_ref[...]).astype(BF)


def finish(hidden, gain, first, count, stages, nd, nt, feat, before):
    rows, width = hidden.shape
    tile = min(32, count)
    base = first // tile
    masks = [g for g, _ in stages]
    row = pl.BlockSpec((tile, width), lambda i: (i + base, 0))
    specs = [row, pl.BlockSpec((1, width), lambda i: (0, 0))]
    for g, _ in stages:
        specs.append(pl.BlockSpec((len(g), nd, tile, feat), lambda i: (0, 0, i, 0)))
    args = [hidden, gain.reshape(1, width)] + [x for _, x in stages]
    alias = {}
    if before is not None:
        alias = {len(args): 0, len(args) + 1: 1}
        specs += [pl.BlockSpec(memory_space=pl.ANY)] * 2
        args += list(before)
    return pl.pallas_call(
        functools.partial(finish_kernel, nd, nt, feat, masks),
        grid=(count // tile,),
        in_specs=specs,
        out_specs=[row, row],
        out_shape=[jax.ShapeDtypeStruct((rows, width), BF)] * 2,
        scratch_shapes=[pltpu.VMEM((tile, width), F32), pltpu.VMEM((tile, feat), F32)],
        input_output_aliases=alias,
        cost_estimate=pl.CostEstimate(flops=count * width * 20, bytes_accessed=8 * count * width, transcendentals=0),
    )(*args)


def flip(i, mask):
    for b in (1, 2, 4, 8, 16, 32, 64):
        if mask & b:
            i = i + b - 2 * b * ((i // b) % 2)
    return i


def sender(started):
    def send(src, dst, ssem, rsem, where):
        copy = pltpu.make_async_remote_copy(
            src_ref=src, dst_ref=dst, send_sem=ssem, recv_sem=rsem,
            device_id=where, device_id_type=pl.DeviceIdType.MESH,
        )
        copy.start()
        started.append(copy)

    return send


def await_into(dst, sem):
    pltpu.make_async_remote_copy(
        src_ref=dst, dst_ref=dst, send_sem=sem, recv_sem=sem,
        device_id={"dp": lax.axis_index("dp")}, device_id_type=pl.DeviceIdType.MESH,
    ).wait_recv()


def greet(nd, nt):
    me, ten = lax.axis_index("dp"), lax.axis_index("tensor")
    peers = sorted(set(bits_of(nt)) | set(range(2, nt, 2)))
    barrier = pltpu.get_barrier_semaphore()
    for m in range(1, nd):
        pl.semaphore_signal(
            barrier, inc=1, device_id={"dp": flip(me, m)}, device_id_type=pl.DeviceIdType.MESH
        )
    for b in peers:
        pl.semaphore_signal(
            barrier, inc=1, device_id={"tensor": flip(ten, b)}, device_id_type=pl.DeviceIdType.MESH
        )
    pl.semaphore_wait(barrier, nd - 1 + len(peers))


def inputs_part(nd, nt, started, prefetch, prepare, place_columns, hidden_ref, gain_ref, q_ref, k_ref, v_ref, *scratch):
    wf, wsend, w2, araw, an, srow, sall, even, away, gotc = scratch[:10]
    hops = bits_of(nd)[1:]
    H = len(hops)
    snd, rcv = scratch[10 : 10 + H], scratch[10 + H : 10 + 2 * H]
    zsnd, zrcv, ls, ws, wr, as_, ar, ss, sr, cs, cr, hs, hr, zs, zr = scratch[10 + 2 * H :]
    me, ten = lax.axis_index("dp"), lax.axis_index("tensor")
    rows, width = hidden_ref.shape
    feat = q_ref.shape[0]
    wide = w2.shape[-1]
    qc, kc = q_ref.shape[1] // nt, k_ref.shape[1] // nt
    keep = list(range(0, nt, 2))[::-1]
    spans = [(q_ref, qc, j) for j in range(qc // wide)]
    spans += [(w, kc, j) for w in (k_ref, v_ref) for j in range(kc // wide)]
    chunks = [(s, n) for s in keep for n in range(len(spans))]
    evens = list(range(0, nd, 2))
    orders = (hops, hops[::-1])
    send = sender(started)

    def load(c, e):
        s, n = chunks[c]
        ref, size, j = spans[n]
        at = pl.ds(pl.multiple_of(flip(ten, s | e) * size + j * wide, wide), wide)
        return pltpu.make_async_copy(ref.at[:, at], wf.at[e, c], ls.at[e, c])

    for e in (1, 0):
        for c in range(len(chunks)):
            load(c, e).start()

    prefetch()
    greet(nd, nt)

    def features(m, e):
        return pl.ds(pl.multiple_of((flip(me, m) * nt + flip(ten, e)) * feat, feat), feat)

    far_first = sorted(range(1, nd), key=lambda m: (-bin(m >> 1).count("1"), m))
    for m in far_first:
        for e in (0, 1):
            send(
                hidden_ref.at[:, features(m, e)], araw.at[m, e],
                as_.at[m, e], ar.at[m, e], {"dp": flip(me, m)},
            )
    for c in range(len(chunks)):
        load(c, 1).wait()
        wsend[c] = wf[1, c].astype(BF)
        send(wsend.at[c], w2.at[c, 1], ws.at[c], wr.at[c], {"tensor": flip(ten, 1)})

    step = 512

    def squares(i, acc):
        h = hidden_ref[:, pl.ds(pl.multiple_of(i * step, step), step)].astype(F32)
        h = h * h
        for j in range(0, step, 128):
            acc = acc + h[:, j : j + 128]
        return acc

    acc = lax.fori_loop(0, width // step, squares, jnp.zeros((rows, 128), F32))
    scale = lax.rsqrt(jnp.sum(acc, axis=-1, keepdims=True) / width + epsilon)
    scale = jnp.broadcast_to(scale, (rows, 128))
    srow[...] = scale.T[:8]
    for m in far_first:
        send(srow, sall.at[m], ss.at[m], sr.at[m], {"dp": flip(me, m)})
    for c in range(len(chunks)):
        load(c, 0).wait()
        w2[c, 0] = wf[0, c].astype(BF)
    prepare()

    def normalise(raw, scale, e):
        out = []
        for j in range(0, feat, 128):
            at = pl.ds(pl.multiple_of((me * nt + flip(ten, e)) * feat + j, 128), 128)
            out.append((raw[:, j : j + 128].astype(F32) * scale * gain_ref[:, at]).astype(BF))
        return jnp.concatenate(out, axis=1)

    for e in (0, 1):
        an[e, 0, 0] = normalise(hidden_ref[:, features(0, e)], scale, e)
    for m in range(1, nd):
        await_into(sall.at[m], sr.at[m])
        other = jnp.broadcast_to(sall[m][:1], (128, rows)).T
        for e in (0, 1):
            await_into(araw.at[m, e], ar.at[m, e])
            an[e, m % 2, m // 2] = normalise(araw[m, e], other, e)

    def place(c):
        order = orders[c % 2]
        return [sum(b for i, b in enumerate(order) if p >> (H - 1 - i) & 1) for p in range(len(evens))]

    def product(c, odd):
        out = None
        for e in (0, 1):
            lhs = an[e, odd].reshape(len(evens) * rows, feat)
            term = jnp.dot(lhs, w2[c, e], preferred_element_type=F32)
            out = term if out is None else out + term
        return out.reshape(len(evens), rows, wide)

    def begin(c):
        await_into(w2.at[c, 1], wr.at[c])
        out = product(c, 1).astype(BF)
        for p, m in enumerate(place(c)):
            away[c, p] = out[m // 2]
        send(away.at[c], gotc.at[c], cs.at[c], cr.at[c], {"dp": flip(me, 1)})
        out = product(c, 0)
        for p, m in enumerate(place(c)):
            even[c, p] = out[m // 2]

    def hop(c, l):
        g = len(evens) >> l
        if l == 0:
            await_into(gotc.at[c], cr.at[c])
            got = gotc[c]
        else:
            await_into(rcv[l - 1].at[c], hr.at[c, l - 1])
            got = rcv[l - 1][c]
        if l < H:
            g //= 2
            even[c, :g] = even[c, :g] + got[:g].astype(F32)
            snd[l][c] = (even[c, g : 2 * g] + got[g:].astype(F32)).astype(BF)
            bit = orders[c % 2][l]
            send(snd[l].at[c], rcv[l].at[c], hs.at[c, l], hr.at[c, l], {"dp": flip(me, bit)})
            return
        done = even[c, 0] + got[0].astype(F32)
        s, n = chunks[c]
        if s:
            zsnd[c] = done.astype(BF)
            send(zsnd.at[c], zrcv.at[c], zs.at[c], zr.at[c], {"tensor": flip(ten, s)})
        else:
            for other, (t, at) in enumerate(chunks):
                if t and at == n:
                    await_into(zrcv.at[other], zr.at[other])
                    done = done + zrcv[other].astype(F32)
            place_columns(n * wide, done)

    lags = [1 + 2 * l for l in range(H + 1)]
    for i in range(len(chunks) + lags[-1]):
        for l in range(H, -1, -1):
            c = i - lags[l]
            if 0 <= c < len(chunks):
                hop(c, l)
        if i < len(chunks):
            begin(i)


def project_part(nd, nt, started, attend_half, weights, fin, att, prod, wt, acc, zs, zr, ds, dr, ps, pr, fs, fr):
    me, ten = lax.axis_index("dp"), lax.axis_index("tensor")
    rows = att.shape[2]
    half = rows // 2
    evens = list(range(0, nd, 2))
    high, zbits = bits_of(nd)[1:], bits_of(nt)[::-1]
    levels = [[m for m in evens if bin(m).count("1") == k] for k in range(len(high) + 1)]
    pairs = [[n for m in level for n in (m, m + 1)] for level in levels]
    slot = {m: k for k, m in enumerate(m for group in pairs for m in group)}
    orders = (high + [1], high[::-1] + [1])
    waves = [[s for s in range(nt) if bin(s).count("1") == k][::-1] for k in range(1, len(zbits) + 1)]
    walk = [0] + [s for wave in waves for s in wave]
    send = sender(started)

    def block(m, s):
        return att.at[s, slot[m]]

    def z_sends(s, h):
        part = pl.ds(h * half, half)
        for b in zbits:
            if b < (s & -s) or s == 0:
                send(
                    block(0, s).at[part], att.at[s | b, 0, part],
                    zs.at[s | b, h], zr.at[s | b, h], {"tensor": flip(ten, b)},
                )

    def dp_sends(m, s, h, bits):
        order = orders[h]
        used = [order.index(b) for b in order if m & b]
        for b in order[max(used) + 1 if used else 0 :]:
            if b in bits:
                part = pl.ds(h * half, half)
                send(
                    block(m, s).at[part], att.at[s, slot[m | b], part],
                    ds.at[s, m | b, h], dr.at[s, m | b, h], {"dp": flip(me, b)},
                )

    def arrive(m, s, h):
        await_into(att.at[s, slot[m], pl.ds(h * half, half)], dr.at[s, m, h])

    def near(level, s):
        for h in (0, 1):
            for m in levels[level]:
                arrive(m, s, h)
                dp_sends(m, s, h, [1])

    def far(level, s):
        for h in (0, 1):
            for m in levels[level]:
                dp_sends(m, s, h, high)

    def relay(level, s):
        near(level, s)
        far(level, s)

    def partial(level, s):
        ms = pairs[level]
        for m in ms[1::2]:
            for h in (0, 1):
                arrive(m, s, h)
        first, group = slot[ms[0]], len(ms)
        lhs = att[s, first : first + group].reshape(group * rows, -1)
        term = jnp.dot(lhs, wt[s], preferred_element_type=F32)
        if s == 0:
            acc[: group * rows] = term
        elif s != walk[-1]:
            acc[: group * rows] += term
        else:
            out = acc[: group * rows] + term
            prod[pl.ds(first, group)] = out.astype(BF).reshape(group, rows, -1)
            for m in ms:
                if m:
                    send(prod.at[slot[m]], fin.at[0, m], ps.at[m], pr.at[m], {"dp": flip(me, m)})

    def spread(m, s):
        for b in zbits:
            if b < (s & -s) or s == 0:
                send(fin.at[s, m], fin.at[s | b, m], fs.at[s | b, m], fr.at[s | b, m], {"tensor": flip(ten, b)})

    def own_results(ms):
        for m in ms:
            if m:
                await_into(fin.at[0, m], pr.at[m])
                spread(m, 0)

    passing = [s for s in walk[1:] if not s & 1]
    ending = [s for s in range(1, nt) if s & 1]

    def pass_on(ms):
        for s in passing:
            for m in ms:
                await_into(fin.at[s, m], fr.at[s, m])
                spread(m, s)

    for h in (0, 1):
        attend_half(h)
        z_sends(0, h)
        dp_sends(0, 0, h, high + [1])
    weights()
    waiting = list(walk)
    for wave in waves:
        for h in (0, 1):
            for s in wave:
                await_into(att.at[s, 0, pl.ds(h * half, half)], zr.at[s, h])
                z_sends(s, h)
                dp_sends(0, s, h, high + [1])
            if h == 0:
                relay(1, waiting.pop(0))

    for s in walk:
        partial(0, s)
    fin[0, 0] = prod[0]
    spread(0, 0)
    own_results(pairs[0])
    for level in range(1, len(levels)):
        for s in waiting[:-1]:
            relay(level, s)
        for s in walk[:-1]:
            partial(level, s)
        pass_on(pairs[level - 1])
        near(level, walk[-1])
        partial(level, walk[-1])
        far(level, walk[-1])
        own_results(pairs[level])
        waiting = list(walk)
    pass_on(pairs[-1])
    for group in pairs:
        for m in group:
            for s in ending:
                await_into(fin.at[s, m], fr.at[s, m])


def block_kernel(nd, nt, refs_in, refs_out, inner, attn, outer):
    hidden_ref, gain_ref, lens_ref, q_ref, k_ref, v_ref, o_ref, keys_ref, vals_ref = refs_in
    fin, fresh_ref, new_ref = refs_out
    kept_keys, kept_vals, turn, qf, kf, vf, lf, of, kvs, ows = attn
    att, wt = outer[0], outer[2]
    ten = lax.axis_index("tensor")
    rows, heads = qf.shape[:2]
    qc, kc = q_ref.shape[1] // nt, k_ref.shape[1] // nt
    group = qc // kc
    wf = inner[0]
    feat, wide = wf.shape[2:]
    started = []
    caches = [
        pltpu.make_async_copy(keys_ref, kept_keys, kvs.at[0]),
        pltpu.make_async_copy(vals_ref, kept_vals, kvs.at[1]),
    ]
    pieces = [(s, j) for s in range(nt) for j in range(qc // wide)]

    def out_load(i):
        s, j = pieces[i]
        at = pl.ds(pl.multiple_of(flip(ten, s) * qc + j * wide, wide), wide)
        return pltpu.make_async_copy(o_ref.at[:, at], wf.at[0, i] if i < wf.shape[1] else wf.at[1, i - wf.shape[1]], ows.at[i])

    def prefetch():
        for copy in caches:
            copy.start()

    def prepare():
        for i in range(len(pieces)):
            out_load(i).start()
        half_dim = HEAD_DIM // 2
        lens = jnp.broadcast_to(lens_ref[...].astype(F32), (rows, HEAD_DIM))
        lane = lax.broadcasted_iota(jnp.int32, (rows, HEAD_DIM), 1)
        low = lane < half_dim
        index = jnp.where(low, lane, lane - half_dim).astype(F32)
        angle = lens * jnp.exp(-math.log(rope_base) * index / half_dim)
        turn[0] = jnp.cos(angle)
        turn[1] = jnp.where(low, -jnp.sin(angle), jnp.sin(angle))
        for h in range(heads):
            lf[:, h, :] = lens
        for i, (s, j) in enumerate(pieces):
            out_load(i).wait()
            w = wf[0, i] if i < wf.shape[1] else wf[1, i - wf.shape[1]]
            wt[s, j * wide : (j + 1) * wide] = w.T.astype(BF)

    def place_columns(first, total):
        for j in range(0, total.shape[1], HEAD_DIM):
            x, at = total[:, j : j + HEAD_DIM], first + j
            if at < qc + kc:
                x = x * turn[0] + pltpu.roll(x, HEAD_DIM // 2, 1) * turn[1]
            x = x.astype(BF)
            if at < qc:
                qf[:, at // HEAD_DIM, :] = x.astype(F32)
                continue
            to, full, off = (fresh_ref, kf, at - qc) if at < qc + kc else (new_ref, vf, at - qc - kc)
            to[:, off : off + HEAD_DIM] = x
            g = off // HEAD_DIM
            for h in range(g * group, (g + 1) * group):
                full[:, h, :] = x.astype(F32)

    def attend_half(part):
        if part == 0:
            for copy in caches:
                copy.wait()
        kinds = kc // HEAD_DIM
        step, span = 16, kept_keys.shape[1]
        shape = (step, heads, span)
        spot = lax.broadcasted_iota(jnp.int32, shape, 2)
        mine = spot % kinds == lax.broadcasted_iota(jnp.int32, shape, 1) // group
        where = (spot // kinds).astype(F32)
        root = 1.0 / math.sqrt(HEAD_DIM)

        def some(i, carry):
            at = pl.ds(pl.multiple_of(part * (rows // 2) + i * step, step), step)
            q = qf[at]
            scores = root * lax.dot_general(
                q.astype(BF), kept_keys[at], (((2,), (2,)), ((0,), (0,))), preferred_element_type=F32
            )
            own = jnp.sum(q * kf[at], axis=-1, keepdims=True) * root
            scores = jnp.where(mine & (where < lf[at][:, :, :1]), scores, -jnp.inf)
            largest = jnp.maximum(jnp.max(scores, axis=-1, keepdims=True), own)
            kept = jnp.exp(scores - largest)
            own = jnp.exp(own - largest)
            divisor = jnp.sum(kept, axis=-1, keepdims=True) + own
            out = lax.dot_general(
                (kept / divisor).astype(BF), kept_vals[at],
                (((2,), (1,)), ((0,), (0,))), preferred_element_type=F32,
            )
            of[at] = out + (own / divisor).astype(BF).astype(F32) * vf[at]
            return carry

        lax.fori_loop(0, rows // 2 // step, some, 0)
        here = slice(part * (rows // 2), (part + 1) * (rows // 2))
        for h in range(heads):
            att[0, 0, here, h * HEAD_DIM : (h + 1) * HEAD_DIM] = of[here, h, :].astype(BF)

    inputs_part(nd, nt, started, prefetch, prepare, place_columns, hidden_ref, gain_ref, q_ref, k_ref, v_ref, *inner)
    project_part(nd, nt, started, attend_half, lambda: None, fin, *outer)
    for copy in started:
        copy.wait_send()


def block(hidden, gain, lengths, weights, key_cache, value_cache, nd, nt):
    rows, width = hidden.shape
    q_weight, k_weight, o_weight = weights[0], weights[1], weights[3]
    feat, wide = q_weight.shape[0], 256
    qc, kc = q_weight.shape[1] // nt, k_weight.shape[1] // nt
    heads = qc // HEAD_DIM
    C, half, H = (qc + 2 * kc) // wide * (nt // 2), nd // 2, nd.bit_length() - 2
    dma, vm = pltpu.SemaphoreType.DMA, pltpu.VMEM
    hop_bufs = [vm((C, half >> (l + 1), rows, wide), BF) for l in range(H)]
    in_place = pl.BlockSpec(memory_space=pltpu.VMEM)
    outside = pl.BlockSpec(memory_space=pl.ANY)
    span = key_cache.shape[1] * key_cache.shape[2]
    caches = [x.reshape(rows, span, HEAD_DIM) for x in (key_cache, value_cache)]
    inner = [
        vm((2, C, feat, wide), F32),
        vm((C, feat, wide), BF),
        vm((C, 2, feat, wide), BF),
        vm((nd, 2, rows, feat), BF),
        vm((2, 2, half, rows, feat), BF),
        vm((8, rows), F32),
        vm((nd, 8, rows), F32),
        vm((C, half, rows, wide), F32),
        vm((C, half, rows, wide), BF),
        vm((C, half, rows, wide), BF),
        *hop_bufs,
        *hop_bufs,
        vm((C, rows, wide), BF),
        vm((C, rows, wide), BF),
        dma((2, C)),
        dma((C,)), dma((C,)),
        dma((nd, 2)), dma((nd, 2)),
        dma((nd,)), dma((nd,)),
        dma((C,)), dma((C,)),
        dma((C, H)), dma((C, H)),
        dma((C,)), dma((C,)),
    ]
    by_head = [vm((rows, heads, HEAD_DIM), F32)] * 5
    attn = [
        vm((rows, span, HEAD_DIM), BF), vm((rows, span, HEAD_DIM), BF),
        vm((2, rows, HEAD_DIM), F32), *by_head, dma((2,)), dma((nt * qc // wide,)),
    ]
    outer = [
        vm((nt, nd, rows, qc), BF),
        vm((nd, rows, feat), BF),
        vm((nt, qc, feat), BF),
        vm((nd // 2 * rows, feat), F32),
        dma((nt, 2)), dma((nt, 2)),
        dma((nt, nd, 2)), dma((nt, nd, 2)),
        dma((nd,)), dma((nd,)),
        dma((nt, nd)), dma((nt, nd)),
    ]
    ends = [9, 12, 12 + len(inner), 12 + len(inner) + len(attn)]

    def kernel(*refs):
        block_kernel(
            nd, nt, refs[: ends[0]], refs[ends[0] : ends[1]],
            refs[ends[1] : ends[2]], refs[ends[2] : ends[3]], refs[ends[3] :],
        )

    return pl.pallas_call(
        kernel,
        in_specs=[in_place] * 3 + [outside] * 6,
        out_specs=[in_place] * 3,
        out_shape=[
            jax.ShapeDtypeStruct((nt, nd, rows, feat), BF),
            jax.ShapeDtypeStruct((rows, kc), BF),
            jax.ShapeDtypeStruct((rows, kc), BF),
        ],
        scratch_shapes=inner + attn + outer,
        compiler_params=pltpu.CompilerParams(
            collective_id=1, has_side_effects=True, vmem_limit_bytes=63 * 1024 * 1024
        ),
    )(hidden, gain.reshape(1, width), lengths.reshape(rows, 1), *weights, *caches)


def shards(
    hidden,
    q_weight,
    k_weight,
    v_weight,
    o_weight,
    input_gain,
    post_gain,
    key_cache,
    value_cache,
    lengths,
):
    nt = lax.axis_size("tensor")
    nd = lax.axis_size("dp")
    me, ten = lax.axis_index("dp"), lax.axis_index("tensor")
    rows, width = hidden.shape
    heads_here, kv_here = HEADS // nt, KV_HEADS // nt
    qc, kc = heads_here * HEAD_DIM, kv_here * HEAD_DIM
    feat = q_weight.shape[0]
    low, high = [1], bits_of(nd)[1:]
    orders = (low + high, low + high[::-1])
    odd = [m for m in range(nd) if m & 1]
    even = [m for m in range(nd) if not m & 1]
    count = rows // CHUNKS

    def columns(w, s, n):
        return lax.dynamic_slice_in_dim(w, (ten ^ s) * n, n, 1).astype(BF)

    together = feat % 128 == 0 and kc % 256 == 0 and rows == 128 and nt > 1 and nd > 2 and CHUNKS == 1
    together = together and kv_here * key_cache.shape[1] == 128 and heads_here == 8
    if together:
        weights = (q_weight, k_weight, v_weight, o_weight)
        mine, keys, news = block(hidden, input_gain, lengths, weights, key_cache, value_cache, nd, nt)
        outs = finish(hidden, post_gain, 0, rows, [(tuple(range(nt)), mine)], nd, nt, feat, None)
        shape = (rows, kv_here, HEAD_DIM)
        return (outs[0], outs[1], keys.reshape(shape), news.reshape(shape))
    pieces = norm_pieces(hidden, input_gain, nd, nt, feat)
    pieces = [swap(p, "dp", m, nd) if m else p for m, p in enumerate(pieces)]
    w_in = [
        jnp.concatenate(
            [columns(q_weight, s, qc), columns(k_weight, s, kc), columns(v_weight, s, kc)], axis=1
        )
        for s in range(nt)
    ]
    w_out = [columns(o_weight, s, qc) for s in range(nt)]

    fresh, values, outs = [], [], None
    for c in range(CHUNKS):
        r0 = c * count
        cut = [p[r0 : r0 + count] for p in pieces]
        lhs_odd = jnp.concatenate([cut[m] for m in odd])
        lhs_even = jnp.concatenate([cut[m] for m in even])
        total, behind = None, []
        for k, s in enumerate(reversed(range(nt))):
            if k and k % 2 == 0:
                held = lax.optimization_barrier((lhs_odd, lhs_even, *behind))
                lhs_odd, lhs_even, behind = held[0], held[1], []
            away = jnp.dot(lhs_odd, w_in[s], preferred_element_type=F32).astype(BF)
            got = swap(away, "dp", 1, nd)
            behind.append(got)
            acc = jnp.dot(lhs_even, w_in[s], preferred_element_type=F32) + got.astype(F32)
            acc = acc.astype(BF).reshape(len(even), count, -1)
            parts = {m: acc[j] for j, m in enumerate(even)}
            part = scatter_sum(parts, orders[k % 2][1:], "dp", nd)
            part = (swap(part, "tensor", s, nt) if s else part).astype(F32)
            total = part if total is None else total + part
        query, key_part, value_part = total[:, :qc], total[:, qc : qc + kc], total[:, qc + kc :]

        here = slice(r0, r0 + count)
        query_b = rotate(query.reshape(count, heads_here, HEAD_DIM), lengths[here]).astype(BF)
        keys = rotate(key_part.reshape(count, kv_here, HEAD_DIM), lengths[here]).astype(BF)
        news = value_part.reshape(count, kv_here, HEAD_DIM).astype(BF)
        fresh.append(keys)
        values.append(news)
        attended = attend(
            query_b, keys, news, key_cache[here], value_cache[here], lengths[here]
        )

        by_tensor = gather_all(attended, bits_of(nt)[::-1], "tensor", nt)
        product = None
        for k, s in enumerate(sorted(by_tensor, key=lambda s: (s & 1, s))):
            blocks = gather_all(by_tensor[s], orders[k % 2][1:] + low, "dp", nd)
            lhs = jnp.concatenate([blocks[m] for m in range(nd)])
            term = lax.dot_general(
                lhs, w_out[s], (((1,), (1,)), ((), ())), preferred_element_type=F32
            )
            product = term if product is None else product + term
        product = product.astype(BF).reshape(nd, count, feat)
        mine = jnp.stack([swap(product[m], "dp", m, nd) if m else product[0] for m in range(nd)])
        for b in bits_of(nd):
            v = mine.reshape(nd // (2 * b), 2, b, count, feat)
            mine = jnp.where((me & b) != 0, v[:, ::-1], v).reshape(nd, count, feat)
        mine = mine[None]
        for b in bits_of(nt)[::-1]:
            got = swap(mine, "tensor", b, nt)
            first = jnp.where((ten & b) != 0, got, mine)
            second = jnp.where((ten & b) != 0, mine, got)
            mine = jnp.stack([first, second], axis=1).reshape((-1,) + mine.shape[1:])
        mixed = mine.transpose(2, 1, 0, 3).reshape(count, width).astype(F32)
        residual = hidden[here].astype(F32) + mixed
        pair = (residual.astype(BF), rms_gain(residual, post_gain).astype(BF))
        outs = pair if outs is None else tuple(jnp.concatenate(z) for z in zip(outs, pair))
    return (outs[0], outs[1], jnp.concatenate(fresh), jnp.concatenate(values))


def solution(mesh):
    in_specs = (
        P("dp", None),
        P(("dp", "tensor"), None),
        P(("dp", "tensor"), None),
        P(("dp", "tensor"), None),
        P(("dp", "tensor"), None),
        P(),
        P(),
        P("dp", None, "tensor", None),
        P("dp", None, "tensor", None),
        P("dp"),
    )
    out_specs = (P("dp", None), P("dp", None), P("dp", "tensor", None), P("dp", "tensor", None))
    return jax.shard_map(shards, mesh=mesh, in_specs=in_specs, out_specs=out_specs, check_vma=False)
```

```python
import functools
import math

import jax
import jax.numpy as jnp
from jax import lax
from jax.experimental import pallas as pl
from jax.experimental.pallas import tpu as pltpu
from jax.sharding import PartitionSpec as P

HEADS = 32
KV_HEADS = 8
HEAD_DIM = 128

CHUNKS = 1

BF = jnp.bfloat16
F32 = jnp.float32

epsilon = 1e-05
rope_base = 500000.0


def rms_gain(values, gain_vector):
    mean_square = jnp.mean(values * values, axis=-1, keepdims=True)
    return values * lax.rsqrt(mean_square + epsilon) * gain_vector


def rotate(values, positions):
    half_dim = values.shape[-1] // 2
    index_row = jnp.arange(half_dim, dtype=jnp.float32)
    frequency = jnp.exp(-math.log(rope_base) * index_row / half_dim)
    angle = positions.astype(jnp.float32)[:, None, None] * frequency[None, None, :]
    first_half = values[..., :half_dim]
    second_half = values[..., half_dim:]
    return jnp.concatenate(
        [
            first_half * jnp.cos(angle) - second_half * jnp.sin(angle),
            second_half * jnp.cos(angle) + first_half * jnp.sin(angle),
        ],
        axis=-1,
    )


def attend(query_b, fresh_token_keys, new_values, key_cache, value_cache, lengths):
    row_count, kv_count = (fresh_token_keys.shape[0], fresh_token_keys.shape[1])
    grouped_heads = query_b.reshape(row_count, kv_count, -1, HEAD_DIM)
    reciprocal_root = 1.0 / math.sqrt(HEAD_DIM)
    scores = (
        jnp.einsum("bkgd,blkd->bkgl", grouped_heads, key_cache, preferred_element_type=jnp.float32)
        * reciprocal_root
    )
    self_token_score = (
        jnp.einsum(
            "lfxa,lfa->lfx", grouped_heads, fresh_token_keys, preferred_element_type=jnp.float32
        )
        * reciprocal_root
    )
    visible = jnp.arange(key_cache.shape[1], dtype=jnp.int32)[None, :] < lengths[:, None]
    scores = jnp.where(visible[:, None, None, :], scores, -jnp.inf)
    largest = jnp.maximum(jnp.max(scores, axis=-1), self_token_score)
    kept_exp = jnp.exp(scores - largest[..., None])
    own_exp = jnp.exp(self_token_score - largest)
    softmax_divisor = jnp.sum(kept_exp, axis=-1) + own_exp
    weights_kept = (kept_exp / softmax_divisor[..., None]).astype(jnp.bfloat16)
    own_weight = (own_exp / softmax_divisor).astype(jnp.bfloat16)
    attended = jnp.einsum(
        "bkgl,blkd->bkgd", weights_kept, value_cache, preferred_element_type=jnp.float32
    )
    attended = (
        attended
        + own_weight.astype(jnp.float32)[..., None] * new_values.astype(jnp.float32)[:, :, None, :]
    )
    return attended.reshape(row_count, -1).astype(jnp.bfloat16)


def swap(x, axis, mask, size):
    return lax.ppermute(x, axis, [(i, i ^ mask) for i in range(size)])


def add(a, b):
    return (a.astype(F32) + b.astype(F32)).astype(BF)


def bits_of(size):
    return [1 << k for k in range(size.bit_length() - 1)]


def scatter_sum(parts, bits, axis, size):
    for b in bits:
        up = sorted(m for m in parts if m & b)
        got = swap(jnp.stack([parts[m] for m in up]), axis, b, size)
        parts = {m: add(parts[m], got[up.index(m | b)]) for m in parts if not m & b}
    return parts[0]


def gather_all(x, bits, axis, size):
    held = {0: x}
    for b in bits:
        keys = sorted(held)
        got = swap(jnp.stack([held[m] for m in keys]), axis, b, size)
        held.update({m | b: got[k] for k, m in enumerate(keys)})
    return held


def norm_pieces_kernel(nd, nt, feat, hidden_ref, gain_ref, *outs):
    me, ten = lax.axis_index("dp"), lax.axis_index("tensor")
    h = hidden_ref[...].astype(F32)
    scale = lax.rsqrt(jnp.mean(h * h, axis=-1, keepdims=True) + epsilon)
    for m in range(nd):
        at = pl.ds(pl.multiple_of(((me ^ m) * nt + ten) * feat, feat), feat)
        outs[m][...] = (hidden_ref[:, at].astype(F32) * scale * gain_ref[:, at]).astype(BF)


def norm_pieces(hidden, gain, nd, nt, feat):
    rows, width = hidden.shape
    if feat % 128:
        me, ten = lax.axis_index("dp"), lax.axis_index("tensor")
        normal_in = rms_gain(hidden.astype(F32), gain).astype(BF)
        return [
            lax.dynamic_slice_in_dim(normal_in, ((me ^ m) * nt + ten) * feat, feat, 1)
            for m in range(nd)
        ]
    tile = min(32, rows)
    return pl.pallas_call(
        functools.partial(norm_pieces_kernel, nd, nt, feat),
        grid=(rows // tile,),
        in_specs=[
            pl.BlockSpec((tile, width), lambda i: (i, 0)),
            pl.BlockSpec((1, width), lambda i: (0, 0)),
        ],
        out_specs=[pl.BlockSpec((tile, feat), lambda i: (i, 0))] * nd,
        out_shape=[jax.ShapeDtypeStruct((rows, feat), BF)] * nd,
        cost_estimate=pl.CostEstimate(flops=rows * width * 20, bytes_accessed=4 * rows * width, transcendentals=0),
    )(hidden, gain.reshape(1, width))


def finish_kernel(nd, nt, feat, masks, hidden_ref, gain_ref, *refs):
    blocks, (new_ref, normed_ref), (res, squares) = refs[: len(masks)], refs[-4:-2], refs[-2:]
    me, ten = lax.axis_index("dp"), lax.axis_index("tensor")
    squares[...] = jnp.zeros_like(squares)
    for ref, group in zip(blocks, masks):
        for k, s in enumerate(group):
            for m in range(nd):
                col = ((me ^ m) * nt + (ten ^ s)) * feat
                at = pl.ds(pl.multiple_of(col, feat), feat)
                r = hidden_ref[:, at].astype(F32) + ref[k, m].astype(F32)
                new_ref[:, at] = r.astype(BF)
                res[:, at] = r
                squares[...] += r * r
    mean = jnp.sum(squares[...], axis=-1, keepdims=True) / res.shape[1]
    normed_ref[...] = (res[...] * lax.rsqrt(mean + epsilon) * gain_ref[...]).astype(BF)


def finish(hidden, gain, first, count, stages, nd, nt, feat, before):
    rows, width = hidden.shape
    tile = min(32, count)
    base = first // tile
    masks = [g for g, _ in stages]
    row = pl.BlockSpec((tile, width), lambda i: (i + base, 0))
    specs = [row, pl.BlockSpec((1, width), lambda i: (0, 0))]
    for g, _ in stages:
        specs.append(pl.BlockSpec((len(g), nd, tile, feat), lambda i: (0, 0, i, 0)))
    args = [hidden, gain.reshape(1, width)] + [x for _, x in stages]
    alias = {}
    if before is not None:
        alias = {len(args): 0, len(args) + 1: 1}
        specs += [pl.BlockSpec(memory_space=pl.ANY)] * 2
        args += list(before)
    return pl.pallas_call(
        functools.partial(finish_kernel, nd, nt, feat, masks),
        grid=(count // tile,),
        in_specs=specs,
        out_specs=[row, row],
        out_shape=[jax.ShapeDtypeStruct((rows, width), BF)] * 2,
        scratch_shapes=[pltpu.VMEM((tile, width), F32), pltpu.VMEM((tile, feat), F32)],
        input_output_aliases=alias,
        cost_estimate=pl.CostEstimate(flops=count * width * 20, bytes_accessed=8 * count * width, transcendentals=0),
    )(*args)


def flip(i, mask):
    for b in (1, 2, 4, 8, 16, 32, 64):
        if mask & b:
            i = i + b - 2 * b * ((i // b) % 2)
    return i


def send(src, dst, ssem, rsem, where):
    pltpu.make_async_remote_copy(
        src_ref=src, dst_ref=dst, send_sem=ssem, recv_sem=rsem,
        device_id=where, device_id_type=pl.DeviceIdType.MESH,
    ).start()


def await_sent(ref, sem):
    pltpu.make_async_remote_copy(
        src_ref=ref, dst_ref=ref, send_sem=sem, recv_sem=sem,
        device_id={"dp": lax.axis_index("dp")}, device_id_type=pl.DeviceIdType.MESH,
    ).wait_send()


def await_into(dst, sem):
    pltpu.make_async_remote_copy(
        src_ref=dst, dst_ref=dst, send_sem=sem, recv_sem=sem,
        device_id={"dp": lax.axis_index("dp")}, device_id_type=pl.DeviceIdType.MESH,
    ).wait_recv()


def greet(nd, nt):
    me, ten = lax.axis_index("dp"), lax.axis_index("tensor")
    peers = sorted(set(bits_of(nt)) | set(range(2, nt, 2)))
    barrier = pltpu.get_barrier_semaphore()
    for m in range(1, nd):
        pl.semaphore_signal(
            barrier, inc=1, device_id={"dp": flip(me, m)}, device_id_type=pl.DeviceIdType.MESH
        )
    for b in peers:
        pl.semaphore_signal(
            barrier, inc=1, device_id={"tensor": flip(ten, b)}, device_id_type=pl.DeviceIdType.MESH
        )
    pl.semaphore_wait(barrier, nd - 1 + len(peers))


def inputs_part(nd, nt, prefetch, late, ready, prepare, place_columns, hidden_ref, gain_ref, q_ref, k_ref, v_ref, *scratch):
    wf, wsend, w2, araw, an, srow, sall, even, away, gotc = scratch[:10]
    hops = bits_of(nd)[1:]
    H = len(hops)
    snd, rcv = scratch[10 : 10 + H], scratch[10 + H : 10 + 2 * H]
    zsnd, zrcv, ls, wr, ar, sr, cr, hr, zr, sent = scratch[10 + 2 * H :]
    me, ten = lax.axis_index("dp"), lax.axis_index("tensor")
    rows, width = hidden_ref.shape
    feat = q_ref.shape[0]
    wide = w2.shape[-1]
    qc, kc = q_ref.shape[1] // nt, k_ref.shape[1] // nt
    keep = list(range(0, nt, 2))[::-1]
    spans = [(q_ref, qc, j) for j in range(qc // wide)]
    spans += [(w, kc, j) for w in (k_ref, v_ref) for j in range(kc // wide)]
    chunks = [(s, n) for s in keep for n in range(len(spans))]
    evens = list(range(0, nd, 2))
    orders = (hops, hops[::-1])
    def load(c, e):
        s, n = chunks[c]
        ref, size, j = spans[n]
        at = pl.ds(pl.multiple_of(flip(ten, s | e) * size + j * wide, wide), wide)
        return pltpu.make_async_copy(ref.at[:, at], wf.at[e, c], ls.at[c if e else len(chunks)])

    prefetch()
    for e in (1, 0):
        for c in range(len(chunks)):
            load(c, e).start()
    late()
    greet(nd, nt)
    ready()

    def features(m, e):
        return pl.ds(pl.multiple_of((flip(me, m) * nt + flip(ten, e)) * feat, feat), feat)

    far_first = sorted(range(1, nd), key=lambda m: (-bin(m >> 1).count("1"), m))
    for m in far_first:
        for e in (0, 1):
            send(
                hidden_ref.at[:, features(m, e)], araw.at[m, e],
                sent.at[0], ar.at[m], {"dp": flip(me, m)},
            )
    for c in range(len(chunks)):
        load(c, 1).wait()
        wsend[c] = wf[1, c].astype(BF)
        send(wsend.at[c], w2.at[c, 1], sent.at[1], wr.at[c], {"tensor": flip(ten, 1)})

    step = 512

    def squares(i, acc):
        h = hidden_ref[:, pl.ds(pl.multiple_of(i * step, step), step)].astype(F32)
        h = h * h
        for j in range(0, step, 128):
            acc = acc + h[:, j : j + 128]
        return acc

    acc = lax.fori_loop(0, width // step, squares, jnp.zeros((rows, 128), F32))
    scale = lax.rsqrt(jnp.sum(acc, axis=-1, keepdims=True) / width + epsilon)
    scale = jnp.broadcast_to(scale, (rows, 128))
    srow[...] = scale.T[:8]
    for m in far_first:
        send(srow, sall.at[m], sent.at[2], sr.at[m], {"dp": flip(me, m)})
    pltpu.make_async_copy(wf.at[0], wf.at[0], ls.at[len(chunks)]).wait()
    for c in range(len(chunks)):
        w2[c, 0] = wf[0, c].astype(BF)
    prepare()

    def normalise(raw, scale, e):
        out = []
        for j in range(0, feat, 128):
            at = pl.ds(pl.multiple_of((me * nt + flip(ten, e)) * feat + j, 128), 128)
            out.append((raw[:, j : j + 128].astype(F32) * scale * gain_ref[:, at]).astype(BF))
        return jnp.concatenate(out, axis=1)

    for e in (0, 1):
        an[e, 0, 0] = normalise(hidden_ref[:, features(0, e)], scale, e)
    for m in range(1, nd):
        await_into(sall.at[m], sr.at[m])
        other = jnp.broadcast_to(sall[m][:1], (128, rows)).T
        await_into(araw.at[m], ar.at[m])
        for e in (0, 1):
            an[e, m % 2, m // 2] = normalise(araw[m, e], other, e)

    def place(c):
        order = orders[c % 2]
        return [sum(b for i, b in enumerate(order) if p >> (H - 1 - i) & 1) for p in range(len(evens))]

    def product(c, odd):
        out = None
        for e in (0, 1):
            lhs = an[e, odd].reshape(len(evens) * rows, feat)
            term = jnp.dot(lhs, w2[c, e], preferred_element_type=F32)
            out = term if out is None else out + term
        return out.reshape(len(evens), rows, wide)

    def begin(c):
        await_into(w2.at[c, 1], wr.at[c])
        out = product(c, 1).astype(BF)
        for p, m in enumerate(place(c)):
            away[c, p] = out[m // 2]
        send(away.at[c], gotc.at[c], sent.at[3], cr.at[c], {"dp": flip(me, 1)})
        out = product(c, 0)
        for p, m in enumerate(place(c)):
            even[c, p] = out[m // 2]

    def hop(c, l):
        g = len(evens) >> l
        if l == 0:
            await_into(gotc.at[c], cr.at[c])
            got = gotc[c]
        else:
            await_into(rcv[l - 1].at[c], hr.at[c, l - 1])
            got = rcv[l - 1][c]
        if l < H:
            g //= 2
            even[c, :g] = even[c, :g] + got[:g].astype(F32)
            snd[l][c] = (even[c, g : 2 * g] + got[g:].astype(F32)).astype(BF)
            bit = orders[c % 2][l]
            send(snd[l].at[c], rcv[l].at[c], sent.at[5 + l], hr.at[c, l], {"dp": flip(me, bit)})
            return
        done = even[c, 0] + got[0].astype(F32)
        s, n = chunks[c]
        if s:
            zsnd[c] = done.astype(BF)
            held.append(c)
            if n < len(spans) // 2:
                cross()
        else:
            even[c, 0] = done

    def cross():
        for c in held:
            send(zsnd.at[c], zrcv.at[c], sent.at[4], zr.at[c], {"tensor": flip(ten, chunks[c][0])})
        held.clear()

    def settle(c):
        n, done = chunks[c][1], even[c, 0]
        for other, (t, at) in enumerate(chunks):
            if t and at == n:
                await_into(zrcv.at[other], zr.at[other])
                done = done + zrcv[other].astype(F32)
        place_columns(n * wide, done)

    held = []
    lags = [1 + 2 * l for l in range(H + 1)]
    final = max(lags[-1] + 1, len(spans) + 1)
    for i in range(len(chunks) + final):
        if 0 <= i - final < len(chunks) and not chunks[i - final][0]:
            settle(i - final)
        for l in range(H, -1, -1):
            c = i - lags[l]
            if 0 <= c < len(chunks):
                hop(c, l)
        if i < len(chunks):
            begin(i)
        if i >= len(chunks) - 1:
            cross()
    crossing = sum(1 for c, _ in chunks if c)
    done = [(araw.at[pl.ds(1, nd - 1)], 0), (wsend, 1), (sall.at[pl.ds(1, nd - 1)], 2)]
    done += [(away, 3), (zsnd.at[pl.ds(0, crossing)], 4)]
    done += [(snd[l], 5 + l) for l in range(H)]
    return [(ref, sent.at[k]) for ref, k in done]


def project_part(nd, nt, attend_half, fin, att, prod, wt, acc, zr, dr, pr, fr, sent):
    me, ten = lax.axis_index("dp"), lax.axis_index("tensor")
    rows = att.shape[2]
    half = rows // 2
    evens = list(range(0, nd, 2))
    high, zbits = bits_of(nd)[1:], bits_of(nt)[::-1]
    levels = [[m for m in evens if bin(m).count("1") == k] for k in range(len(high) + 1)]
    pairs = [[n for m in level for n in (m, m + 1)] for level in levels]
    slot = {m: k for k, m in enumerate(m for group in pairs for m in group)}
    orders = (high + [1], high[::-1] + [1])
    waves = [[s for s in range(nt) if bin(s).count("1") == k][::-1] for k in range(1, len(zbits) + 1)]
    walk = [0] + [s for wave in waves for s in wave]
    def block(m, s):
        return att.at[s, slot[m]]

    def z_sends(s, h):
        part = pl.ds(h * half, half)
        for b in zbits:
            if b < (s & -s) or s == 0:
                send(
                    block(0, s).at[part], att.at[s | b, 0, part],
                    sent.at[0], zr.at[s | b, h], {"tensor": flip(ten, b)},
                )

    def dp_sends(m, s, h, bits):
        order = orders[h]
        used = [order.index(b) for b in order if m & b]
        for b in order[max(used) + 1 if used else 0 :]:
            if b in bits:
                part = pl.ds(h * half, half)
                send(
                    block(m, s).at[part], att.at[s, slot[m | b], part],
                    sent.at[1], dr.at[s, m | b], {"dp": flip(me, b)},
                )

    def arrive(m, s):
        await_into(att.at[s, slot[m]], dr.at[s, m])

    def near(level, s):
        for m in levels[level]:
            arrive(m, s)
            for h in (0, 1):
                dp_sends(m, s, h, [1])

    def far(level, s):
        for h in (0, 1):
            for m in levels[level]:
                dp_sends(m, s, h, high)

    def relay(level, s):
        near(level, s)
        far(level, s)

    def partial(level, s):
        ms = pairs[level]
        for m in ms[1::2]:
            arrive(m, s)
        first, group = slot[ms[0]], len(ms)
        lhs = att[s, first : first + group].reshape(group * rows, -1)
        term = jnp.dot(lhs, wt[s], preferred_element_type=F32)
        if s == 0:
            acc[: group * rows] = term
        elif s != walk[-1]:
            acc[: group * rows] += term
        else:
            out = acc[: group * rows] + term
            prod[pl.ds(first, group)] = out.astype(BF).reshape(group, rows, -1)
            for m in ms:
                if m:
                    send(prod.at[slot[m]], fin.at[0, m], sent.at[2], pr.at[m], {"dp": flip(me, m)})

    def done_at(s, m):
        return fr.at[nd * (passing.index(s) if s in passing else len(passing)) + (m if s in passing else ending.index(s))]

    def spread(m, s):
        for b in zbits:
            if b < (s & -s) or s == 0:
                send(fin.at[s, m], fin.at[s | b, m], sent.at[3], done_at(s | b, m), {"tensor": flip(ten, b)})

    def own_results(ms):
        for m in ms:
            if m:
                await_into(fin.at[0, m], pr.at[m])
                spread(m, 0)

    passing = [s for s in walk[1:] if not s & 1]
    ending = [s for s in range(1, nt) if s & 1]

    def pass_on(ms):
        for s in passing:
            for m in ms:
                await_into(fin.at[s, m], done_at(s, m))
                spread(m, s)

    for h in (0, 1):
        attend_half(h)
        z_sends(0, h)
        dp_sends(0, 0, h, high + [1])
    for wave in waves:
        for h in (0, 1):
            for s in wave:
                await_into(att.at[s, 0, pl.ds(h * half, half)], zr.at[s, h])
                z_sends(s, h)
                dp_sends(0, s, h, high + [1])

    for s in walk:
        partial(0, s)
    fin[0, 0] = prod[0]
    spread(0, 0)
    relay(1, walk[0])
    own_results(pairs[0])
    for level in range(1, len(levels)):
        for s in walk[1:-1] if level == 1 else walk[:-1]:
            near(level, s)
        for s in walk[:-1]:
            partial(level, s)
        behind = pairs[level - 1]
        cut = len(behind) if level == 1 else len(behind) // 2
        pass_on(behind[:cut])
        near(level, walk[-1])
        partial(level, walk[-1])
        for s in walk[1:] if level == 1 else walk:
            far(level, s)
        pass_on(behind[cut:])
        own_results(pairs[level])
    pass_on(pairs[-1])
    for s in ending:
        await_into(fin.at[s], done_at(s, 0))
    one, rest = pl.ds(1, nt - 1), pl.ds(1, nd - 1)
    done = [(att.at[one, 0], 0), (att.at[:, rest], 1), (prod.at[rest], 2), (fin.at[one], 3)]
    return [(ref, sent.at[k]) for ref, k in done]


def block_kernel(nd, nt, refs_in, refs_out, inner, attn, outer):
    rows_ref, gain_ref, lens_ref, q_ref, k_ref, v_ref, o_ref, keys_ref, vals_ref = refs_in
    fin, fresh_ref, new_ref = refs_out
    hidden_ref, kept_keys, kept_vals, turn, qf, kf, vf, lf, of, kvs, ows = attn
    att, wt = outer[0], outer[2]
    ten = lax.axis_index("tensor")
    rows, heads = qf.shape[:2]
    qc, kc = q_ref.shape[1] // nt, k_ref.shape[1] // nt
    group = qc // kc
    wf = inner[0]
    feat, wide = wf.shape[2:]
    caches = [
        pltpu.make_async_copy(keys_ref, kept_keys, kvs.at[0]),
        pltpu.make_async_copy(vals_ref, kept_vals, kvs.at[1]),
    ]
    pieces = [(s, j) for s in range(nt) for j in range(qc // wide)]

    def out_load(i):
        s, j = pieces[i]
        at = pl.ds(pl.multiple_of(flip(ten, s) * qc + j * wide, wide), wide)
        return pltpu.make_async_copy(o_ref.at[:, at], wf.at[0, i] if i < wf.shape[1] else wf.at[1, i - wf.shape[1]], ows.at[0])

    row_copy = pltpu.make_async_copy(rows_ref, hidden_ref, kvs.at[2])

    def prefetch():
        row_copy.start()

    def late():
        for copy in caches:
            copy.start()

    def ready():
        row_copy.wait()

    def prepare():
        for i in range(len(pieces)):
            out_load(i).start()
        half_dim = HEAD_DIM // 2
        lens = jnp.broadcast_to(lens_ref[...].astype(F32), (HEAD_DIM, rows)).T
        lane = lax.broadcasted_iota(jnp.int32, (rows, HEAD_DIM), 1)
        low = lane < half_dim
        index = jnp.where(low, lane, lane - half_dim).astype(F32)
        angle = lens * jnp.exp(-math.log(rope_base) * index / half_dim)
        turn[0] = jnp.cos(angle)
        turn[1] = jnp.where(low, -jnp.sin(angle), jnp.sin(angle))
        for h in range(heads):
            lf[:, h, :] = lens
        pltpu.make_async_copy(o_ref, o_ref, ows.at[0]).wait()
        for i, (s, j) in enumerate(pieces):
            w = wf[0, i] if i < wf.shape[1] else wf[1, i - wf.shape[1]]
            wt[s, j * wide : (j + 1) * wide] = w.T.astype(BF)

    def place_columns(first, total):
        for j in range(0, total.shape[1], HEAD_DIM):
            x, at = total[:, j : j + HEAD_DIM], first + j
            if at < qc + kc:
                x = x * turn[0] + pltpu.roll(x, HEAD_DIM // 2, 1) * turn[1]
            x = x.astype(BF)
            if at < qc:
                qf[:, at // HEAD_DIM, :] = x.astype(F32)
                continue
            to, full, off = (fresh_ref, kf, at - qc) if at < qc + kc else (new_ref, vf, at - qc - kc)
            to[:, off : off + HEAD_DIM] = x
            g = off // HEAD_DIM
            for h in range(g * group, (g + 1) * group):
                full[:, h, :] = x.astype(F32)

    def attend_half(part):
        if part == 0:
            for copy in caches:
                copy.wait()
        kinds = kc // HEAD_DIM
        step, span = 16, kept_keys.shape[1]
        shape = (step, heads, span)
        spot = lax.broadcasted_iota(jnp.int32, shape, 2)
        mine = spot % kinds == lax.broadcasted_iota(jnp.int32, shape, 1) // group
        where = (spot // kinds).astype(F32)
        root = 1.0 / math.sqrt(HEAD_DIM)

        def some(i, carry):
            at = pl.ds(pl.multiple_of(part * (rows // 2) + i * step, step), step)
            q = qf[at]
            scores = root * lax.dot_general(
                q.astype(BF), kept_keys[at], (((2,), (2,)), ((0,), (0,))), preferred_element_type=F32
            )
            own = jnp.sum(q * kf[at], axis=-1, keepdims=True) * root
            scores = jnp.where(mine & (where < lf[at][:, :, :1]), scores, -jnp.inf)
            largest = jnp.maximum(jnp.max(scores, axis=-1, keepdims=True), own)
            kept = jnp.exp(scores - largest)
            own = jnp.exp(own - largest)
            divisor = jnp.sum(kept, axis=-1, keepdims=True) + own
            out = lax.dot_general(
                (kept / divisor).astype(BF), kept_vals[at],
                (((2,), (1,)), ((0,), (0,))), preferred_element_type=F32,
            )
            of[at] = out + (own / divisor).astype(BF).astype(F32) * vf[at]
            return carry

        lax.fori_loop(0, rows // 2 // step, some, 0)
        here = slice(part * (rows // 2), (part + 1) * (rows // 2))
        for h in range(heads):
            att[0, 0, here, h * HEAD_DIM : (h + 1) * HEAD_DIM] = of[here, h, :].astype(BF)

    sent = inputs_part(nd, nt, prefetch, late, ready, prepare, place_columns, hidden_ref, gain_ref, q_ref, k_ref, v_ref, *inner)
    sent += project_part(nd, nt, attend_half, fin, *outer)
    for ref, sem in sent:
        await_sent(ref, sem)


def block(hidden, gain, lengths, weights, key_cache, value_cache, nd, nt):
    rows, width = hidden.shape
    q_weight, k_weight, o_weight = weights[0], weights[1], weights[3]
    feat, wide = q_weight.shape[0], 256
    qc, kc = q_weight.shape[1] // nt, k_weight.shape[1] // nt
    heads = qc // HEAD_DIM
    C, half, H = (qc + 2 * kc) // wide * (nt // 2), nd // 2, nd.bit_length() - 2
    dma, vm = pltpu.SemaphoreType.DMA, pltpu.VMEM
    hop_bufs = [vm((C, half >> (l + 1), rows, wide), BF) for l in range(H)]
    in_place = pl.BlockSpec(memory_space=pltpu.VMEM)
    outside = pl.BlockSpec(memory_space=pl.ANY)
    span = key_cache.shape[1] * key_cache.shape[2]
    caches = [x.reshape(rows, span, HEAD_DIM) for x in (key_cache, value_cache)]
    inner = [
        vm((2, C, feat, wide), F32),
        vm((C, feat, wide), BF),
        vm((C, 2, feat, wide), BF),
        vm((nd, 2, rows, feat), BF),
        vm((2, 2, half, rows, feat), BF),
        vm((8, rows), F32),
        vm((nd, 8, rows), F32),
        vm((C, half, rows, wide), F32),
        vm((C, half, rows, wide), BF),
        vm((C, half, rows, wide), BF),
        *hop_bufs,
        *hop_bufs,
        vm((C, rows, wide), BF),
        vm((C, rows, wide), BF),
        dma((C + 1,)), dma((C,)), dma((nd,)), dma((nd,)), dma((C,)), dma((C, H)), dma((C,)), dma((5 + H,)),
    ]
    by_head = [vm((rows, heads, HEAD_DIM), F32)] * 5
    attn = [
        vm((rows, width), BF),
        vm((rows, span, HEAD_DIM), BF), vm((rows, span, HEAD_DIM), BF),
        vm((2, rows, HEAD_DIM), F32), *by_head, dma((3,)), dma((1,)),
    ]
    outer = [
        vm((nt, nd, rows, qc), BF),
        vm((nd, rows, feat), BF),
        vm((nt, qc, feat), BF),
        vm((nd // 2 * rows, feat), F32),
        dma((nt, 2)), dma((nt, nd)), dma((nd,)), dma((nd * (nt // 2),)), dma((4,)),
    ]
    ends = [9, 12, 12 + len(inner), 12 + len(inner) + len(attn)]

    def kernel(*refs):
        block_kernel(
            nd, nt, refs[: ends[0]], refs[ends[0] : ends[1]],
            refs[ends[1] : ends[2]], refs[ends[2] : ends[3]], refs[ends[3] :],
        )

    return pl.pallas_call(
        kernel,
        in_specs=[outside] + [in_place] * 2 + [outside] * 6,
        out_specs=[in_place] * 3,
        out_shape=[
            jax.ShapeDtypeStruct((nt, nd, rows, feat), BF),
            jax.ShapeDtypeStruct((rows, kc), BF),
            jax.ShapeDtypeStruct((rows, kc), BF),
        ],
        scratch_shapes=inner + attn + outer,
        compiler_params=pltpu.CompilerParams(
            collective_id=1, has_side_effects=True, vmem_limit_bytes=63 * 1024 * 1024
        ),
    )(hidden, gain.reshape(1, width), lengths.reshape(1, rows), *weights, *caches)


def shards(
    hidden,
    q_weight,
    k_weight,
    v_weight,
    o_weight,
    input_gain,
    post_gain,
    key_cache,
    value_cache,
    lengths,
):
    nt = lax.axis_size("tensor")
    nd = lax.axis_size("dp")
    me, ten = lax.axis_index("dp"), lax.axis_index("tensor")
    rows, width = hidden.shape
    heads_here, kv_here = HEADS // nt, KV_HEADS // nt
    qc, kc = heads_here * HEAD_DIM, kv_here * HEAD_DIM
    feat = q_weight.shape[0]
    low, high = [1], bits_of(nd)[1:]
    orders = (low + high, low + high[::-1])
    odd = [m for m in range(nd) if m & 1]
    even = [m for m in range(nd) if not m & 1]
    count = rows // CHUNKS

    def columns(w, s, n):
        return lax.dynamic_slice_in_dim(w, (ten ^ s) * n, n, 1).astype(BF)

    together = feat % 128 == 0 and kc % 256 == 0 and rows == 128 and nt > 1 and nd > 2 and CHUNKS == 1
    together = together and kv_here * key_cache.shape[1] == 128 and heads_here == 8
    if together:
        weights = (q_weight, k_weight, v_weight, o_weight)
        mine, keys, news = block(hidden, input_gain, lengths, weights, key_cache, value_cache, nd, nt)
        outs = finish(hidden, post_gain, 0, rows, [(tuple(range(nt)), mine)], nd, nt, feat, None)
        shape = (rows, kv_here, HEAD_DIM)
        return (outs[0], outs[1], keys.reshape(shape), news.reshape(shape))
    pieces = norm_pieces(hidden, input_gain, nd, nt, feat)
    pieces = [swap(p, "dp", m, nd) if m else p for m, p in enumerate(pieces)]
    w_in = [
        jnp.concatenate(
            [columns(q_weight, s, qc), columns(k_weight, s, kc), columns(v_weight, s, kc)], axis=1
        )
        for s in range(nt)
    ]
    w_out = [columns(o_weight, s, qc) for s in range(nt)]

    fresh, values, outs = [], [], None
    for c in range(CHUNKS):
        r0 = c * count
        cut = [p[r0 : r0 + count] for p in pieces]
        lhs_odd = jnp.concatenate([cut[m] for m in odd])
        lhs_even = jnp.concatenate([cut[m] for m in even])
        total, behind = None, []
        for k, s in enumerate(reversed(range(nt))):
            if k and k % 2 == 0:
                held = lax.optimization_barrier((lhs_odd, lhs_even, *behind))
                lhs_odd, lhs_even, behind = held[0], held[1], []
            away = jnp.dot(lhs_odd, w_in[s], preferred_element_type=F32).astype(BF)
            got = swap(away, "dp", 1, nd)
            behind.append(got)
            acc = jnp.dot(lhs_even, w_in[s], preferred_element_type=F32) + got.astype(F32)
            acc = acc.astype(BF).reshape(len(even), count, -1)
            parts = {m: acc[j] for j, m in enumerate(even)}
            part = scatter_sum(parts, orders[k % 2][1:], "dp", nd)
            part = (swap(part, "tensor", s, nt) if s else part).astype(F32)
            total = part if total is None else total + part
        query, key_part, value_part = total[:, :qc], total[:, qc : qc + kc], total[:, qc + kc :]

        here = slice(r0, r0 + count)
        query_b = rotate(query.reshape(count, heads_here, HEAD_DIM), lengths[here]).astype(BF)
        keys = rotate(key_part.reshape(count, kv_here, HEAD_DIM), lengths[here]).astype(BF)
        news = value_part.reshape(count, kv_here, HEAD_DIM).astype(BF)
        fresh.append(keys)
        values.append(news)
        attended = attend(
            query_b, keys, news, key_cache[here], value_cache[here], lengths[here]
        )

        by_tensor = gather_all(attended, bits_of(nt)[::-1], "tensor", nt)
        product = None
        for k, s in enumerate(sorted(by_tensor, key=lambda s: (s & 1, s))):
            blocks = gather_all(by_tensor[s], orders[k % 2][1:] + low, "dp", nd)
            lhs = jnp.concatenate([blocks[m] for m in range(nd)])
            term = lax.dot_general(
                lhs, w_out[s], (((1,), (1,)), ((), ())), preferred_element_type=F32
            )
            product = term if product is None else product + term
        product = product.astype(BF).reshape(nd, count, feat)
        mine = jnp.stack([swap(product[m], "dp", m, nd) if m else product[0] for m in range(nd)])
        for b in bits_of(nd):
            v = mine.reshape(nd // (2 * b), 2, b, count, feat)
            mine = jnp.where((me & b) != 0, v[:, ::-1], v).reshape(nd, count, feat)
        mine = mine[None]
        for b in bits_of(nt)[::-1]:
            got = swap(mine, "tensor", b, nt)
            first = jnp.where((ten & b) != 0, got, mine)
            second = jnp.where((ten & b) != 0, mine, got)
            mine = jnp.stack([first, second], axis=1).reshape((-1,) + mine.shape[1:])
        mixed = mine.transpose(2, 1, 0, 3).reshape(count, width).astype(F32)
        residual = hidden[here].astype(F32) + mixed
        pair = (residual.astype(BF), rms_gain(residual, post_gain).astype(BF))
        outs = pair if outs is None else tuple(jnp.concatenate(z) for z in zip(outs, pair))
    return (outs[0], outs[1], jnp.concatenate(fresh), jnp.concatenate(values))


def solution(mesh):
    in_specs = (
        P("dp", None),
        P(("dp", "tensor"), None),
        P(("dp", "tensor"), None),
        P(("dp", "tensor"), None),
        P(("dp", "tensor"), None),
        P(),
        P(),
        P("dp", None, "tensor", None),
        P("dp", None, "tensor", None),
        P("dp"),
    )
    out_specs = (P("dp", None), P("dp", None), P("dp", "tensor", None), P("dp", "tensor", None))
    return jax.shard_map(shards, mesh=mesh, in_specs=in_specs, out_specs=out_specs, check_vma=False)
```

```python
import functools
import math

import jax
import jax.numpy as jnp
from jax import lax
from jax.experimental import pallas as pl
from jax.experimental.pallas import tpu as pltpu
from jax.sharding import PartitionSpec as P

HEADS = 32
KV_HEADS = 8
HEAD_DIM = 128

CHUNKS = 1
TILE = 64

BF = jnp.bfloat16
F32 = jnp.float32

epsilon = 1e-05
rope_base = 500000.0


def rms_gain(values, gain_vector):
    mean_square = jnp.mean(values * values, axis=-1, keepdims=True)
    return values * lax.rsqrt(mean_square + epsilon) * gain_vector


def rotate(values, positions):
    half_dim = values.shape[-1] // 2
    index_row = jnp.arange(half_dim, dtype=jnp.float32)
    frequency = jnp.exp(-math.log(rope_base) * index_row / half_dim)
    angle = positions.astype(jnp.float32)[:, None, None] * frequency[None, None, :]
    first_half = values[..., :half_dim]
    second_half = values[..., half_dim:]
    return jnp.concatenate(
        [
            first_half * jnp.cos(angle) - second_half * jnp.sin(angle),
            second_half * jnp.cos(angle) + first_half * jnp.sin(angle),
        ],
        axis=-1,
    )


def attend(query_b, fresh_token_keys, new_values, key_cache, value_cache, lengths):
    row_count, kv_count = (fresh_token_keys.shape[0], fresh_token_keys.shape[1])
    grouped_heads = query_b.reshape(row_count, kv_count, -1, HEAD_DIM)
    reciprocal_root = 1.0 / math.sqrt(HEAD_DIM)
    scores = (
        jnp.einsum("bkgd,blkd->bkgl", grouped_heads, key_cache, preferred_element_type=jnp.float32)
        * reciprocal_root
    )
    self_token_score = (
        jnp.einsum(
            "lfxa,lfa->lfx", grouped_heads, fresh_token_keys, preferred_element_type=jnp.float32
        )
        * reciprocal_root
    )
    visible = jnp.arange(key_cache.shape[1], dtype=jnp.int32)[None, :] < lengths[:, None]
    scores = jnp.where(visible[:, None, None, :], scores, -jnp.inf)
    largest = jnp.maximum(jnp.max(scores, axis=-1), self_token_score)
    kept_exp = jnp.exp(scores - largest[..., None])
    own_exp = jnp.exp(self_token_score - largest)
    softmax_divisor = jnp.sum(kept_exp, axis=-1) + own_exp
    weights_kept = (kept_exp / softmax_divisor[..., None]).astype(jnp.bfloat16)
    own_weight = (own_exp / softmax_divisor).astype(jnp.bfloat16)
    attended = jnp.einsum(
        "bkgl,blkd->bkgd", weights_kept, value_cache, preferred_element_type=jnp.float32
    )
    attended = (
        attended
        + own_weight.astype(jnp.float32)[..., None] * new_values.astype(jnp.float32)[:, :, None, :]
    )
    return attended.reshape(row_count, -1).astype(jnp.bfloat16)


def swap(x, axis, mask, size):
    return lax.ppermute(x, axis, [(i, i ^ mask) for i in range(size)])


def add(a, b):
    return (a.astype(F32) + b.astype(F32)).astype(BF)


def bits_of(size):
    return [1 << k for k in range(size.bit_length() - 1)]


def scatter_sum(parts, bits, axis, size):
    for b in bits:
        up = sorted(m for m in parts if m & b)
        got = swap(jnp.stack([parts[m] for m in up]), axis, b, size)
        parts = {m: add(parts[m], got[up.index(m | b)]) for m in parts if not m & b}
    return parts[0]


def gather_all(x, bits, axis, size):
    held = {0: x}
    for b in bits:
        keys = sorted(held)
        got = swap(jnp.stack([held[m] for m in keys]), axis, b, size)
        held.update({m | b: got[k] for k, m in enumerate(keys)})
    return held


def norm_pieces_kernel(nd, nt, feat, hidden_ref, gain_ref, *outs):
    me, ten = lax.axis_index("dp"), lax.axis_index("tensor")
    h = hidden_ref[...].astype(F32)
    scale = lax.rsqrt(jnp.mean(h * h, axis=-1, keepdims=True) + epsilon)
    for m in range(nd):
        at = pl.ds(pl.multiple_of(((me ^ m) * nt + ten) * feat, feat), feat)
        outs[m][...] = (hidden_ref[:, at].astype(F32) * scale * gain_ref[:, at]).astype(BF)


def norm_pieces(hidden, gain, nd, nt, feat):
    rows, width = hidden.shape
    if feat % 128:
        me, ten = lax.axis_index("dp"), lax.axis_index("tensor")
        normal_in = rms_gain(hidden.astype(F32), gain).astype(BF)
        return [
            lax.dynamic_slice_in_dim(normal_in, ((me ^ m) * nt + ten) * feat, feat, 1)
            for m in range(nd)
        ]
    tile = min(32, rows)
    return pl.pallas_call(
        functools.partial(norm_pieces_kernel, nd, nt, feat),
        grid=(rows // tile,),
        in_specs=[
            pl.BlockSpec((tile, width), lambda i: (i, 0)),
            pl.BlockSpec((1, width), lambda i: (0, 0)),
        ],
        out_specs=[pl.BlockSpec((tile, feat), lambda i: (i, 0))] * nd,
        out_shape=[jax.ShapeDtypeStruct((rows, feat), BF)] * nd,
        cost_estimate=pl.CostEstimate(flops=rows * width * 20, bytes_accessed=4 * rows * width, transcendentals=0),
    )(hidden, gain.reshape(1, width))


def finish_kernel(nd, nt, feat, hidden_ref, gain_ref, ref, keys_ref, values_ref, new_ref, normed_ref, k_ref, v_ref, res, squares):
    me, ten = lax.axis_index("dp"), lax.axis_index("tensor")
    k_ref[...] = keys_ref[...].astype(BF)
    v_ref[...] = values_ref[...].astype(BF)
    total = jnp.zeros(squares.shape, F32)
    for s in range(nt):
        for m in range(nd):
            col = ((me ^ m) * nt + (ten ^ s)) * feat
            at = pl.ds(pl.multiple_of(col, feat), feat)
            r = hidden_ref[:, at].astype(F32) + ref[s, m].astype(F32)
            new_ref[:, at] = r.astype(BF)
            res[:, at] = r
            r = r * r
            for j in range(0, feat, 128):
                total = total + r[:, j : j + 128]
    mean = jnp.sum(total, axis=-1, keepdims=True) / res.shape[1]
    normed_ref[...] = (res[...] * lax.rsqrt(mean + epsilon) * gain_ref[...]).astype(BF)


def finish(hidden, gain, mine, keys, values, nd, nt, feat):
    rows, width = hidden.shape
    tile = min(TILE, rows)
    row = pl.BlockSpec((tile, width), lambda i: (i, 0))
    small = pl.BlockSpec((tile,) + keys.shape[1:], lambda i: (i, 0, 0))
    return pl.pallas_call(
        functools.partial(finish_kernel, nd, nt, feat),
        grid=(rows // tile,),
        in_specs=[
            row, pl.BlockSpec((1, width), lambda i: (0, 0)),
            pl.BlockSpec((nt, nd, tile, feat), lambda i: (0, 0, i, 0)), small, small,
        ],
        out_specs=[row, row, small, small],
        out_shape=[jax.ShapeDtypeStruct((rows, width), BF)] * 2 + [jax.ShapeDtypeStruct(keys.shape, BF)] * 2,
        scratch_shapes=[pltpu.VMEM((tile, width), F32), pltpu.VMEM((tile, 128), F32)],
        cost_estimate=pl.CostEstimate(flops=rows * width * 20, bytes_accessed=8 * rows * width, transcendentals=0),
    )(hidden, gain.reshape(1, width), mine, keys, values)


def flip(i, mask):
    for b in (1, 2, 4, 8, 16, 32, 64):
        if mask & b:
            i = i + b - 2 * b * ((i // b) % 2)
    return i


def send(src, dst, ssem, rsem, where):
    pltpu.make_async_remote_copy(
        src_ref=src, dst_ref=dst, send_sem=ssem, recv_sem=rsem,
        device_id=where, device_id_type=pl.DeviceIdType.MESH,
    ).start()


def await_sent(ref, sem):
    pltpu.make_async_remote_copy(
        src_ref=ref, dst_ref=ref, send_sem=sem, recv_sem=sem,
        device_id={"dp": lax.axis_index("dp")}, device_id_type=pl.DeviceIdType.MESH,
    ).wait_send()


def await_into(dst, sem):
    pltpu.make_async_remote_copy(
        src_ref=dst, dst_ref=dst, send_sem=sem, recv_sem=sem,
        device_id={"dp": lax.axis_index("dp")}, device_id_type=pl.DeviceIdType.MESH,
    ).wait_recv()


def greet(nd, nt):
    me, ten = lax.axis_index("dp"), lax.axis_index("tensor")
    peers = sorted(set(bits_of(nt)) | set(range(2, nt, 2)))
    barrier = pltpu.get_barrier_semaphore()
    for m in range(1, nd):
        pl.semaphore_signal(
            barrier, inc=1, device_id={"dp": flip(me, m)}, device_id_type=pl.DeviceIdType.MESH
        )
    for b in peers:
        pl.semaphore_signal(
            barrier, inc=1, device_id={"tensor": flip(ten, b)}, device_id_type=pl.DeviceIdType.MESH
        )
    pl.semaphore_wait(barrier, nd - 1 + len(peers))


def inputs_part(nd, nt, prefetch, late, ready, prepare, place_columns, hidden_ref, gain_ref, q_ref, k_ref, v_ref, *scratch):
    wf, wsend, w2, araw, an, srow, sall, even, away, gotc = scratch[:10]
    hops = bits_of(nd)[1:]
    H = len(hops)
    snd, rcv = scratch[10 : 10 + H], scratch[10 + H : 10 + 2 * H]
    zsnd, zrcv, ls, wr, ar, sr, cr, hr, zr, sent = scratch[10 + 2 * H :]
    me, ten = lax.axis_index("dp"), lax.axis_index("tensor")
    rows, width = hidden_ref.shape
    feat = q_ref.shape[0]
    wide = w2.shape[-1]
    qc, kc = q_ref.shape[1] // nt, k_ref.shape[1] // nt
    keep = list(range(0, nt, 2))[::-1]
    spans = [(q_ref, qc, j) for j in range(qc // wide)]
    spans += [(w, kc, j) for w in (k_ref, v_ref) for j in range(kc // wide)]
    chunks = [(s, n) for s in keep for n in range(len(spans))]
    evens = list(range(0, nd, 2))
    orders = (hops, hops[::-1])
    def load(c, e):
        s, n = chunks[c]
        ref, size, j = spans[n]
        at = pl.ds(pl.multiple_of(flip(ten, s | e) * size + j * wide, wide), wide)
        return pltpu.make_async_copy(ref.at[:, at], wf.at[e, c], ls.at[c if e else len(chunks)])

    prefetch()
    for e in (1, 0):
        for c in range(len(chunks)):
            load(c, e).start()
    late()
    greet(nd, nt)
    ready()

    def features(m, e):
        return pl.ds(pl.multiple_of((flip(me, m) * nt + flip(ten, e)) * feat, feat), feat)

    far_first = sorted(range(1, nd), key=lambda m: (-bin(m >> 1).count("1"), m))
    for m in far_first:
        for e in (0, 1):
            send(
                hidden_ref.at[:, features(m, e)], araw.at[m, e],
                sent.at[0], ar.at[m], {"dp": flip(me, m)},
            )
    for c in range(len(chunks)):
        load(c, 1).wait()
        wsend[c] = wf[1, c].astype(BF)
        send(wsend.at[c], w2.at[c, 1], sent.at[1], wr.at[c], {"tensor": flip(ten, 1)})

    step = 512

    def squares(i, acc):
        h = hidden_ref[:, pl.ds(pl.multiple_of(i * step, step), step)].astype(F32)
        h = h * h
        for j in range(0, step, 128):
            acc = acc + h[:, j : j + 128]
        return acc

    acc = lax.fori_loop(0, width // step, squares, jnp.zeros((rows, 128), F32))
    scale = lax.rsqrt(jnp.sum(acc, axis=-1, keepdims=True) / width + epsilon)
    scale = jnp.broadcast_to(scale, (rows, 128))
    srow[...] = scale.T[:8]
    for m in far_first:
        send(srow, sall.at[m], sent.at[2], sr.at[m], {"dp": flip(me, m)})
    pltpu.make_async_copy(wf.at[0], wf.at[0], ls.at[len(chunks)]).wait()
    for c in range(len(chunks)):
        w2[c, 0] = wf[0, c].astype(BF)
    prepare()

    def normalise(raw, scale, e):
        out = []
        for j in range(0, feat, 128):
            at = pl.ds(pl.multiple_of((me * nt + flip(ten, e)) * feat + j, 128), 128)
            out.append((raw[:, j : j + 128].astype(F32) * scale * gain_ref[:, at]).astype(BF))
        return jnp.concatenate(out, axis=1)

    for e in (0, 1):
        an[e, 0, 0] = normalise(hidden_ref[:, features(0, e)], scale, e)
    for m in range(1, nd):
        await_into(sall.at[m], sr.at[m])
        other = jnp.broadcast_to(sall[m][:1], (128, rows)).T
        await_into(araw.at[m], ar.at[m])
        for e in (0, 1):
            an[e, m % 2, m // 2] = normalise(araw[m, e], other, e)

    half = rows // 2
    parts = [slice(h * half, (h + 1) * half) for h in (0, 1)]

    def place(h):
        order = orders[h]
        return [sum(b for i, b in enumerate(order) if p >> (H - 1 - i) & 1) for p in range(len(evens))]

    def product(c, odd):
        out = None
        for e in (0, 1):
            lhs = an[e, odd].reshape(len(evens) * rows, feat)
            term = jnp.dot(lhs, w2[c, e], preferred_element_type=F32)
            out = term if out is None else out + term
        return out.reshape(len(evens), rows, wide)

    def begin(c):
        await_into(w2.at[c, 1], wr.at[c])
        out = product(c, 1).astype(BF)
        for h in (0, 1):
            for p, m in enumerate(place(h)):
                away[c, p, parts[h]] = out[m // 2, parts[h]]
        send(away.at[c], gotc.at[c], sent.at[3], cr.at[c], {"dp": flip(me, 1)})
        out = product(c, 0)
        for h in (0, 1):
            for p, m in enumerate(place(h)):
                even[c, p, parts[h]] = out[m // 2, parts[h]]

    def hop(c, l):
        g = len(evens) >> l
        if l == 0:
            await_into(gotc.at[c], cr.at[c])
            got = gotc[c]
        else:
            await_into(rcv[l - 1].at[c], hr.at[c, l - 1])
            got = rcv[l - 1][c]
        if l < H:
            g //= 2
            even[c, :g] = even[c, :g] + got[:g].astype(F32)
            snd[l][c] = (even[c, g : 2 * g] + got[g:].astype(F32)).astype(BF)
            for h in (0, 1):
                part = pl.ds(h * half, half)
                send(
                    snd[l].at[c, :, part], rcv[l].at[c, :, part],
                    sent.at[5 + l], hr.at[c, l], {"dp": flip(me, orders[h][l])},
                )
            return
        done = even[c, 0] + got[0].astype(F32)
        s, n = chunks[c]
        if s:
            zsnd[c] = done.astype(BF)
            held.append(c)
            if n < len(spans) // 2:
                cross()
        else:
            even[c, 0] = done

    def cross():
        for c in held:
            send(zsnd.at[c], zrcv.at[c], sent.at[4], zr.at[c], {"tensor": flip(ten, chunks[c][0])})
        held.clear()

    def settle(c):
        n, done = chunks[c][1], even[c, 0]
        for other, (t, at) in enumerate(chunks):
            if t and at == n:
                await_into(zrcv.at[other], zr.at[other])
                done = done + zrcv[other].astype(F32)
        place_columns(n * wide, done)

    held = []
    lags = [1 + 2 * l for l in range(H + 1)]
    final = max(lags[-1] + 1, len(spans) + 1)
    for i in range(len(chunks) + final):
        if 0 <= i - final < len(chunks) and not chunks[i - final][0]:
            settle(i - final)
        for l in range(H, -1, -1):
            c = i - lags[l]
            if 0 <= c < len(chunks):
                hop(c, l)
        if i < len(chunks):
            begin(i)
        if i >= len(chunks) - 1:
            cross()
    crossing = sum(1 for c, _ in chunks if c)
    done = [(araw.at[pl.ds(1, nd - 1)], 0), (wsend, 1), (sall.at[pl.ds(1, nd - 1)], 2)]
    done += [(away, 3), (zsnd.at[pl.ds(0, crossing)], 4)]
    done += [(snd[l], 5 + l) for l in range(H)]
    return [(ref, sent.at[k]) for ref, k in done]


def project_part(nd, nt, attend_part, fin, att, prod, wt, acc, zr, dr, pr, fr, sent):
    me, ten = lax.axis_index("dp"), lax.axis_index("tensor")
    rows = att.shape[2]
    half = rows // 2
    evens = list(range(0, nd, 2))
    high, zbits = bits_of(nd)[1:], bits_of(nt)[::-1]
    levels = [[m for m in evens if bin(m).count("1") == k] for k in range(len(high) + 1)]
    pairs = [[n for m in level for n in (m, m + 1)] for level in levels]
    slot = {m: k for k, m in enumerate(m for group in pairs for m in group)}
    orders = (high + [1], high[::-1] + [1])
    waves = [[s for s in range(nt) if bin(s).count("1") == k][::-1] for k in range(1, len(zbits) + 1)]
    walk = [0] + [s for wave in waves for s in wave]
    def block(m, s):
        return att.at[s, slot[m]]

    def z_sends(s, h):
        part = pl.ds(h * half, half)
        for b in zbits:
            if b < (s & -s) or s == 0:
                send(
                    block(0, s).at[part], att.at[s | b, 0, part],
                    sent.at[0], zr.at[s | b, h], {"tensor": flip(ten, b)},
                )

    def dp_sends(m, s, h, bits):
        order = orders[h]
        used = [order.index(b) for b in order if m & b]
        for b in order[max(used) + 1 if used else 0 :]:
            if b in bits:
                part = pl.ds(h * half, half)
                send(
                    block(m, s).at[part], att.at[s, slot[m | b], part],
                    sent.at[1], dr.at[s, m | b], {"dp": flip(me, b)},
                )

    def arrive(m, s):
        await_into(att.at[s, slot[m]], dr.at[s, m])

    def near(level, s):
        for m in levels[level]:
            arrive(m, s)
            for h in (0, 1):
                dp_sends(m, s, h, [1])

    def far(level, s):
        for h in (0, 1):
            for m in levels[level]:
                dp_sends(m, s, h, high)

    def relay(level, s):
        near(level, s)
        far(level, s)

    def partial(level, s):
        ms = pairs[level]
        for m in ms[1::2]:
            arrive(m, s)
        first, group = slot[ms[0]], len(ms)
        lhs = att[s, first : first + group].reshape(group * rows, -1)
        term = jnp.dot(lhs, wt[s], preferred_element_type=F32)
        if s == 0:
            acc[: group * rows] = term
        elif s != walk[-1]:
            acc[: group * rows] += term
        else:
            out = acc[: group * rows] + term
            prod[pl.ds(first, group)] = out.astype(BF).reshape(group, rows, -1)
            for m in ms:
                if m:
                    send(prod.at[slot[m]], fin.at[0, m], sent.at[2], pr.at[m], {"dp": flip(me, m)})

    def done_at(s, m):
        return fr.at[nd * (passing.index(s) if s in passing else len(passing)) + (m if s in passing else ending.index(s))]

    def spread(m, s):
        for b in zbits:
            if b < (s & -s) or s == 0:
                send(fin.at[s, m], fin.at[s | b, m], sent.at[3], done_at(s | b, m), {"tensor": flip(ten, b)})

    def own_results(ms):
        for m in ms:
            if m:
                await_into(fin.at[0, m], pr.at[m])
                spread(m, 0)

    passing = [s for s in walk[1:] if not s & 1]
    ending = [s for s in range(1, nt) if s & 1]

    def pass_on(ms):
        for s in passing:
            for m in ms:
                await_into(fin.at[s, m], done_at(s, m))
                spread(m, s)

    for h in (0, 1):
        for q in (0, 1):
            attend_part(2 * h + q)
            part = pl.ds((2 * h + q) * (half // 2), half // 2)
            for b in zbits:
                send(block(0, 0).at[part], att.at[b, 0, part], sent.at[0], zr.at[b, h], {"tensor": flip(ten, b)})
        dp_sends(0, 0, h, high + [1])
    for wave in waves:
        for h in (0, 1):
            for s in wave:
                await_into(att.at[s, 0, pl.ds(h * half, half)], zr.at[s, h])
                z_sends(s, h)
                dp_sends(0, s, h, high + [1])

    for s in walk:
        partial(0, s)
    fin[0, 0] = prod[0]
    spread(0, 0)
    relay(1, walk[0])
    own_results(pairs[0])
    for level in range(1, len(levels)):
        for s in walk[1:-1] if level == 1 else walk[:-1]:
            near(level, s)
        for s in walk[:-1]:
            partial(level, s)
        behind = pairs[level - 1]
        cut = len(behind) if level == 1 else len(behind) // 2
        pass_on(behind[:cut])
        near(level, walk[-1])
        partial(level, walk[-1])
        for s in walk[1:] if level == 1 else walk:
            far(level, s)
        pass_on(behind[cut:])
        own_results(pairs[level])
    pass_on(pairs[-1])
    for s in ending:
        await_into(fin.at[s], done_at(s, 0))
    one, rest = pl.ds(1, nt - 1), pl.ds(1, nd - 1)
    done = [(att.at[one, 0], 0), (att.at[:, rest], 1), (prod.at[rest], 2), (fin.at[one], 3)]
    return [(ref, sent.at[k]) for ref, k in done]


def block_kernel(nd, nt, refs_in, refs_out, inner, attn, outer):
    rows_ref, gain_ref, lens_ref, q_ref, k_ref, v_ref, o_ref, keys_ref, vals_ref = refs_in
    fin, fresh_ref, new_ref = refs_out
    hidden_ref, kept_keys, kept_vals, turn, qf, kf, vf, lf, of, kvs, ows = attn
    att, wt = outer[0], outer[2]
    ten = lax.axis_index("tensor")
    rows, heads = qf.shape[:2]
    qc, kc = q_ref.shape[1] // nt, k_ref.shape[1] // nt
    group = qc // kc
    wf = inner[0]
    feat, wide = wf.shape[2:]
    caches = [
        pltpu.make_async_copy(keys_ref, kept_keys, kvs.at[0]),
        pltpu.make_async_copy(vals_ref, kept_vals, kvs.at[1]),
    ]
    pieces = [(s, j) for s in range(nt) for j in range(qc // wide)]

    def out_load(i):
        s, j = pieces[i]
        at = pl.ds(pl.multiple_of(flip(ten, s) * qc + j * wide, wide), wide)
        return pltpu.make_async_copy(o_ref.at[:, at], wf.at[0, i] if i < wf.shape[1] else wf.at[1, i - wf.shape[1]], ows.at[0])

    row_copy = pltpu.make_async_copy(rows_ref, hidden_ref, kvs.at[2])

    def prefetch():
        row_copy.start()

    def late():
        for copy in caches:
            copy.start()

    def ready():
        row_copy.wait()

    def prepare():
        for i in range(len(pieces)):
            out_load(i).start()
        half_dim = HEAD_DIM // 2
        lens = jnp.broadcast_to(lens_ref[...].astype(F32), (HEAD_DIM, rows)).T
        lane = lax.broadcasted_iota(jnp.int32, (rows, HEAD_DIM), 1)
        low = lane < half_dim
        index = jnp.where(low, lane, lane - half_dim).astype(F32)
        angle = lens * jnp.exp(-math.log(rope_base) * index / half_dim)
        turn[0] = jnp.cos(angle)
        turn[1] = jnp.where(low, -jnp.sin(angle), jnp.sin(angle))
        for h in range(heads):
            lf[:, h, :] = lens
        pltpu.make_async_copy(o_ref, o_ref, ows.at[0]).wait()
        for i, (s, j) in enumerate(pieces):
            w = wf[0, i] if i < wf.shape[1] else wf[1, i - wf.shape[1]]
            wt[s, j * wide : (j + 1) * wide] = w.T.astype(BF)

    def place_columns(first, total):
        for j in range(0, total.shape[1], HEAD_DIM):
            x, at = total[:, j : j + HEAD_DIM], first + j
            if at < qc + kc:
                x = x * turn[0] + pltpu.roll(x, HEAD_DIM // 2, 1) * turn[1]
            x = x.astype(BF)
            if at < qc:
                qf[:, at // HEAD_DIM, :] = x.astype(F32)
                continue
            to, full, off = (fresh_ref, kf, at - qc) if at < qc + kc else (new_ref, vf, at - qc - kc)
            g = off // HEAD_DIM
            to[:, g, :] = x.astype(F32)
            for h in range(g * group, (g + 1) * group):
                full[:, h, :] = x.astype(F32)

    def attend_part(part):
        if part == 0:
            for copy in caches:
                copy.wait()
        kinds = kc // HEAD_DIM
        step, span = 16, kept_keys.shape[1]
        shape = (step, heads, span)
        spot = lax.broadcasted_iota(jnp.int32, shape, 2)
        mine = spot % kinds == lax.broadcasted_iota(jnp.int32, shape, 1) // group
        where = (spot // kinds).astype(F32)
        root = 1.0 / math.sqrt(HEAD_DIM)

        def some(i, carry):
            at = pl.ds(pl.multiple_of(part * (rows // 4) + i * step, step), step)
            q = qf[at]
            scores = root * lax.dot_general(
                q.astype(BF), kept_keys[at], (((2,), (2,)), ((0,), (0,))), preferred_element_type=F32
            )
            own = jnp.sum(q * kf[at], axis=-1, keepdims=True) * root
            scores = jnp.where(mine & (where < lf[at][:, :, :1]), scores, -jnp.inf)
            largest = jnp.maximum(jnp.max(scores, axis=-1, keepdims=True), own)
            kept = jnp.exp(scores - largest)
            own = jnp.exp(own - largest)
            divisor = jnp.sum(kept, axis=-1, keepdims=True) + own
            out = lax.dot_general(
                (kept / divisor).astype(BF), kept_vals[at],
                (((2,), (1,)), ((0,), (0,))), preferred_element_type=F32,
            )
            of[at] = out + (own / divisor).astype(BF).astype(F32) * vf[at]
            return carry

        lax.fori_loop(0, rows // 4 // step, some, 0)
        here = slice(part * (rows // 4), (part + 1) * (rows // 4))
        for h in range(heads):
            att[0, 0, here, h * HEAD_DIM : (h + 1) * HEAD_DIM] = of[here, h, :].astype(BF)

    sent = inputs_part(nd, nt, prefetch, late, ready, prepare, place_columns, hidden_ref, gain_ref, q_ref, k_ref, v_ref, *inner)
    sent += project_part(nd, nt, attend_part, fin, *outer)
    for ref, sem in sent:
        await_sent(ref, sem)


def block(hidden, gain, lengths, weights, key_cache, value_cache, nd, nt):
    rows, width = hidden.shape
    q_weight, k_weight, o_weight = weights[0], weights[1], weights[3]
    feat, wide = q_weight.shape[0], 256
    qc, kc = q_weight.shape[1] // nt, k_weight.shape[1] // nt
    heads = qc // HEAD_DIM
    C, half, H = (qc + 2 * kc) // wide * (nt // 2), nd // 2, nd.bit_length() - 2
    dma, vm = pltpu.SemaphoreType.DMA, pltpu.VMEM
    hop_bufs = [vm((C, half >> (l + 1), rows, wide), BF) for l in range(H)]
    in_place = pl.BlockSpec(memory_space=pltpu.VMEM)
    outside = pl.BlockSpec(memory_space=pl.ANY)
    span = key_cache.shape[1] * key_cache.shape[2]
    caches = [x.reshape(rows, span, HEAD_DIM) for x in (key_cache, value_cache)]
    inner = [
        vm((2, C, feat, wide), F32),
        vm((C, feat, wide), BF),
        vm((C, 2, feat, wide), BF),
        vm((nd, 2, rows, feat), BF),
        vm((2, 2, half, rows, feat), BF),
        vm((8, rows), F32),
        vm((nd, 8, rows), F32),
        vm((C, half, rows, wide), F32),
        vm((C, half, rows, wide), BF),
        vm((C, half, rows, wide), BF),
        *hop_bufs,
        *hop_bufs,
        vm((C, rows, wide), BF),
        vm((C, rows, wide), BF),
        dma((C + 1,)), dma((C,)), dma((nd,)), dma((nd,)), dma((C,)), dma((C, H)), dma((C,)), dma((5 + H,)),
    ]
    by_head = [vm((rows, heads, HEAD_DIM), F32)] * 5
    attn = [
        vm((rows, width), BF),
        vm((rows, span, HEAD_DIM), BF), vm((rows, span, HEAD_DIM), BF),
        vm((2, rows, HEAD_DIM), F32), *by_head, dma((3,)), dma((1,)),
    ]
    outer = [
        vm((nt, nd, rows, qc), BF),
        vm((nd, rows, feat), BF),
        vm((nt, qc, feat), BF),
        vm((nd // 2 * rows, feat), F32),
        dma((nt, 2)), dma((nt, nd)), dma((nd,)), dma((nd * (nt // 2),)), dma((4,)),
    ]
    ends = [9, 12, 12 + len(inner), 12 + len(inner) + len(attn)]

    def kernel(*refs):
        block_kernel(
            nd, nt, refs[: ends[0]], refs[ends[0] : ends[1]],
            refs[ends[1] : ends[2]], refs[ends[2] : ends[3]], refs[ends[3] :],
        )

    return pl.pallas_call(
        kernel,
        in_specs=[outside] + [in_place] * 2 + [outside] * 6,
        out_specs=[in_place] * 3,
        out_shape=[
            jax.ShapeDtypeStruct((nt, nd, rows, feat), BF),
            jax.ShapeDtypeStruct((rows, kc // HEAD_DIM, HEAD_DIM), F32),
            jax.ShapeDtypeStruct((rows, kc // HEAD_DIM, HEAD_DIM), F32),
        ],
        scratch_shapes=inner + attn + outer,
        compiler_params=pltpu.CompilerParams(
            collective_id=1, has_side_effects=True, vmem_limit_bytes=63 * 1024 * 1024
        ),
    )(hidden, gain.reshape(1, width), lengths.reshape(1, rows), *weights, *caches)


def shards(
    hidden,
    q_weight,
    k_weight,
    v_weight,
    o_weight,
    input_gain,
    post_gain,
    key_cache,
    value_cache,
    lengths,
):
    nt = lax.axis_size("tensor")
    nd = lax.axis_size("dp")
    me, ten = lax.axis_index("dp"), lax.axis_index("tensor")
    rows, width = hidden.shape
    heads_here, kv_here = HEADS // nt, KV_HEADS // nt
    qc, kc = heads_here * HEAD_DIM, kv_here * HEAD_DIM
    feat = q_weight.shape[0]
    low, high = [1], bits_of(nd)[1:]
    orders = (low + high, low + high[::-1])
    odd = [m for m in range(nd) if m & 1]
    even = [m for m in range(nd) if not m & 1]
    count = rows // CHUNKS

    def columns(w, s, n):
        return lax.dynamic_slice_in_dim(w, (ten ^ s) * n, n, 1).astype(BF)

    together = feat % 128 == 0 and kc % 256 == 0 and rows == 128 and nt > 1 and nd > 2 and CHUNKS == 1
    together = together and kv_here * key_cache.shape[1] == 128 and heads_here == 8
    if together:
        weights = (q_weight, k_weight, v_weight, o_weight)
        mine, keys, news = block(hidden, input_gain, lengths, weights, key_cache, value_cache, nd, nt)
        return tuple(finish(hidden, post_gain, mine, keys, news, nd, nt, feat))
    pieces = norm_pieces(hidden, input_gain, nd, nt, feat)
    pieces = [swap(p, "dp", m, nd) if m else p for m, p in enumerate(pieces)]
    w_in = [
        jnp.concatenate(
            [columns(q_weight, s, qc), columns(k_weight, s, kc), columns(v_weight, s, kc)], axis=1
        )
        for s in range(nt)
    ]
    w_out = [columns(o_weight, s, qc) for s in range(nt)]

    fresh, values, outs = [], [], None
    for c in range(CHUNKS):
        r0 = c * count
        cut = [p[r0 : r0 + count] for p in pieces]
        lhs_odd = jnp.concatenate([cut[m] for m in odd])
        lhs_even = jnp.concatenate([cut[m] for m in even])
        total, behind = None, []
        for k, s in enumerate(reversed(range(nt))):
            if k and k % 2 == 0:
                held = lax.optimization_barrier((lhs_odd, lhs_even, *behind))
                lhs_odd, lhs_even, behind = held[0], held[1], []
            away = jnp.dot(lhs_odd, w_in[s], preferred_element_type=F32).astype(BF)
            got = swap(away, "dp", 1, nd)
            behind.append(got)
            acc = jnp.dot(lhs_even, w_in[s], preferred_element_type=F32) + got.astype(F32)
            acc = acc.astype(BF).reshape(len(even), count, -1)
            parts = {m: acc[j] for j, m in enumerate(even)}
            part = scatter_sum(parts, orders[k % 2][1:], "dp", nd)
            part = (swap(part, "tensor", s, nt) if s else part).astype(F32)
            total = part if total is None else total + part
        query, key_part, value_part = total[:, :qc], total[:, qc : qc + kc], total[:, qc + kc :]

        here = slice(r0, r0 + count)
        query_b = rotate(query.reshape(count, heads_here, HEAD_DIM), lengths[here]).astype(BF)
        keys = rotate(key_part.reshape(count, kv_here, HEAD_DIM), lengths[here]).astype(BF)
        news = value_part.reshape(count, kv_here, HEAD_DIM).astype(BF)
        fresh.append(keys)
        values.append(news)
        attended = attend(
            query_b, keys, news, key_cache[here], value_cache[here], lengths[here]
        )

        by_tensor = gather_all(attended, bits_of(nt)[::-1], "tensor", nt)
        product = None
        for k, s in enumerate(sorted(by_tensor, key=lambda s: (s & 1, s))):
            blocks = gather_all(by_tensor[s], orders[k % 2][1:] + low, "dp", nd)
            lhs = jnp.concatenate([blocks[m] for m in range(nd)])
            term = lax.dot_general(
                lhs, w_out[s], (((1,), (1,)), ((), ())), preferred_element_type=F32
            )
            product = term if product is None else product + term
        product = product.astype(BF).reshape(nd, count, feat)
        mine = jnp.stack([swap(product[m], "dp", m, nd) if m else product[0] for m in range(nd)])
        for b in bits_of(nd):
            v = mine.reshape(nd // (2 * b), 2, b, count, feat)
            mine = jnp.where((me & b) != 0, v[:, ::-1], v).reshape(nd, count, feat)
        mine = mine[None]
        for b in bits_of(nt)[::-1]:
            got = swap(mine, "tensor", b, nt)
            first = jnp.where((ten & b) != 0, got, mine)
            second = jnp.where((ten & b) != 0, mine, got)
            mine = jnp.stack([first, second], axis=1).reshape((-1,) + mine.shape[1:])
        mixed = mine.transpose(2, 1, 0, 3).reshape(count, width).astype(F32)
        residual = hidden[here].astype(F32) + mixed
        pair = (residual.astype(BF), rms_gain(residual, post_gain).astype(BF))
        outs = pair if outs is None else tuple(jnp.concatenate(z) for z in zip(outs, pair))
    return (outs[0], outs[1], jnp.concatenate(fresh), jnp.concatenate(values))


def solution(mesh):
    in_specs = (
        P("dp", None),
        P(("dp", "tensor"), None),
        P(("dp", "tensor"), None),
        P(("dp", "tensor"), None),
        P(("dp", "tensor"), None),
        P(),
        P(),
        P("dp", None, "tensor", None),
        P("dp", None, "tensor", None),
        P("dp"),
    )
    out_specs = (P("dp", None), P("dp", None), P("dp", "tensor", None), P("dp", "tensor", None))
    return jax.shard_map(shards, mesh=mesh, in_specs=in_specs, out_specs=out_specs, check_vma=False)
```

```python
import functools
import math

import jax
import jax.numpy as jnp
from jax import lax
from jax.experimental import pallas as pl
from jax.experimental.pallas import tpu as pltpu
from jax.sharding import PartitionSpec as P

HEADS = 32
KV_HEADS = 8
HEAD_DIM = 128

CHUNKS = 1
TILE = 64

BF = jnp.bfloat16
F32 = jnp.float32

epsilon = 1e-05
rope_base = 500000.0


def rms_gain(values, gain_vector):
    mean_square = jnp.mean(values * values, axis=-1, keepdims=True)
    return values * lax.rsqrt(mean_square + epsilon) * gain_vector


def rotate(values, positions):
    half_dim = values.shape[-1] // 2
    index_row = jnp.arange(half_dim, dtype=jnp.float32)
    frequency = jnp.exp(-math.log(rope_base) * index_row / half_dim)
    angle = positions.astype(jnp.float32)[:, None, None] * frequency[None, None, :]
    first_half = values[..., :half_dim]
    second_half = values[..., half_dim:]
    return jnp.concatenate(
        [
            first_half * jnp.cos(angle) - second_half * jnp.sin(angle),
            second_half * jnp.cos(angle) + first_half * jnp.sin(angle),
        ],
        axis=-1,
    )


def attend(query_b, fresh_token_keys, new_values, key_cache, value_cache, lengths):
    row_count, kv_count = (fresh_token_keys.shape[0], fresh_token_keys.shape[1])
    grouped_heads = query_b.reshape(row_count, kv_count, -1, HEAD_DIM)
    reciprocal_root = 1.0 / math.sqrt(HEAD_DIM)
    scores = (
        jnp.einsum("bkgd,blkd->bkgl", grouped_heads, key_cache, preferred_element_type=jnp.float32)
        * reciprocal_root
    )
    self_token_score = (
        jnp.einsum(
            "lfxa,lfa->lfx", grouped_heads, fresh_token_keys, preferred_element_type=jnp.float32
        )
        * reciprocal_root
    )
    visible = jnp.arange(key_cache.shape[1], dtype=jnp.int32)[None, :] < lengths[:, None]
    scores = jnp.where(visible[:, None, None, :], scores, -jnp.inf)
    largest = jnp.maximum(jnp.max(scores, axis=-1), self_token_score)
    kept_exp = jnp.exp(scores - largest[..., None])
    own_exp = jnp.exp(self_token_score - largest)
    softmax_divisor = jnp.sum(kept_exp, axis=-1) + own_exp
    weights_kept = (kept_exp / softmax_divisor[..., None]).astype(jnp.bfloat16)
    own_weight = (own_exp / softmax_divisor).astype(jnp.bfloat16)
    attended = jnp.einsum(
        "bkgl,blkd->bkgd", weights_kept, value_cache, preferred_element_type=jnp.float32
    )
    attended = (
        attended
        + own_weight.astype(jnp.float32)[..., None] * new_values.astype(jnp.float32)[:, :, None, :]
    )
    return attended.reshape(row_count, -1).astype(jnp.bfloat16)


def swap(x, axis, mask, size):
    return lax.ppermute(x, axis, [(i, i ^ mask) for i in range(size)])


def add(a, b):
    return (a.astype(F32) + b.astype(F32)).astype(BF)


def bits_of(size):
    return [1 << k for k in range(size.bit_length() - 1)]


def scatter_sum(parts, bits, axis, size):
    for b in bits:
        up = sorted(m for m in parts if m & b)
        got = swap(jnp.stack([parts[m] for m in up]), axis, b, size)
        parts = {m: add(parts[m], got[up.index(m | b)]) for m in parts if not m & b}
    return parts[0]


def gather_all(x, bits, axis, size):
    held = {0: x}
    for b in bits:
        keys = sorted(held)
        got = swap(jnp.stack([held[m] for m in keys]), axis, b, size)
        held.update({m | b: got[k] for k, m in enumerate(keys)})
    return held


def norm_pieces_kernel(nd, nt, feat, hidden_ref, gain_ref, *outs):
    me, ten = lax.axis_index("dp"), lax.axis_index("tensor")
    h = hidden_ref[...].astype(F32)
    scale = lax.rsqrt(jnp.mean(h * h, axis=-1, keepdims=True) + epsilon)
    for m in range(nd):
        at = pl.ds(pl.multiple_of(((me ^ m) * nt + ten) * feat, feat), feat)
        outs[m][...] = (hidden_ref[:, at].astype(F32) * scale * gain_ref[:, at]).astype(BF)


def norm_pieces(hidden, gain, nd, nt, feat):
    rows, width = hidden.shape
    if feat % 128:
        me, ten = lax.axis_index("dp"), lax.axis_index("tensor")
        normal_in = rms_gain(hidden.astype(F32), gain).astype(BF)
        return [
            lax.dynamic_slice_in_dim(normal_in, ((me ^ m) * nt + ten) * feat, feat, 1)
            for m in range(nd)
        ]
    tile = min(32, rows)
    return pl.pallas_call(
        functools.partial(norm_pieces_kernel, nd, nt, feat),
        grid=(rows // tile,),
        in_specs=[
            pl.BlockSpec((tile, width), lambda i: (i, 0)),
            pl.BlockSpec((1, width), lambda i: (0, 0)),
        ],
        out_specs=[pl.BlockSpec((tile, feat), lambda i: (i, 0))] * nd,
        out_shape=[jax.ShapeDtypeStruct((rows, feat), BF)] * nd,
        cost_estimate=pl.CostEstimate(flops=rows * width * 20, bytes_accessed=4 * rows * width, transcendentals=0),
    )(hidden, gain.reshape(1, width))


def finish_kernel(nd, nt, feat, hidden_ref, gain_ref, ref, keys_ref, values_ref, new_ref, normed_ref, k_ref, v_ref, res, squares):
    me, ten = lax.axis_index("dp"), lax.axis_index("tensor")
    k_ref[...] = keys_ref[...].astype(BF)
    v_ref[...] = values_ref[...].astype(BF)
    total = jnp.zeros(squares.shape, F32)
    for s in range(nt):
        for m in range(nd):
            col = ((me ^ m) * nt + (ten ^ s)) * feat
            at = pl.ds(pl.multiple_of(col, feat), feat)
            r = hidden_ref[:, at].astype(F32) + ref[s, m].astype(F32)
            new_ref[:, at] = r.astype(BF)
            res[:, at] = r
            r = r * r
            for j in range(0, feat, 128):
                total = total + r[:, j : j + 128]
    mean = jnp.sum(total, axis=-1, keepdims=True) / res.shape[1]
    normed_ref[...] = (res[...] * lax.rsqrt(mean + epsilon) * gain_ref[...]).astype(BF)


def finish(hidden, gain, mine, keys, values, nd, nt, feat):
    rows, width = hidden.shape
    tile = min(TILE, rows)
    row = pl.BlockSpec((tile, width), lambda i: (i, 0))
    small = pl.BlockSpec((tile,) + keys.shape[1:], lambda i: (i, 0, 0))
    return pl.pallas_call(
        functools.partial(finish_kernel, nd, nt, feat),
        grid=(rows // tile,),
        in_specs=[
            row, pl.BlockSpec((1, width), lambda i: (0, 0)),
            pl.BlockSpec((nt, nd, tile, feat), lambda i: (0, 0, i, 0)), small, small,
        ],
        out_specs=[row, row, small, small],
        out_shape=[jax.ShapeDtypeStruct((rows, width), BF)] * 2 + [jax.ShapeDtypeStruct(keys.shape, BF)] * 2,
        scratch_shapes=[pltpu.VMEM((tile, width), F32), pltpu.VMEM((tile, 128), F32)],
        cost_estimate=pl.CostEstimate(flops=rows * width * 20, bytes_accessed=8 * rows * width, transcendentals=0),
    )(hidden, gain.reshape(1, width), mine, keys, values)


def flip(i, mask):
    for b in (1, 2, 4, 8, 16, 32, 64):
        if mask & b:
            i = i + b - 2 * b * ((i // b) % 2)
    return i


def send(src, dst, ssem, rsem, where):
    pltpu.make_async_remote_copy(
        src_ref=src, dst_ref=dst, send_sem=ssem, recv_sem=rsem,
        device_id=where, device_id_type=pl.DeviceIdType.MESH,
    ).start()


def await_sent(ref, sem):
    pltpu.make_async_remote_copy(
        src_ref=ref, dst_ref=ref, send_sem=sem, recv_sem=sem,
        device_id={"dp": lax.axis_index("dp")}, device_id_type=pl.DeviceIdType.MESH,
    ).wait_send()


def await_into(dst, sem):
    pltpu.make_async_remote_copy(
        src_ref=dst, dst_ref=dst, send_sem=sem, recv_sem=sem,
        device_id={"dp": lax.axis_index("dp")}, device_id_type=pl.DeviceIdType.MESH,
    ).wait_recv()


def greet(nd, nt):
    me, ten = lax.axis_index("dp"), lax.axis_index("tensor")
    peers = sorted(set(bits_of(nt)) | set(range(2, nt, 2)))
    barrier = pltpu.get_barrier_semaphore()
    for m in range(1, nd):
        pl.semaphore_signal(
            barrier, inc=1, device_id={"dp": flip(me, m)}, device_id_type=pl.DeviceIdType.MESH
        )
    for b in peers:
        pl.semaphore_signal(
            barrier, inc=1, device_id={"tensor": flip(ten, b)}, device_id_type=pl.DeviceIdType.MESH
        )
    pl.semaphore_wait(barrier, nd - 1 + len(peers))


def inputs_part(nd, nt, prefetch, late, ready, prepare, place_columns, hidden_ref, gain_ref, q_ref, k_ref, v_ref, *scratch):
    wf, wsend, w2, araw, an, srow, sall, even, away, gotc = scratch[:10]
    hops = bits_of(nd)[1:]
    H = len(hops)
    snd, rcv = scratch[10 : 10 + H], scratch[10 + H : 10 + 2 * H]
    zsnd, zrcv, ls, wr, ar, sr, cr, hr, zr, sent = scratch[10 + 2 * H :]
    me, ten = lax.axis_index("dp"), lax.axis_index("tensor")
    rows, width = hidden_ref.shape
    feat = q_ref.shape[0]
    wide = w2.shape[-1]
    qc, kc = q_ref.shape[1] // nt, k_ref.shape[1] // nt
    keep = list(range(0, nt, 2))[::-1]
    spans = [(q_ref, qc, j) for j in range(qc // wide)]
    spans += [(w, kc, j) for w in (k_ref, v_ref) for j in range(kc // wide)]
    chunks = [(s, n) for s in keep for n in range(len(spans))]
    evens = list(range(0, nd, 2))
    orders = (hops, hops[::-1])
    def load(c, e):
        s, n = chunks[c]
        ref, size, j = spans[n]
        at = pl.ds(pl.multiple_of(flip(ten, s | e) * size + j * wide, wide), wide)
        return pltpu.make_async_copy(ref.at[:, at], wf.at[e, c], ls.at[c if e else len(chunks)])

    prefetch()
    for e in (1, 0):
        for c in range(len(chunks)):
            load(c, e).start()
    late()
    greet(nd, nt)
    ready()

    def features(m, e):
        return pl.ds(pl.multiple_of((flip(me, m) * nt + flip(ten, e)) * feat, feat), feat)

    far_first = sorted(range(1, nd), key=lambda m: (-bin(m >> 1).count("1"), m))
    for m in far_first:
        for e in (0, 1):
            send(
                hidden_ref.at[:, features(m, e)], araw.at[m, e],
                sent.at[0], ar.at[m], {"dp": flip(me, m)},
            )
    for c in range(len(chunks)):
        load(c, 1).wait()
        wsend[c] = wf[1, c].astype(BF)
        send(wsend.at[c], w2.at[c, 1], sent.at[1], wr.at[c], {"tensor": flip(ten, 1)})

    step = 512

    def squares(i, acc):
        h = hidden_ref[:, pl.ds(pl.multiple_of(i * step, step), step)].astype(F32)
        h = h * h
        for j in range(0, step, 128):
            acc = acc + h[:, j : j + 128]
        return acc

    acc = lax.fori_loop(0, width // step, squares, jnp.zeros((rows, 128), F32))
    scale = lax.rsqrt(jnp.sum(acc, axis=-1, keepdims=True) / width + epsilon)
    scale = jnp.broadcast_to(scale, (rows, 128))
    srow[...] = scale.T[:8]
    for m in far_first:
        send(srow, sall.at[m], sent.at[2], sr.at[m], {"dp": flip(me, m)})
    pltpu.make_async_copy(wf.at[0], wf.at[0], ls.at[len(chunks)]).wait()
    for c in range(len(chunks)):
        w2[c, 0] = wf[0, c].astype(BF)
    prepare()

    def normalise(raw, scale, e):
        out = []
        for j in range(0, feat, 128):
            at = pl.ds(pl.multiple_of((me * nt + flip(ten, e)) * feat + j, 128), 128)
            out.append((raw[:, j : j + 128].astype(F32) * scale * gain_ref[:, at]).astype(BF))
        return jnp.concatenate(out, axis=1)

    for e in (0, 1):
        an[e, 0, 0] = normalise(hidden_ref[:, features(0, e)], scale, e)
    for m in range(1, nd):
        await_into(sall.at[m], sr.at[m])
        other = jnp.broadcast_to(sall[m][:1], (128, rows)).T
        await_into(araw.at[m], ar.at[m])
        for e in (0, 1):
            an[e, m % 2, m // 2] = normalise(araw[m, e], other, e)

    half = rows // 2
    parts = [slice(h * half, (h + 1) * half) for h in (0, 1)]

    def place(h):
        order = orders[h]
        return [sum(b for i, b in enumerate(order) if p >> (H - 1 - i) & 1) for p in range(len(evens))]

    def product(c, odd):
        out = None
        for e in (0, 1):
            lhs = an[e, odd].reshape(len(evens) * rows, feat)
            term = jnp.dot(lhs, w2[c, e], preferred_element_type=F32)
            out = term if out is None else out + term
        return out.reshape(len(evens), rows, wide)

    def begin(c):
        await_into(w2.at[c, 1], wr.at[c])
        out = product(c, 1).astype(BF)
        for h in (0, 1):
            for p, m in enumerate(place(h)):
                away[c, p, parts[h]] = out[m // 2, parts[h]]
        send(away.at[c], gotc.at[c], sent.at[3], cr.at[c], {"dp": flip(me, 1)})
        out = product(c, 0)
        for h in (0, 1):
            for p, m in enumerate(place(h)):
                even[c, p, parts[h]] = out[m // 2, parts[h]]

    def hop(c, l):
        g = len(evens) >> l
        if l == 0:
            await_into(gotc.at[c], cr.at[c])
            got = gotc[c]
        else:
            await_into(rcv[l - 1].at[c], hr.at[c, l - 1])
            got = rcv[l - 1][c]
        if l < H:
            g //= 2
            even[c, :g] = even[c, :g] + got[:g].astype(F32)
            snd[l][c] = (even[c, g : 2 * g] + got[g:].astype(F32)).astype(BF)
            for h in (0, 1):
                part = pl.ds(h * half, half)
                send(
                    snd[l].at[c, :, part], rcv[l].at[c, :, part],
                    sent.at[5 + l], hr.at[c, l], {"dp": flip(me, orders[h][l])},
                )
            return
        done = even[c, 0] + got[0].astype(F32)
        s, n = chunks[c]
        if s:
            zsnd[c] = done.astype(BF)
            held.append(c)
            if n < len(spans) // 2:
                cross()
        else:
            even[c, 0] = done

    def cross():
        for c in held:
            send(zsnd.at[c], zrcv.at[c], sent.at[4], zr.at[c], {"tensor": flip(ten, chunks[c][0])})
        held.clear()

    def settle(c):
        n, done = chunks[c][1], even[c, 0]
        for other, (t, at) in enumerate(chunks):
            if t and at == n:
                await_into(zrcv.at[other], zr.at[other])
                done = done + zrcv[other].astype(F32)
        place_columns(n * wide, done)

    held = []
    lags = [1 + 3 * l for l in range(H + 1)]
    final = max(lags[-1] + 1, len(spans) + 1)
    for i in range(len(chunks) + final):
        if 0 <= i - final < len(chunks) and not chunks[i - final][0]:
            settle(i - final)
        for l in range(H, -1, -1):
            c = i - lags[l]
            if 0 <= c < len(chunks):
                hop(c, l)
        if i < len(chunks):
            begin(i)
        if i >= len(chunks) - 1:
            cross()
    crossing = sum(1 for c, _ in chunks if c)
    done = [(araw.at[pl.ds(1, nd - 1)], 0), (wsend, 1), (sall.at[pl.ds(1, nd - 1)], 2)]
    done += [(away, 3), (zsnd.at[pl.ds(0, crossing)], 4)]
    done += [(snd[l], 5 + l) for l in range(H)]
    return [(ref, sent.at[k]) for ref, k in done]


def project_part(nd, nt, attend_part, fin, att, prod, wt, acc, zr, dr, pr, fr, sent):
    me, ten = lax.axis_index("dp"), lax.axis_index("tensor")
    rows = att.shape[2]
    half = rows // 2
    evens = list(range(0, nd, 2))
    high, zbits = bits_of(nd)[1:], bits_of(nt)[::-1]
    levels = [[m for m in evens if bin(m).count("1") == k] for k in range(len(high) + 1)]
    pairs = [[n for m in level for n in (m, m + 1)] for level in levels]
    slot = {m: k for k, m in enumerate(m for group in pairs for m in group)}
    orders = (high + [1], high[::-1] + [1])
    waves = [[s for s in range(nt) if bin(s).count("1") == k][::-1] for k in range(1, len(zbits) + 1)]
    walk = [0] + [s for wave in waves for s in wave]
    def block(m, s):
        return att.at[s, slot[m]]

    def z_sends(s, h):
        part = pl.ds(h * half, half)
        for b in zbits:
            if b < (s & -s) or s == 0:
                send(
                    block(0, s).at[part], att.at[s | b, 0, part],
                    sent.at[0], zr.at[s | b, h], {"tensor": flip(ten, b)},
                )

    def dp_sends(m, s, h, bits):
        order = orders[h]
        used = [order.index(b) for b in order if m & b]
        for b in order[max(used) + 1 if used else 0 :]:
            if b in bits:
                part = pl.ds(h * half, half)
                send(
                    block(m, s).at[part], att.at[s, slot[m | b], part],
                    sent.at[1], dr.at[s, m | b], {"dp": flip(me, b)},
                )

    def arrive(m, s):
        await_into(att.at[s, slot[m]], dr.at[s, m])

    def near(level, s):
        for m in levels[level]:
            arrive(m, s)
            for h in (0, 1):
                dp_sends(m, s, h, [1])

    def far(level, s):
        for h in (0, 1):
            for m in levels[level]:
                dp_sends(m, s, h, high)

    def relay(level, s):
        near(level, s)
        far(level, s)

    def partial(level, s):
        ms = pairs[level]
        for m in ms[1::2]:
            arrive(m, s)
        first, group = slot[ms[0]], len(ms)
        lhs = att[s, first : first + group].reshape(group * rows, -1)
        term = jnp.dot(lhs, wt[s], preferred_element_type=F32)
        if s == 0:
            acc[: group * rows] = term
        elif s != walk[-1]:
            acc[: group * rows] += term
        else:
            out = acc[: group * rows] + term
            prod[pl.ds(first, group)] = out.astype(BF).reshape(group, rows, -1)
            for m in ms:
                if m:
                    send(prod.at[slot[m]], fin.at[0, m], sent.at[2], pr.at[m], {"dp": flip(me, m)})

    def done_at(s, m):
        return fr.at[nd * (passing.index(s) if s in passing else len(passing)) + (m if s in passing else ending.index(s))]

    def spread(m, s):
        for b in zbits:
            if b < (s & -s) or s == 0:
                send(fin.at[s, m], fin.at[s | b, m], sent.at[3], done_at(s | b, m), {"tensor": flip(ten, b)})

    def own_results(ms):
        for m in ms:
            if m:
                await_into(fin.at[0, m], pr.at[m])
                spread(m, 0)

    passing = [s for s in walk[1:] if not s & 1]
    ending = [s for s in range(1, nt) if s & 1]

    def pass_on(ms):
        for s in passing:
            for m in ms:
                await_into(fin.at[s, m], done_at(s, m))
                spread(m, s)

    for h in (0, 1):
        for q in (0, 1):
            attend_part(2 * h + q)
            part = pl.ds((2 * h + q) * (half // 2), half // 2)
            for b in zbits:
                send(block(0, 0).at[part], att.at[b, 0, part], sent.at[0], zr.at[b, h], {"tensor": flip(ten, b)})
        dp_sends(0, 0, h, high + [1])
    for wave in waves:
        for h in (0, 1):
            for s in wave:
                await_into(att.at[s, 0, pl.ds(h * half, half)], zr.at[s, h])
                z_sends(s, h)
                dp_sends(0, s, h, high + [1])

    for s in walk:
        partial(0, s)
    fin[0, 0] = prod[0]
    spread(0, 0)
    relay(1, walk[0])
    own_results(pairs[0])
    for level in range(1, len(levels)):
        for s in walk[1:-1] if level == 1 else walk[:-1]:
            near(level, s)
        for s in walk[:-1]:
            partial(level, s)
        behind = pairs[level - 1]
        cut = len(behind) if level == 1 else len(behind) // 2
        pass_on(behind[:cut])
        near(level, walk[-1])
        partial(level, walk[-1])
        for s in walk[1:] if level == 1 else walk:
            far(level, s)
        pass_on(behind[cut:])
        own_results(pairs[level])
    pass_on(pairs[-1])
    for s in ending:
        await_into(fin.at[s], done_at(s, 0))
    one, rest = pl.ds(1, nt - 1), pl.ds(1, nd - 1)
    done = [(att.at[one, 0], 0), (att.at[:, rest], 1), (prod.at[rest], 2), (fin.at[one], 3)]
    return [(ref, sent.at[k]) for ref, k in done]


def block_kernel(nd, nt, refs_in, refs_out, inner, attn, outer):
    rows_ref, gain_ref, lens_ref, q_ref, k_ref, v_ref, o_ref, keys_ref, vals_ref = refs_in
    fin, fresh_ref, new_ref = refs_out
    hidden_ref, kept_keys, kept_vals, turn, qf, kf, vf, lf, of, kvs, ows = attn
    att, wt = outer[0], outer[2]
    ten = lax.axis_index("tensor")
    rows, heads = qf.shape[:2]
    qc, kc = q_ref.shape[1] // nt, k_ref.shape[1] // nt
    group = qc // kc
    wf = inner[0]
    feat, wide = wf.shape[2:]
    caches = [
        pltpu.make_async_copy(keys_ref, kept_keys, kvs.at[0]),
        pltpu.make_async_copy(vals_ref, kept_vals, kvs.at[1]),
    ]
    pieces = [(s, j) for s in range(nt) for j in range(qc // wide)]

    def out_load(i):
        s, j = pieces[i]
        at = pl.ds(pl.multiple_of(flip(ten, s) * qc + j * wide, wide), wide)
        return pltpu.make_async_copy(o_ref.at[:, at], wf.at[0, i] if i < wf.shape[1] else wf.at[1, i - wf.shape[1]], ows.at[0])

    row_copy = pltpu.make_async_copy(rows_ref, hidden_ref, kvs.at[2])

    def prefetch():
        row_copy.start()

    def late():
        for copy in caches:
            copy.start()

    def ready():
        row_copy.wait()

    def prepare():
        for i in range(len(pieces)):
            out_load(i).start()
        half_dim = HEAD_DIM // 2
        lens = jnp.broadcast_to(lens_ref[...].astype(F32), (HEAD_DIM, rows)).T
        lane = lax.broadcasted_iota(jnp.int32, (rows, HEAD_DIM), 1)
        low = lane < half_dim
        index = jnp.where(low, lane, lane - half_dim).astype(F32)
        angle = lens * jnp.exp(-math.log(rope_base) * index / half_dim)
        turn[0] = jnp.cos(angle)
        turn[1] = jnp.where(low, -jnp.sin(angle), jnp.sin(angle))
        for h in range(heads):
            lf[:, h, :] = lens
        pltpu.make_async_copy(o_ref, o_ref, ows.at[0]).wait()
        for i, (s, j) in enumerate(pieces):
            w = wf[0, i] if i < wf.shape[1] else wf[1, i - wf.shape[1]]
            wt[s, j * wide : (j + 1) * wide] = w.T.astype(BF)

    def place_columns(first, total):
        for j in range(0, total.shape[1], HEAD_DIM):
            x, at = total[:, j : j + HEAD_DIM], first + j
            if at < qc + kc:
                x = x * turn[0] + pltpu.roll(x, HEAD_DIM // 2, 1) * turn[1]
            x = x.astype(BF)
            if at < qc:
                qf[:, at // HEAD_DIM, :] = x.astype(F32)
                continue
            to, full, off = (fresh_ref, kf, at - qc) if at < qc + kc else (new_ref, vf, at - qc - kc)
            g = off // HEAD_DIM
            to[:, g, :] = x.astype(F32)
            for h in range(g * group, (g + 1) * group):
                full[:, h, :] = x.astype(F32)

    def attend_part(part):
        if part == 0:
            for copy in caches:
                copy.wait()
        kinds = kc // HEAD_DIM
        step, span = 32, kept_keys.shape[1]
        shape = (step, heads, span)
        spot = lax.broadcasted_iota(jnp.int32, shape, 2)
        mine = spot % kinds == lax.broadcasted_iota(jnp.int32, shape, 1) // group
        where = (spot // kinds).astype(F32)
        root = 1.0 / math.sqrt(HEAD_DIM)

        def some(i, carry):
            at = pl.ds(pl.multiple_of(part * (rows // 4) + i * step, step), step)
            q = qf[at]
            scores = root * lax.dot_general(
                q.astype(BF), kept_keys[at], (((2,), (2,)), ((0,), (0,))), preferred_element_type=F32
            )
            own = jnp.sum(q * kf[at], axis=-1, keepdims=True) * root
            scores = jnp.where(mine & (where < lf[at][:, :, :1]), scores, -jnp.inf)
            largest = jnp.maximum(jnp.max(scores, axis=-1, keepdims=True), own)
            kept = jnp.exp(scores - largest)
            own = jnp.exp(own - largest)
            divisor = jnp.sum(kept, axis=-1, keepdims=True) + own
            out = lax.dot_general(
                (kept / divisor).astype(BF), kept_vals[at],
                (((2,), (1,)), ((0,), (0,))), preferred_element_type=F32,
            )
            of[at] = out + (own / divisor).astype(BF).astype(F32) * vf[at]
            return carry

        lax.fori_loop(0, rows // 4 // step, some, 0)
        here = slice(part * (rows // 4), (part + 1) * (rows // 4))
        for h in range(heads):
            att[0, 0, here, h * HEAD_DIM : (h + 1) * HEAD_DIM] = of[here, h, :].astype(BF)

    sent = inputs_part(nd, nt, prefetch, late, ready, prepare, place_columns, hidden_ref, gain_ref, q_ref, k_ref, v_ref, *inner)
    sent += project_part(nd, nt, attend_part, fin, *outer)
    for ref, sem in sent:
        await_sent(ref, sem)


def block(hidden, gain, lengths, weights, key_cache, value_cache, nd, nt):
    rows, width = hidden.shape
    q_weight, k_weight, o_weight = weights[0], weights[1], weights[3]
    feat, wide = q_weight.shape[0], 256
    qc, kc = q_weight.shape[1] // nt, k_weight.shape[1] // nt
    heads = qc // HEAD_DIM
    C, half, H = (qc + 2 * kc) // wide * (nt // 2), nd // 2, nd.bit_length() - 2
    dma, vm = pltpu.SemaphoreType.DMA, pltpu.VMEM
    hop_bufs = [vm((C, half >> (l + 1), rows, wide), BF) for l in range(H)]
    in_place = pl.BlockSpec(memory_space=pltpu.VMEM)
    outside = pl.BlockSpec(memory_space=pl.ANY)
    span = key_cache.shape[1] * key_cache.shape[2]
    caches = [x.reshape(rows, span, HEAD_DIM) for x in (key_cache, value_cache)]
    inner = [
        vm((2, C, feat, wide), F32),
        vm((C, feat, wide), BF),
        vm((C, 2, feat, wide), BF),
        vm((nd, 2, rows, feat), BF),
        vm((2, 2, half, rows, feat), BF),
        vm((8, rows), F32),
        vm((nd, 8, rows), F32),
        vm((C, half, rows, wide), F32),
        vm((C, half, rows, wide), BF),
        vm((C, half, rows, wide), BF),
        *hop_bufs,
        *hop_bufs,
        vm((C, rows, wide), BF),
        vm((C, rows, wide), BF),
        dma((C + 1,)), dma((C,)), dma((nd,)), dma((nd,)), dma((C,)), dma((C, H)), dma((C,)), dma((5 + H,)),
    ]
    by_head = [vm((rows, heads, HEAD_DIM), F32)] * 5
    attn = [
        vm((rows, width), BF),
        vm((rows, span, HEAD_DIM), BF), vm((rows, span, HEAD_DIM), BF),
        vm((2, rows, HEAD_DIM), F32), *by_head, dma((3,)), dma((1,)),
    ]
    outer = [
        vm((nt, nd, rows, qc), BF),
        vm((nd, rows, feat), BF),
        vm((nt, qc, feat), BF),
        vm((nd // 2 * rows, feat), F32),
        dma((nt, 2)), dma((nt, nd)), dma((nd,)), dma((nd * (nt // 2),)), dma((4,)),
    ]
    ends = [9, 12, 12 + len(inner), 12 + len(inner) + len(attn)]

    def kernel(*refs):
        block_kernel(
            nd, nt, refs[: ends[0]], refs[ends[0] : ends[1]],
            refs[ends[1] : ends[2]], refs[ends[2] : ends[3]], refs[ends[3] :],
        )

    return pl.pallas_call(
        kernel,
        in_specs=[outside] + [in_place] * 2 + [outside] * 6,
        out_specs=[in_place] * 3,
        out_shape=[
            jax.ShapeDtypeStruct((nt, nd, rows, feat), BF),
            jax.ShapeDtypeStruct((rows, kc // HEAD_DIM, HEAD_DIM), F32),
            jax.ShapeDtypeStruct((rows, kc // HEAD_DIM, HEAD_DIM), F32),
        ],
        scratch_shapes=inner + attn + outer,
        compiler_params=pltpu.CompilerParams(
            collective_id=1, has_side_effects=True, vmem_limit_bytes=63 * 1024 * 1024
        ),
    )(hidden, gain.reshape(1, width), lengths.reshape(1, rows), *weights, *caches)


def shards(
    hidden,
    q_weight,
    k_weight,
    v_weight,
    o_weight,
    input_gain,
    post_gain,
    key_cache,
    value_cache,
    lengths,
):
    nt = lax.axis_size("tensor")
    nd = lax.axis_size("dp")
    me, ten = lax.axis_index("dp"), lax.axis_index("tensor")
    rows, width = hidden.shape
    heads_here, kv_here = HEADS // nt, KV_HEADS // nt
    qc, kc = heads_here * HEAD_DIM, kv_here * HEAD_DIM
    feat = q_weight.shape[0]
    low, high = [1], bits_of(nd)[1:]
    orders = (low + high, low + high[::-1])
    odd = [m for m in range(nd) if m & 1]
    even = [m for m in range(nd) if not m & 1]
    count = rows // CHUNKS

    def columns(w, s, n):
        return lax.dynamic_slice_in_dim(w, (ten ^ s) * n, n, 1).astype(BF)

    together = feat % 128 == 0 and kc % 256 == 0 and rows == 128 and nt > 1 and nd > 2 and CHUNKS == 1
    together = together and kv_here * key_cache.shape[1] == 128 and heads_here == 8
    if together:
        weights = (q_weight, k_weight, v_weight, o_weight)
        mine, keys, news = block(hidden, input_gain, lengths, weights, key_cache, value_cache, nd, nt)
        return tuple(finish(hidden, post_gain, mine, keys, news, nd, nt, feat))
    pieces = norm_pieces(hidden, input_gain, nd, nt, feat)
    pieces = [swap(p, "dp", m, nd) if m else p for m, p in enumerate(pieces)]
    w_in = [
        jnp.concatenate(
            [columns(q_weight, s, qc), columns(k_weight, s, kc), columns(v_weight, s, kc)], axis=1
        )
        for s in range(nt)
    ]
    w_out = [columns(o_weight, s, qc) for s in range(nt)]

    fresh, values, outs = [], [], None
    for c in range(CHUNKS):
        r0 = c * count
        cut = [p[r0 : r0 + count] for p in pieces]
        lhs_odd = jnp.concatenate([cut[m] for m in odd])
        lhs_even = jnp.concatenate([cut[m] for m in even])
        total, behind = None, []
        for k, s in enumerate(reversed(range(nt))):
            if k and k % 2 == 0:
                held = lax.optimization_barrier((lhs_odd, lhs_even, *behind))
                lhs_odd, lhs_even, behind = held[0], held[1], []
            away = jnp.dot(lhs_odd, w_in[s], preferred_element_type=F32).astype(BF)
            got = swap(away, "dp", 1, nd)
            behind.append(got)
            acc = jnp.dot(lhs_even, w_in[s], preferred_element_type=F32) + got.astype(F32)
            acc = acc.astype(BF).reshape(len(even), count, -1)
            parts = {m: acc[j] for j, m in enumerate(even)}
            part = scatter_sum(parts, orders[k % 2][1:], "dp", nd)
            part = (swap(part, "tensor", s, nt) if s else part).astype(F32)
            total = part if total is None else total + part
        query, key_part, value_part = total[:, :qc], total[:, qc : qc + kc], total[:, qc + kc :]

        here = slice(r0, r0 + count)
        query_b = rotate(query.reshape(count, heads_here, HEAD_DIM), lengths[here]).astype(BF)
        keys = rotate(key_part.reshape(count, kv_here, HEAD_DIM), lengths[here]).astype(BF)
        news = value_part.reshape(count, kv_here, HEAD_DIM).astype(BF)
        fresh.append(keys)
        values.append(news)
        attended = attend(
            query_b, keys, news, key_cache[here], value_cache[here], lengths[here]
        )

        by_tensor = gather_all(attended, bits_of(nt)[::-1], "tensor", nt)
        product = None
        for k, s in enumerate(sorted(by_tensor, key=lambda s: (s & 1, s))):
            blocks = gather_all(by_tensor[s], orders[k % 2][1:] + low, "dp", nd)
            lhs = jnp.concatenate([blocks[m] for m in range(nd)])
            term = lax.dot_general(
                lhs, w_out[s], (((1,), (1,)), ((), ())), preferred_element_type=F32
            )
            product = term if product is None else product + term
        product = product.astype(BF).reshape(nd, count, feat)
        mine = jnp.stack([swap(product[m], "dp", m, nd) if m else product[0] for m in range(nd)])
        for b in bits_of(nd):
            v = mine.reshape(nd // (2 * b), 2, b, count, feat)
            mine = jnp.where((me & b) != 0, v[:, ::-1], v).reshape(nd, count, feat)
        mine = mine[None]
        for b in bits_of(nt)[::-1]:
            got = swap(mine, "tensor", b, nt)
            first = jnp.where((ten & b) != 0, got, mine)
            second = jnp.where((ten & b) != 0, mine, got)
            mine = jnp.stack([first, second], axis=1).reshape((-1,) + mine.shape[1:])
        mixed = mine.transpose(2, 1, 0, 3).reshape(count, width).astype(F32)
        residual = hidden[here].astype(F32) + mixed
        pair = (residual.astype(BF), rms_gain(residual, post_gain).astype(BF))
        outs = pair if outs is None else tuple(jnp.concatenate(z) for z in zip(outs, pair))
    return (outs[0], outs[1], jnp.concatenate(fresh), jnp.concatenate(values))


def solution(mesh):
    in_specs = (
        P("dp", None),
        P(("dp", "tensor"), None),
        P(("dp", "tensor"), None),
        P(("dp", "tensor"), None),
        P(("dp", "tensor"), None),
        P(),
        P(),
        P("dp", None, "tensor", None),
        P("dp", None, "tensor", None),
        P("dp"),
    )
    out_specs = (P("dp", None), P("dp", None), P("dp", "tensor", None), P("dp", "tensor", None))
    return jax.shard_map(shards, mesh=mesh, in_specs=in_specs, out_specs=out_specs, check_vma=False)
```

```python
import functools
import math

import jax
import jax.numpy as jnp
from jax import lax
from jax.experimental import pallas as pl
from jax.experimental.pallas import tpu as pltpu
from jax.sharding import PartitionSpec as P

HEADS = 32
KV_HEADS = 8
HEAD_DIM = 128

CHUNKS = 1
TILE = 64

BF = jnp.bfloat16
F32 = jnp.float32

epsilon = 1e-05
rope_base = 500000.0


def rms_gain(values, gain_vector):
    mean_square = jnp.mean(values * values, axis=-1, keepdims=True)
    return values * lax.rsqrt(mean_square + epsilon) * gain_vector


def rotate(values, positions):
    half_dim = values.shape[-1] // 2
    index_row = jnp.arange(half_dim, dtype=jnp.float32)
    frequency = jnp.exp(-math.log(rope_base) * index_row / half_dim)
    angle = positions.astype(jnp.float32)[:, None, None] * frequency[None, None, :]
    first_half = values[..., :half_dim]
    second_half = values[..., half_dim:]
    return jnp.concatenate(
        [
            first_half * jnp.cos(angle) - second_half * jnp.sin(angle),
            second_half * jnp.cos(angle) + first_half * jnp.sin(angle),
        ],
        axis=-1,
    )


def attend(query_b, fresh_token_keys, new_values, key_cache, value_cache, lengths):
    row_count, kv_count = (fresh_token_keys.shape[0], fresh_token_keys.shape[1])
    grouped_heads = query_b.reshape(row_count, kv_count, -1, HEAD_DIM)
    reciprocal_root = 1.0 / math.sqrt(HEAD_DIM)
    scores = (
        jnp.einsum("bkgd,blkd->bkgl", grouped_heads, key_cache, preferred_element_type=jnp.float32)
        * reciprocal_root
    )
    self_token_score = (
        jnp.einsum(
            "lfxa,lfa->lfx", grouped_heads, fresh_token_keys, preferred_element_type=jnp.float32
        )
        * reciprocal_root
    )
    visible = jnp.arange(key_cache.shape[1], dtype=jnp.int32)[None, :] < lengths[:, None]
    scores = jnp.where(visible[:, None, None, :], scores, -jnp.inf)
    largest = jnp.maximum(jnp.max(scores, axis=-1), self_token_score)
    kept_exp = jnp.exp(scores - largest[..., None])
    own_exp = jnp.exp(self_token_score - largest)
    softmax_divisor = jnp.sum(kept_exp, axis=-1) + own_exp
    weights_kept = (kept_exp / softmax_divisor[..., None]).astype(jnp.bfloat16)
    own_weight = (own_exp / softmax_divisor).astype(jnp.bfloat16)
    attended = jnp.einsum(
        "bkgl,blkd->bkgd", weights_kept, value_cache, preferred_element_type=jnp.float32
    )
    attended = (
        attended
        + own_weight.astype(jnp.float32)[..., None] * new_values.astype(jnp.float32)[:, :, None, :]
    )
    return attended.reshape(row_count, -1).astype(jnp.bfloat16)


def swap(x, axis, mask, size):
    return lax.ppermute(x, axis, [(i, i ^ mask) for i in range(size)])


def add(a, b):
    return (a.astype(F32) + b.astype(F32)).astype(BF)


def bits_of(size):
    return [1 << k for k in range(size.bit_length() - 1)]


def scatter_sum(parts, bits, axis, size):
    for b in bits:
        up = sorted(m for m in parts if m & b)
        got = swap(jnp.stack([parts[m] for m in up]), axis, b, size)
        parts = {m: add(parts[m], got[up.index(m | b)]) for m in parts if not m & b}
    return parts[0]


def gather_all(x, bits, axis, size):
    held = {0: x}
    for b in bits:
        keys = sorted(held)
        got = swap(jnp.stack([held[m] for m in keys]), axis, b, size)
        held.update({m | b: got[k] for k, m in enumerate(keys)})
    return held


def norm_pieces_kernel(nd, nt, feat, hidden_ref, gain_ref, *outs):
    me, ten = lax.axis_index("dp"), lax.axis_index("tensor")
    h = hidden_ref[...].astype(F32)
    scale = lax.rsqrt(jnp.mean(h * h, axis=-1, keepdims=True) + epsilon)
    for m in range(nd):
        at = pl.ds(pl.multiple_of(((me ^ m) * nt + ten) * feat, feat), feat)
        outs[m][...] = (hidden_ref[:, at].astype(F32) * scale * gain_ref[:, at]).astype(BF)


def norm_pieces(hidden, gain, nd, nt, feat):
    rows, width = hidden.shape
    if feat % 128:
        me, ten = lax.axis_index("dp"), lax.axis_index("tensor")
        normal_in = rms_gain(hidden.astype(F32), gain).astype(BF)
        return [
            lax.dynamic_slice_in_dim(normal_in, ((me ^ m) * nt + ten) * feat, feat, 1)
            for m in range(nd)
        ]
    tile = min(32, rows)
    return pl.pallas_call(
        functools.partial(norm_pieces_kernel, nd, nt, feat),
        grid=(rows // tile,),
        in_specs=[
            pl.BlockSpec((tile, width), lambda i: (i, 0)),
            pl.BlockSpec((1, width), lambda i: (0, 0)),
        ],
        out_specs=[pl.BlockSpec((tile, feat), lambda i: (i, 0))] * nd,
        out_shape=[jax.ShapeDtypeStruct((rows, feat), BF)] * nd,
        cost_estimate=pl.CostEstimate(flops=rows * width * 20, bytes_accessed=4 * rows * width, transcendentals=0),
    )(hidden, gain.reshape(1, width))


def finish_kernel(nd, nt, feat, hidden_ref, gain_ref, ref, keys_ref, values_ref, new_ref, normed_ref, k_ref, v_ref, res, squares):
    me, ten = lax.axis_index("dp"), lax.axis_index("tensor")
    k_ref[...] = keys_ref[...].astype(BF)
    v_ref[...] = values_ref[...].astype(BF)
    total = jnp.zeros(squares.shape, F32)
    for s in range(nt):
        for m in range(nd):
            col = ((me ^ m) * nt + (ten ^ s)) * feat
            at = pl.ds(pl.multiple_of(col, feat), feat)
            r = hidden_ref[:, at].astype(F32) + ref[s, m].astype(F32)
            new_ref[:, at] = r.astype(BF)
            res[:, at] = r
            r = r * r
            for j in range(0, feat, 128):
                total = total + r[:, j : j + 128]
    mean = jnp.sum(total, axis=-1, keepdims=True) / res.shape[1]
    normed_ref[...] = (res[...] * lax.rsqrt(mean + epsilon) * gain_ref[...]).astype(BF)


def finish(hidden, gain, mine, keys, values, nd, nt, feat):
    rows, width = hidden.shape
    tile = min(TILE, rows)
    row = pl.BlockSpec((tile, width), lambda i: (i, 0))
    small = pl.BlockSpec((tile,) + keys.shape[1:], lambda i: (i, 0, 0))
    return pl.pallas_call(
        functools.partial(finish_kernel, nd, nt, feat),
        grid=(rows // tile,),
        in_specs=[
            row, pl.BlockSpec((1, width), lambda i: (0, 0)),
            pl.BlockSpec((nt, nd, tile, feat), lambda i: (0, 0, i, 0)), small, small,
        ],
        out_specs=[row, row, small, small],
        out_shape=[jax.ShapeDtypeStruct((rows, width), BF)] * 2 + [jax.ShapeDtypeStruct(keys.shape, BF)] * 2,
        scratch_shapes=[pltpu.VMEM((tile, width), F32), pltpu.VMEM((tile, 128), F32)],
        cost_estimate=pl.CostEstimate(flops=rows * width * 20, bytes_accessed=8 * rows * width, transcendentals=0),
    )(hidden, gain.reshape(1, width), mine, keys, values)


def flip(i, mask):
    for b in (1, 2, 4, 8, 16, 32, 64):
        if mask & b:
            i = i + b - 2 * b * ((i // b) % 2)
    return i


def send(src, dst, ssem, rsem, where):
    pltpu.make_async_remote_copy(
        src_ref=src, dst_ref=dst, send_sem=ssem, recv_sem=rsem,
        device_id=where, device_id_type=pl.DeviceIdType.MESH,
    ).start()


def await_sent(ref, sem):
    pltpu.make_async_remote_copy(
        src_ref=ref, dst_ref=ref, send_sem=sem, recv_sem=sem,
        device_id={"dp": lax.axis_index("dp")}, device_id_type=pl.DeviceIdType.MESH,
    ).wait_send()


def await_into(dst, sem):
    pltpu.make_async_remote_copy(
        src_ref=dst, dst_ref=dst, send_sem=sem, recv_sem=sem,
        device_id={"dp": lax.axis_index("dp")}, device_id_type=pl.DeviceIdType.MESH,
    ).wait_recv()


def greet(nd, nt):
    me, ten = lax.axis_index("dp"), lax.axis_index("tensor")
    peers = sorted(set(bits_of(nt)) | set(range(2, nt, 2)))
    barrier = pltpu.get_barrier_semaphore()
    for m in range(1, nd):
        pl.semaphore_signal(
            barrier, inc=1, device_id={"dp": flip(me, m)}, device_id_type=pl.DeviceIdType.MESH
        )
    for b in peers:
        pl.semaphore_signal(
            barrier, inc=1, device_id={"tensor": flip(ten, b)}, device_id_type=pl.DeviceIdType.MESH
        )
    pl.semaphore_wait(barrier, nd - 1 + len(peers))


def inputs_part(nd, nt, prefetch, late, ready, prepare, place_columns, hidden_ref, gain_ref, q_ref, k_ref, v_ref, *scratch):
    wf, wsend, w2, araw, an, srow, sall, even, away, gotc = scratch[:10]
    hops = bits_of(nd)[1:]
    H = len(hops)
    snd, rcv = scratch[10 : 10 + H], scratch[10 + H : 10 + 2 * H]
    zsnd, zrcv, ls, wr, ar, sr, cr, hr, zr, sent = scratch[10 + 2 * H :]
    me, ten = lax.axis_index("dp"), lax.axis_index("tensor")
    rows, width = hidden_ref.shape
    feat = q_ref.shape[0]
    wide = w2.shape[-1]
    qc, kc = q_ref.shape[1] // nt, k_ref.shape[1] // nt
    keep = list(range(0, nt, 2))[::-1]
    spans = [(q_ref, qc, j) for j in range(qc // wide)]
    spans += [(w, kc, j) for w in (k_ref, v_ref) for j in range(kc // wide)]
    chunks = [(s, n) for s in keep for n in range(len(spans))]
    evens = list(range(0, nd, 2))
    orders = (hops, hops[::-1])
    def load(c, e):
        s, n = chunks[c]
        ref, size, j = spans[n]
        at = pl.ds(pl.multiple_of(flip(ten, s | e) * size + j * wide, wide), wide)
        return pltpu.make_async_copy(ref.at[:, at], wf.at[e, c], ls.at[c if e else len(chunks)])

    prefetch()
    for e in (1, 0):
        for c in range(len(chunks)):
            load(c, e).start()
    late()
    greet(nd, nt)
    ready()

    def features(m, e):
        return pl.ds(pl.multiple_of((flip(me, m) * nt + flip(ten, e)) * feat, feat), feat)

    far_first = sorted(range(1, nd), key=lambda m: (-bin(m >> 1).count("1"), m))
    for m in far_first:
        for e in (0, 1):
            send(
                hidden_ref.at[:, features(m, e)], araw.at[m, e],
                sent.at[0], ar.at[m], {"dp": flip(me, m)},
            )
    for c in range(len(chunks)):
        load(c, 1).wait()
        wsend[c] = wf[1, c].astype(BF)
        send(wsend.at[c], w2.at[c, 1], sent.at[1], wr.at[c], {"tensor": flip(ten, 1)})

    step = 512

    def squares(i, acc):
        h = hidden_ref[:, pl.ds(pl.multiple_of(i * step, step), step)].astype(F32)
        h = h * h
        for j in range(0, step, 128):
            acc = acc + h[:, j : j + 128]
        return acc

    acc = lax.fori_loop(0, width // step, squares, jnp.zeros((rows, 128), F32))
    scale = lax.rsqrt(jnp.sum(acc, axis=-1, keepdims=True) / width + epsilon)
    scale = jnp.broadcast_to(scale, (rows, 128))
    srow[...] = scale.T[:8]
    for m in far_first:
        send(srow, sall.at[m], sent.at[2], sr.at[m], {"dp": flip(me, m)})
    pltpu.make_async_copy(wf.at[0], wf.at[0], ls.at[len(chunks)]).wait()
    for c in range(len(chunks)):
        w2[c, 0] = wf[0, c].astype(BF)
    prepare()

    def normalise(raw, scale, e):
        out = []
        for j in range(0, feat, 128):
            at = pl.ds(pl.multiple_of((me * nt + flip(ten, e)) * feat + j, 128), 128)
            out.append((raw[:, j : j + 128].astype(F32) * scale * gain_ref[:, at]).astype(BF))
        return jnp.concatenate(out, axis=1)

    for e in (0, 1):
        an[e, 0, 0] = normalise(hidden_ref[:, features(0, e)], scale, e)
    for m in range(1, nd):
        await_into(sall.at[m], sr.at[m])
        other = jnp.broadcast_to(sall[m][:1], (128, rows)).T
        await_into(araw.at[m], ar.at[m])
        for e in (0, 1):
            an[e, m % 2, m // 2] = normalise(araw[m, e], other, e)

    half = rows // 2
    parts = [slice(h * half, (h + 1) * half) for h in (0, 1)]

    def place(h):
        order = orders[h]
        return [sum(b for i, b in enumerate(order) if p >> (H - 1 - i) & 1) for p in range(len(evens))]

    def product(c, odd):
        out = None
        for e in (0, 1):
            lhs = an[e, odd].reshape(len(evens) * rows, feat)
            term = jnp.dot(lhs, w2[c, e], preferred_element_type=F32)
            out = term if out is None else out + term
        return out.reshape(len(evens), rows, wide)

    def begin(c):
        await_into(w2.at[c, 1], wr.at[c])
        out = product(c, 1).astype(BF)
        for h in (0, 1):
            for p, m in enumerate(place(h)):
                away[c, p, parts[h]] = out[m // 2, parts[h]]
        send(away.at[c], gotc.at[c], sent.at[3], cr.at[c], {"dp": flip(me, 1)})
        out = product(c, 0)
        for h in (0, 1):
            for p, m in enumerate(place(h)):
                even[c, p, parts[h]] = out[m // 2, parts[h]]

    def hop(c, l):
        g = len(evens) >> l
        if l == 0:
            await_into(gotc.at[c], cr.at[c])
            got = gotc[c]
        else:
            await_into(rcv[l - 1].at[c], hr.at[c, l - 1])
            got = rcv[l - 1][c]
        if l < H:
            g //= 2
            even[c, :g] = even[c, :g] + got[:g].astype(F32)
            snd[l][c] = (even[c, g : 2 * g] + got[g:].astype(F32)).astype(BF)
            for h in (0, 1):
                part = pl.ds(h * half, half)
                send(
                    snd[l].at[c, :, part], rcv[l].at[c, :, part],
                    sent.at[5 + l], hr.at[c, l], {"dp": flip(me, orders[h][l])},
                )
            return
        done = even[c, 0] + got[0].astype(F32)
        s, n = chunks[c]
        if s:
            zsnd[c] = done.astype(BF)
            held.append(c)
            if n < len(spans) // 2:
                cross()
        else:
            even[c, 0] = done

    def cross():
        for c in held:
            send(zsnd.at[c], zrcv.at[c], sent.at[4], zr.at[c], {"tensor": flip(ten, chunks[c][0])})
        held.clear()

    def settle(c):
        n, done = chunks[c][1], even[c, 0]
        for other, (t, at) in enumerate(chunks):
            if t and at == n:
                await_into(zrcv.at[other], zr.at[other])
                done = done + zrcv[other].astype(F32)
        place_columns(n * wide, done)

    held = []
    lags = [1 + 3 * l for l in range(H + 1)]
    final = max(lags[-1] + 1, len(spans) + 1)
    for i in range(len(chunks) + final):
        if 0 <= i - final < len(chunks) and not chunks[i - final][0]:
            settle(i - final)
        for l in range(H, -1, -1):
            c = i - lags[l]
            if 0 <= c < len(chunks):
                hop(c, l)
        if i < len(chunks):
            begin(i)
        if i >= len(chunks) - 1:
            cross()
    crossing = sum(1 for c, _ in chunks if c)
    done = [(araw.at[pl.ds(1, nd - 1)], 0), (wsend, 1), (sall.at[pl.ds(1, nd - 1)], 2)]
    done += [(away, 3), (zsnd.at[pl.ds(0, crossing)], 4)]
    done += [(snd[l], 5 + l) for l in range(H)]
    return [(ref, sent.at[k]) for ref, k in done]


def project_part(nd, nt, attend_part, fin, att, prod, wt, acc, zr, dr, pr, fr, sent):
    me, ten = lax.axis_index("dp"), lax.axis_index("tensor")
    rows = att.shape[2]
    half = rows // 2
    evens = list(range(0, nd, 2))
    high, zbits = bits_of(nd)[1:], bits_of(nt)[::-1]
    levels = [[m for m in evens if bin(m).count("1") == k] for k in range(len(high) + 1)]
    pairs = [[n for m in level for n in (m, m + 1)] for level in levels]
    slot = {m: k for k, m in enumerate(m for group in pairs for m in group)}
    orders = (high + [1], high[::-1] + [1])
    waves = [[s for s in range(nt) if bin(s).count("1") == k][::-1] for k in range(1, len(zbits) + 1)]
    walk = [0] + [s for wave in waves for s in wave]
    def block(m, s):
        return att.at[s, slot[m]]

    def z_sends(s, h):
        part = pl.ds(h * half, half)
        for b in zbits:
            if b < (s & -s) or s == 0:
                send(
                    block(0, s).at[part], att.at[s | b, 0, part],
                    sent.at[0], zr.at[s | b, h], {"tensor": flip(ten, b)},
                )

    def dp_sends(m, s, h, bits):
        order = orders[h]
        used = [order.index(b) for b in order if m & b]
        for b in order[max(used) + 1 if used else 0 :]:
            if b in bits:
                part = pl.ds(h * half, half)
                send(
                    block(m, s).at[part], att.at[s, slot[m | b], part],
                    sent.at[1], dr.at[s, m | b], {"dp": flip(me, b)},
                )

    def arrive(m, s):
        await_into(att.at[s, slot[m]], dr.at[s, m])

    def near(level, s):
        for m in levels[level]:
            arrive(m, s)
            for h in (0, 1):
                dp_sends(m, s, h, [1])

    def far(level, s):
        for h in (0, 1):
            for m in levels[level]:
                dp_sends(m, s, h, high)

    def relay(level, s):
        near(level, s)
        far(level, s)

    def partial(level, s):
        ms = pairs[level]
        for m in ms[1::2]:
            arrive(m, s)
        first, group = slot[ms[0]], len(ms)
        lhs = att[s, first : first + group].reshape(group * rows, -1)
        term = jnp.dot(lhs, wt[s], preferred_element_type=F32)
        if s == 0:
            acc[: group * rows] = term
        elif s != walk[-1]:
            acc[: group * rows] += term
        else:
            out = acc[: group * rows] + term
            prod[pl.ds(first, group)] = out.astype(BF).reshape(group, rows, -1)
            for m in ms:
                if m:
                    send(prod.at[slot[m]], fin.at[0, m], sent.at[2], pr.at[m], {"dp": flip(me, m)})

    def done_at(s, m):
        return fr.at[nd * (passing.index(s) if s in passing else len(passing)) + (m if s in passing else ending.index(s))]

    def spread(m, s):
        for b in zbits:
            if b < (s & -s) or s == 0:
                send(fin.at[s, m], fin.at[s | b, m], sent.at[3], done_at(s | b, m), {"tensor": flip(ten, b)})

    def own_results(ms):
        for m in ms:
            if m:
                await_into(fin.at[0, m], pr.at[m])
                spread(m, 0)

    passing = [s for s in walk[1:] if not s & 1]
    ending = [s for s in range(1, nt) if s & 1]

    def pass_on(ms):
        for s in passing:
            for m in ms:
                await_into(fin.at[s, m], done_at(s, m))
                spread(m, s)

    for h in (0, 1):
        for q in (0, 1):
            attend_part(2 * h + q)
            part = pl.ds((2 * h + q) * (half // 2), half // 2)
            for b in zbits:
                send(block(0, 0).at[part], att.at[b, 0, part], sent.at[0], zr.at[b, h], {"tensor": flip(ten, b)})
        dp_sends(0, 0, h, high + [1])
    for wave in waves:
        for h in (0, 1):
            for s in wave:
                await_into(att.at[s, 0, pl.ds(h * half, half)], zr.at[s, h])
                z_sends(s, h)
                dp_sends(0, s, h, high + [1])

    for s in walk:
        partial(0, s)
    fin[0, 0] = prod[0]
    spread(0, 0)
    relay(1, walk[0])
    own_results(pairs[0])
    for level in range(1, len(levels)):
        for s in walk[1:-1] if level == 1 else walk[:-1]:
            near(level, s)
            if s == walk[1] and level == 1:
                far(level, s)
        for s in walk[:-1]:
            partial(level, s)
        behind = pairs[level - 1]
        cut = len(behind) if level == 1 else len(behind) // 2
        pass_on(behind[:cut])
        near(level, walk[-1])
        partial(level, walk[-1])
        for s in walk[2:] if level == 1 else walk:
            far(level, s)
        pass_on(behind[cut:])
        own_results(pairs[level])
    pass_on(pairs[-1])
    for s in ending:
        await_into(fin.at[s], done_at(s, 0))
    one, rest = pl.ds(1, nt - 1), pl.ds(1, nd - 1)
    done = [(att.at[one, 0], 0), (att.at[:, rest], 1), (prod.at[rest], 2), (fin.at[one], 3)]
    return [(ref, sent.at[k]) for ref, k in done]


def block_kernel(nd, nt, refs_in, refs_out, inner, attn, outer):
    rows_ref, gain_ref, lens_ref, q_ref, k_ref, v_ref, o_ref, keys_ref, vals_ref = refs_in
    fin, fresh_ref, new_ref = refs_out
    hidden_ref, kept_keys, kept_vals, turn, qf, kf, vf, lf, of, kvs, ows = attn
    att, wt = outer[0], outer[2]
    ten = lax.axis_index("tensor")
    rows, heads = qf.shape[:2]
    qc, kc = q_ref.shape[1] // nt, k_ref.shape[1] // nt
    group = qc // kc
    wf = inner[0]
    feat, wide = wf.shape[2:]
    caches = [
        pltpu.make_async_copy(keys_ref, kept_keys, kvs.at[0]),
        pltpu.make_async_copy(vals_ref, kept_vals, kvs.at[1]),
    ]
    pieces = [(s, j) for s in range(nt) for j in range(qc // wide)]

    def out_load(i):
        s, j = pieces[i]
        at = pl.ds(pl.multiple_of(flip(ten, s) * qc + j * wide, wide), wide)
        return pltpu.make_async_copy(o_ref.at[:, at], wf.at[0, i] if i < wf.shape[1] else wf.at[1, i - wf.shape[1]], ows.at[0])

    row_copy = pltpu.make_async_copy(rows_ref, hidden_ref, kvs.at[2])

    def prefetch():
        row_copy.start()

    def late():
        for copy in caches:
            copy.start()

    def ready():
        row_copy.wait()

    def prepare():
        for i in range(len(pieces)):
            out_load(i).start()
        half_dim = HEAD_DIM // 2
        lens = jnp.broadcast_to(lens_ref[...].astype(F32), (HEAD_DIM, rows)).T
        lane = lax.broadcasted_iota(jnp.int32, (rows, HEAD_DIM), 1)
        low = lane < half_dim
        index = jnp.where(low, lane, lane - half_dim).astype(F32)
        angle = lens * jnp.exp(-math.log(rope_base) * index / half_dim)
        turn[0] = jnp.cos(angle)
        turn[1] = jnp.where(low, -jnp.sin(angle), jnp.sin(angle))
        for h in range(heads):
            lf[:, h, :] = lens
        pltpu.make_async_copy(o_ref, o_ref, ows.at[0]).wait()
        for i, (s, j) in enumerate(pieces):
            w = wf[0, i] if i < wf.shape[1] else wf[1, i - wf.shape[1]]
            wt[s, j * wide : (j + 1) * wide] = w.T.astype(BF)

    def place_columns(first, total):
        for j in range(0, total.shape[1], HEAD_DIM):
            x, at = total[:, j : j + HEAD_DIM], first + j
            if at < qc + kc:
                x = x * turn[0] + pltpu.roll(x, HEAD_DIM // 2, 1) * turn[1]
            x = x.astype(BF)
            if at < qc:
                qf[:, at // HEAD_DIM, :] = x.astype(F32)
                continue
            to, full, off = (fresh_ref, kf, at - qc) if at < qc + kc else (new_ref, vf, at - qc - kc)
            g = off // HEAD_DIM
            to[:, g, :] = x.astype(F32)
            for h in range(g * group, (g + 1) * group):
                full[:, h, :] = x.astype(F32)

    def attend_part(part):
        if part == 0:
            for copy in caches:
                copy.wait()
        kinds = kc // HEAD_DIM
        step, span = 32, kept_keys.shape[1]
        shape = (step, heads, span)
        spot = lax.broadcasted_iota(jnp.int32, shape, 2)
        mine = spot % kinds == lax.broadcasted_iota(jnp.int32, shape, 1) // group
        where = (spot // kinds).astype(F32)
        root = 1.0 / math.sqrt(HEAD_DIM)

        def some(i, carry):
            at = pl.ds(pl.multiple_of(part * (rows // 4) + i * step, step), step)
            q = qf[at]
            scores = root * lax.dot_general(
                q.astype(BF), kept_keys[at], (((2,), (2,)), ((0,), (0,))), preferred_element_type=F32
            )
            own = jnp.sum(q * kf[at], axis=-1, keepdims=True) * root
            scores = jnp.where(mine & (where < lf[at][:, :, :1]), scores, -jnp.inf)
            largest = jnp.maximum(jnp.max(scores, axis=-1, keepdims=True), own)
            kept = jnp.exp(scores - largest)
            own = jnp.exp(own - largest)
            divisor = jnp.sum(kept, axis=-1, keepdims=True) + own
            out = lax.dot_general(
                (kept / divisor).astype(BF), kept_vals[at],
                (((2,), (1,)), ((0,), (0,))), preferred_element_type=F32,
            )
            of[at] = out + (own / divisor).astype(BF).astype(F32) * vf[at]
            return carry

        lax.fori_loop(0, rows // 4 // step, some, 0)
        here = slice(part * (rows // 4), (part + 1) * (rows // 4))
        for h in range(heads):
            att[0, 0, here, h * HEAD_DIM : (h + 1) * HEAD_DIM] = of[here, h, :].astype(BF)

    sent = inputs_part(nd, nt, prefetch, late, ready, prepare, place_columns, hidden_ref, gain_ref, q_ref, k_ref, v_ref, *inner)
    sent += project_part(nd, nt, attend_part, fin, *outer)
    for ref, sem in sent:
        await_sent(ref, sem)


def block(hidden, gain, lengths, weights, key_cache, value_cache, nd, nt):
    rows, width = hidden.shape
    q_weight, k_weight, o_weight = weights[0], weights[1], weights[3]
    feat, wide = q_weight.shape[0], 256
    qc, kc = q_weight.shape[1] // nt, k_weight.shape[1] // nt
    heads = qc // HEAD_DIM
    C, half, H = (qc + 2 * kc) // wide * (nt // 2), nd // 2, nd.bit_length() - 2
    dma, vm = pltpu.SemaphoreType.DMA, pltpu.VMEM
    hop_bufs = [vm((C, half >> (l + 1), rows, wide), BF) for l in range(H)]
    in_place = pl.BlockSpec(memory_space=pltpu.VMEM)
    outside = pl.BlockSpec(memory_space=pl.ANY)
    span = key_cache.shape[1] * key_cache.shape[2]
    caches = [x.reshape(rows, span, HEAD_DIM) for x in (key_cache, value_cache)]
    inner = [
        vm((2, C, feat, wide), F32),
        vm((C, feat, wide), BF),
        vm((C, 2, feat, wide), BF),
        vm((nd, 2, rows, feat), BF),
        vm((2, 2, half, rows, feat), BF),
        vm((8, rows), F32),
        vm((nd, 8, rows), F32),
        vm((C, half, rows, wide), F32),
        vm((C, half, rows, wide), BF),
        vm((C, half, rows, wide), BF),
        *hop_bufs,
        *hop_bufs,
        vm((C, rows, wide), BF),
        vm((C, rows, wide), BF),
        dma((C + 1,)), dma((C,)), dma((nd,)), dma((nd,)), dma((C,)), dma((C, H)), dma((C,)), dma((5 + H,)),
    ]
    by_head = [vm((rows, heads, HEAD_DIM), F32)] * 5
    attn = [
        vm((rows, width), BF),
        vm((rows, span, HEAD_DIM), BF), vm((rows, span, HEAD_DIM), BF),
        vm((2, rows, HEAD_DIM), F32), *by_head, dma((3,)), dma((1,)),
    ]
    outer = [
        vm((nt, nd, rows, qc), BF),
        vm((nd, rows, feat), BF),
        vm((nt, qc, feat), BF),
        vm((nd // 2 * rows, feat), F32),
        dma((nt, 2)), dma((nt, nd)), dma((nd,)), dma((nd * (nt // 2),)), dma((4,)),
    ]
    ends = [9, 12, 12 + len(inner), 12 + len(inner) + len(attn)]

    def kernel(*refs):
        block_kernel(
            nd, nt, refs[: ends[0]], refs[ends[0] : ends[1]],
            refs[ends[1] : ends[2]], refs[ends[2] : ends[3]], refs[ends[3] :],
        )

    return pl.pallas_call(
        kernel,
        in_specs=[outside] + [in_place] * 2 + [outside] * 6,
        out_specs=[in_place] * 3,
        out_shape=[
            jax.ShapeDtypeStruct((nt, nd, rows, feat), BF),
            jax.ShapeDtypeStruct((rows, kc // HEAD_DIM, HEAD_DIM), F32),
            jax.ShapeDtypeStruct((rows, kc // HEAD_DIM, HEAD_DIM), F32),
        ],
        scratch_shapes=inner + attn + outer,
        compiler_params=pltpu.CompilerParams(
            collective_id=1, has_side_effects=True, vmem_limit_bytes=63 * 1024 * 1024
        ),
    )(hidden, gain.reshape(1, width), lengths.reshape(1, rows), *weights, *caches)


def shards(
    hidden,
    q_weight,
    k_weight,
    v_weight,
    o_weight,
    input_gain,
    post_gain,
    key_cache,
    value_cache,
    lengths,
):
    nt = lax.axis_size("tensor")
    nd = lax.axis_size("dp")
    me, ten = lax.axis_index("dp"), lax.axis_index("tensor")
    rows, width = hidden.shape
    heads_here, kv_here = HEADS // nt, KV_HEADS // nt
    qc, kc = heads_here * HEAD_DIM, kv_here * HEAD_DIM
    feat = q_weight.shape[0]
    low, high = [1], bits_of(nd)[1:]
    orders = (low + high, low + high[::-1])
    odd = [m for m in range(nd) if m & 1]
    even = [m for m in range(nd) if not m & 1]
    count = rows // CHUNKS

    def columns(w, s, n):
        return lax.dynamic_slice_in_dim(w, (ten ^ s) * n, n, 1).astype(BF)

    together = feat % 128 == 0 and kc % 256 == 0 and rows == 128 and nt > 1 and nd > 2 and CHUNKS == 1
    together = together and kv_here * key_cache.shape[1] == 128 and heads_here == 8
    if together:
        weights = (q_weight, k_weight, v_weight, o_weight)
        mine, keys, news = block(hidden, input_gain, lengths, weights, key_cache, value_cache, nd, nt)
        return tuple(finish(hidden, post_gain, mine, keys, news, nd, nt, feat))
    pieces = norm_pieces(hidden, input_gain, nd, nt, feat)
    pieces = [swap(p, "dp", m, nd) if m else p for m, p in enumerate(pieces)]
    w_in = [
        jnp.concatenate(
            [columns(q_weight, s, qc), columns(k_weight, s, kc), columns(v_weight, s, kc)], axis=1
        )
        for s in range(nt)
    ]
    w_out = [columns(o_weight, s, qc) for s in range(nt)]

    fresh, values, outs = [], [], None
    for c in range(CHUNKS):
        r0 = c * count
        cut = [p[r0 : r0 + count] for p in pieces]
        lhs_odd = jnp.concatenate([cut[m] for m in odd])
        lhs_even = jnp.concatenate([cut[m] for m in even])
        total, behind = None, []
        for k, s in enumerate(reversed(range(nt))):
            if k and k % 2 == 0:
                held = lax.optimization_barrier((lhs_odd, lhs_even, *behind))
                lhs_odd, lhs_even, behind = held[0], held[1], []
            away = jnp.dot(lhs_odd, w_in[s], preferred_element_type=F32).astype(BF)
            got = swap(away, "dp", 1, nd)
            behind.append(got)
            acc = jnp.dot(lhs_even, w_in[s], preferred_element_type=F32) + got.astype(F32)
            acc = acc.astype(BF).reshape(len(even), count, -1)
            parts = {m: acc[j] for j, m in enumerate(even)}
            part = scatter_sum(parts, orders[k % 2][1:], "dp", nd)
            part = (swap(part, "tensor", s, nt) if s else part).astype(F32)
            total = part if total is None else total + part
        query, key_part, value_part = total[:, :qc], total[:, qc : qc + kc], total[:, qc + kc :]

        here = slice(r0, r0 + count)
        query_b = rotate(query.reshape(count, heads_here, HEAD_DIM), lengths[here]).astype(BF)
        keys = rotate(key_part.reshape(count, kv_here, HEAD_DIM), lengths[here]).astype(BF)
        news = value_part.reshape(count, kv_here, HEAD_DIM).astype(BF)
        fresh.append(keys)
        values.append(news)
        attended = attend(
            query_b, keys, news, key_cache[here], value_cache[here], lengths[here]
        )

        by_tensor = gather_all(attended, bits_of(nt)[::-1], "tensor", nt)
        product = None
        for k, s in enumerate(sorted(by_tensor, key=lambda s: (s & 1, s))):
            blocks = gather_all(by_tensor[s], orders[k % 2][1:] + low, "dp", nd)
            lhs = jnp.concatenate([blocks[m] for m in range(nd)])
            term = lax.dot_general(
                lhs, w_out[s], (((1,), (1,)), ((), ())), preferred_element_type=F32
            )
            product = term if product is None else product + term
        product = product.astype(BF).reshape(nd, count, feat)
        mine = jnp.stack([swap(product[m], "dp", m, nd) if m else product[0] for m in range(nd)])
        for b in bits_of(nd):
            v = mine.reshape(nd // (2 * b), 2, b, count, feat)
            mine = jnp.where((me & b) != 0, v[:, ::-1], v).reshape(nd, count, feat)
        mine = mine[None]
        for b in bits_of(nt)[::-1]:
            got = swap(mine, "tensor", b, nt)
            first = jnp.where((ten & b) != 0, got, mine)
            second = jnp.where((ten & b) != 0, mine, got)
            mine = jnp.stack([first, second], axis=1).reshape((-1,) + mine.shape[1:])
        mixed = mine.transpose(2, 1, 0, 3).reshape(count, width).astype(F32)
        residual = hidden[here].astype(F32) + mixed
        pair = (residual.astype(BF), rms_gain(residual, post_gain).astype(BF))
        outs = pair if outs is None else tuple(jnp.concatenate(z) for z in zip(outs, pair))
    return (outs[0], outs[1], jnp.concatenate(fresh), jnp.concatenate(values))


def solution(mesh):
    in_specs = (
        P("dp", None),
        P(("dp", "tensor"), None),
        P(("dp", "tensor"), None),
        P(("dp", "tensor"), None),
        P(("dp", "tensor"), None),
        P(),
        P(),
        P("dp", None, "tensor", None),
        P("dp", None, "tensor", None),
        P("dp"),
    )
    out_specs = (P("dp", None), P("dp", None), P("dp", "tensor", None), P("dp", "tensor", None))
    return jax.shard_map(shards, mesh=mesh, in_specs=in_specs, out_specs=out_specs, check_vma=False)
```
